256 devices in a mesh: grp: 4 (over y_hi, core), blk: 64 (over z, x, y_lo).
Axes of the slice: x: 4, y: 4 (y_hi: 2, y_lo: 2; y = y_hi * 2 + y_lo), z: 8, core: 2. Of those that a mesh axis runs over, the one named last changes fastest.
Arguments:
- primal: float32 [2097152], P(('blk', 'grp')), may hold values from -3 to 3
- dual: float32 [1048576], P(('blk', 'grp')), may hold values from -3 to 3
- objective: float32 [2097152], P(('blk', 'grp')), may hold values from -6 to 6
- lower: float32 [2097152], P(('blk', 'grp')), may hold values from -2 to -0.5
- upper: float32 [2097152], P(('blk', 'grp')), may hold values from 0.5 to 2
- bound_kind: int32 [2097152], P(('blk', 'grp')), may hold values from 0 to 3
- rhs: float32 [1048576], P(('blk', 'grp')), may hold values from -6 to 6
- row_kind: int32 [1048576], P(('blk', 'grp')), may hold values 0 or 1
- q_tiles: float32 [4, 256, 512, 512], P('grp', 'blk'), may hold values from -0.25 to 0.25
- q_index: int32 [4, 2, 256], P('grp', None, 'blk'), may hold values from 0 to 1023
- k_tiles: float32 [4, 384, 512, 512], P('grp', 'blk'), may hold values from -0.25 to 0.25
- k_rows: int32 [4, 384], P('grp', 'blk'), may hold values from 0 to 31
- k_cols: int32 [4, 384], P('grp', 'blk'), may hold values from 0 to 1023
Outputs:
- final_primal: float32 [2097152], P(('blk', 'grp'))
- final_dual: float32 [1048576], P(('blk', 'grp'))
- primal_weight: float32 [], replicated
The draws below stay inside these ranges and needn't reach their ends.
Inputs may be any that keep to these rules, and one draw needn't show every extreme that they name: `q_index`: row and column tile indices of Hessian tiles, within the column group. `k_rows`: row tile within the tile's dual block. `bound_kind`: 0 free, 1 lower bound only, 2 both bounds, 3 upper bound only.
All inputs are finite; a program needn't handle non-finite values. No bound on the sum of `row_kind` on one device may be relied on, other than what follows from the above.
Results may differ from the reference program's by a relative error of at most 0.00017.
Values sent between devices are 32-bit elements; how exact they have to be, the bound alone decides.
No kernel may reach another device: no remote copies, remote signals or barrier semaphores. Data moves between devices by JAX's collectives and lax.ppermute only.
A program may use at most 64 MiB of HBM per device.

```python
import jax
import jax.numpy as jnp
from jax import lax

TILE = 512
X_DEV = 8192
Y_DEV = 4096
KT = 6
ITERS = 2
NX = 2097152
M = 1048576
GT_COUNT = 1024
RT = 32
QTILES = 256
KTILES = 384
N_GRP = 4
N_BLK = 64


def place_ends(result, rng, smallest, top_value):
    dims = result.shape
    place = [jax.random.randint(jax.random.fold_in(rng, axis), (), 0, dims[axis]) for axis in range(len(dims))]
    result = result.at[tuple(place)].set(smallest)
    longest = dims.index(max(dims))
    place[longest] = (place[longest] + 1) % dims[longest]
    return result.at[tuple(place)].set(top_value)


def steps_of(key, extent, split, low, largest):
    def one(axis_at, blocks):
        draws = jax.random.uniform(jax.random.fold_in(jax.random.fold_in(key, 6), axis_at), (blocks,), jnp.float32, low / len(split), largest / len(split))
        return jnp.repeat(jnp.exp(draws), extent[axis_at] // blocks).reshape((-1,) + (1,) * (len(extent) - axis_at - 1))

    gain = one(*split[0])
    for cut in split[1:]:
        gain = gain * one(*cut)
    return gain


def scatter_about(key, shape, spread, reach, cuts=(), kind=jnp.bfloat16):
    result = spread * jax.random.normal(key, shape, jnp.float32)
    if cuts:
        result = result * steps_of(key, shape, cuts, -0.22, 0.18)
    return jnp.clip(result, -reach, reach).astype(kind)


def setup_inputs(seed: int = 0) -> dict:
    keys = jax.random.split(jax.random.key(seed), 14)
    return {
        "primal": scatter_about(keys[0], (NX,), 0.5, 3.0, ((0, 256),), jnp.float32),
        "dual": scatter_about(keys[1], (M,), 0.5, 3.0, ((0, 256),), jnp.float32),
        "objective": scatter_about(keys[2], (NX,), 1.0, 6.0, ((0, 256),), jnp.float32),
        "lower": jnp.clip(-2.0 + 1.5 * jax.random.uniform(keys[3], (NX,), jnp.float32) ** steps_of(keys[3], (NX,), ((0, 256),), -0.2, 0.2), -2.0, -0.5),
        "upper": jnp.clip(0.5 + 1.5 * jax.random.uniform(keys[4], (NX,), jnp.float32) ** steps_of(keys[4], (NX,), ((0, 256),), -0.2, 0.2), 0.5, 2.0),
        "bound_kind": place_ends(jax.random.randint(keys[5], (NX,), 0, 4), jax.random.fold_in(keys[5], 1), 0, 3).astype(jnp.int32),
        "rhs": scatter_about(keys[6], (M,), 1.0, 6.0, ((0, 256),), jnp.float32),
        "row_kind": place_ends((jax.random.randint(keys[7], (M,), 0, 2) < 1).astype(jnp.int32), jax.random.fold_in(keys[7], 1), 0, 1),
        "q_tiles": scatter_about(keys[8], (N_GRP, QTILES, TILE, TILE), TILE ** -0.5, 0.25, ((0, 4), (1, 64)), jnp.float32),
        "q_index": place_ends(jax.random.randint(keys[9], (N_GRP, 2, QTILES), 0, GT_COUNT), jax.random.fold_in(keys[9], 1), 0, GT_COUNT - 1).astype(jnp.int32),
        "k_tiles": scatter_about(keys[10], (N_GRP, KTILES, TILE, TILE), TILE ** -0.5, 0.25, ((0, 4), (1, 64)), jnp.float32),
        "k_rows": place_ends(jax.random.randint(keys[11], (N_GRP, KTILES), 0, RT), jax.random.fold_in(keys[11], 1), 0, RT - 1).astype(jnp.int32),
        "k_cols": place_ends(jax.random.randint(keys[12], (N_GRP, KTILES), 0, GT_COUNT), jax.random.fold_in(keys[12], 1), 0, GT_COUNT - 1).astype(jnp.int32),
    }


def apply_tiles(tiles, rows, cols, vec, count):
    pieces = vec.reshape(-1, TILE)[cols]
    product = jnp.einsum('tij,tj->ti', tiles, pieces, precision=lax.Precision.HIGHEST)
    return jnp.zeros((count, TILE), product.dtype).at[rows].add(product).reshape(-1)

def apply_transposed(tiles, rows, cols, vec, count):
    pieces = vec.reshape(-1, TILE)[rows]
    product = jnp.einsum('tij,ti->tj', tiles, pieces, precision=lax.Precision.HIGHEST)
    return jnp.zeros((count, TILE), product.dtype).at[cols].add(product).reshape(-1)

def project(values, lower, upper, bound_kind):
    values = jnp.where((bound_kind == 1) | (bound_kind == 2), jnp.maximum(values, lower), values)
    return jnp.where((bound_kind == 2) | (bound_kind == 3), jnp.minimum(values, upper), values)

def reference(primal, dual, objective, lower, upper, bound_kind, rhs, row_kind, q_tiles, q_index, k_tiles, k_rows, k_cols):
    group_tiles = N_BLK * X_DEV // TILE
    block_tiles = N_GRP * Y_DEV // TILE
    owner = (jnp.arange(N_BLK * KT) // KT).astype(jnp.int32)

    def group_vec(values, group):
        return values.reshape(N_BLK, N_GRP, X_DEV)[:, group, :].reshape(-1)

    def to_layout(parts):
        return jnp.stack([p.reshape(N_BLK, X_DEV) for p in parts], axis=1).reshape(-1)

    def forward(values):
        cons_prod = None
        parts = []
        for group in range(N_GRP):
            column_vec = group_vec(values, group)
            parts.append(apply_tiles(q_tiles[group], q_index[group, 0], q_index[group, 1], column_vec, group_tiles))
            term = apply_tiles(k_tiles[group], owner * block_tiles + k_rows[group], k_cols[group], column_vec, N_BLK * block_tiles)
            cons_prod = term if cons_prod is None else cons_prod + term
        return (cons_prod, to_layout(parts))

    def transposed(duals):
        parts = []
        for group in range(N_GRP):
            parts.append(apply_transposed(k_tiles[group], owner * block_tiles + k_rows[group], k_cols[group], duals, group_tiles))
        return to_layout(parts)
    weight = jnp.asarray(1.0, jnp.float32)
    current, duals = (primal, dual)
    cons_prod, hess_prod = forward(current)
    for step in range(ITERS):
        step_primal = 0.5 / weight
        step_dual = 0.5 * weight
        gradient = hess_prod + objective - transposed(duals)
        updated = project(current - step_primal * gradient, lower, upper, bound_kind)
        next_cons, next_hess = forward(updated)
        extrap = 2.0 * next_cons - cons_prod
        dual_new = duals + step_dual * (rhs - extrap)
        dual_new = jnp.where(row_kind == 1, jnp.maximum(dual_new, 0.0), dual_new)
        primal_sq = jnp.sum((updated - current) ** 2)
        dual_sq = jnp.sum((dual_new - duals) ** 2)
        weight = jnp.sqrt(weight * jnp.sqrt((dual_sq + 1e-06) / (primal_sq + 1e-06)))
        current, duals = (updated, dual_new)
        cons_prod, hess_prod = (next_cons, next_hess)
    return (current, duals, weight)
```

```python
import jax
import jax.numpy as jnp
from jax import lax
from jax.sharding import Mesh
from jax.sharding import PartitionSpec as P

ITERS = 2
BLK = ("blk_0", "blk_1", "blk_2")
GRP = ("grp_0", "grp_1")
BLK_GRP = ("blk_0", "blk_1", "blk_2", "grp_0", "grp_1")
EPSILON = 1e-06
STEP_SCALE = 0.5
HIGHEST = lax.Precision.HIGHEST

NB = 64
OWN = 16
TILE = 512
LANES = 128
SLOTS = 16


def exchange(rows):
    k = rows.shape[0] // NB
    out = lax.all_to_all(rows.reshape(NB, 1, k * LANES), BLK, 0, 0, tiled=True)
    return out.reshape(NB * k, LANES)


def spread(rows):
    return rows.reshape(NB, 2, NB).transpose(2, 1, 0).reshape(NB, LANES)


def pieces_of(table):
    return table.reshape(NB, 2, SLOTS, 4).transpose(0, 2, 1, 3).reshape(NB * SLOTS, 8)


def table_of(pieces):
    return pieces.reshape(NB, SLOTS, 2, 4).transpose(0, 2, 1, 3).reshape(NB, LANES)


def over_group(rows):
    parts = [rows]
    for k in (1, 2, 3):
        parts.append(lax.ppermute(rows, GRP, [(i, i ^ k) for i in range(4)]))
    return parts


def shards(primal, dual, objective, lower, upper, bound_kind, rhs, row_kind,
           q_tiles, q_index, k_tiles, k_rows, k_cols):
    hess = q_tiles[0]
    cons = k_tiles[0]
    nq, nk = hess.shape[0], cons.shape[0]
    me = lax.axis_index(GRP)
    low = jnp.where((bound_kind == 1) | (bound_kind == 2), lower, -jnp.inf)
    high = jnp.where((bound_kind == 2) | (bound_kind == 3), upper, jnp.inf)
    ids = jnp.concatenate([q_index[0, 1], k_cols[0], q_index[0, 0]]).astype(jnp.float32)
    ids = jnp.pad(ids, (0, LANES - ids.shape[0]))
    first = jnp.stack(
        [spread(v.reshape(NB, LANES)) for v in (primal, objective, low, high)]
        + [jnp.broadcast_to(ids, (NB, LANES))],
        axis=1,
    )
    y_own = jnp.concatenate([
        dual.reshape(-1, LANES), rhs.reshape(-1, LANES), row_kind.astype(jnp.float32).reshape(-1, LANES),
        jnp.pad(k_rows[0].astype(jnp.float32), (0, LANES - nk))[None]])
    y_parts = over_group(y_own)
    n = dual.shape[0] // LANES
    duals = jnp.concatenate([p[:n] for p in y_parts]).reshape(-1, TILE)
    rhs_all = jnp.concatenate([p[n:2 * n] for p in y_parts]).reshape(-1, TILE)
    kind_all = jnp.concatenate([p[2 * n:3 * n] for p in y_parts]).reshape(-1, TILE)
    rows_all = jnp.concatenate([p[3 * n, :nk] for p in y_parts]).astype(jnp.int32)
    rows_all = (((rows_all >> 3) ^ me) << 3) | (rows_all & 7)

    got = exchange(first.reshape(-1, LANES)).reshape(NB, 5, LANES)
    x, c, low, high, ids = (got[:, i] for i in range(5))
    ids = ids.astype(jnp.int32)
    cols = ids[:, : nq + nk]
    rows = jnp.concatenate([ids[:, nq + nk : 2 * nq + nk], ids[:, nq : nq + nk]], axis=1)

    def gather(hess_table, cons_table, extra):
        a = pieces_of(hess_table)[cols[:, :nq]]
        b = pieces_of(cons_table)[cols[:, nq:]]
        e = jnp.zeros((NB, SLOTS - nq - nk, 8), jnp.float32).at[:, -1, 0].set(extra)
        return table_of(jnp.concatenate([a, b, e], axis=1))

    def scatter(msg):
        p = pieces_of(msg).reshape(NB, SLOTS, 8)
        extra = jnp.sum(p[:, -1, 0])
        return table_of(jnp.zeros((NB * OWN, 8), jnp.float32).at[rows].add(p[:, : nq + nk])), extra

    def matvec(tiles, vecs):
        return jnp.einsum("tij,tj->ti", tiles, vecs, precision=HIGHEST)

    def trans(y):
        return jnp.einsum("tij,ti->tj", cons, y[rows_all[:nk]], precision=HIGHEST)

    def pack(hp, tp, extra):
        e = jnp.zeros((SLOTS - nq - nk, TILE), jnp.float32)
        m = spread(jnp.concatenate([hp, -tp, e]).reshape(NB, LANES))
        return m.at[:, (SLOTS - 1) * 4].set(extra)

    def unpack(msg):
        extra = jnp.sum(msg[:, (SLOTS - 1) * 4])
        return spread(msg).reshape(SLOTS, TILE), extra

    weight = jnp.asarray(1.0, jnp.float32)
    want, _ = unpack(exchange(gather(x, x, 0.0)))
    dual_sq = jnp.asarray(0.0, jnp.float32)
    primal_sq = jnp.asarray(0.0, jnp.float32)
    for step in range(ITERS):
        hess_prod = matvec(hess, want[:nq])
        grad, dual_sum = scatter(exchange(pack(hess_prod, trans(duals), dual_sq)))
        if step > 0:
            weight = jnp.sqrt(weight * jnp.sqrt((dual_sum + EPSILON) / (primal_sq + EPSILON)))
        x_new = jnp.minimum(jnp.maximum(x - (STEP_SCALE / weight) * (grad + c), low), high)
        moved = x_new - x
        msg = gather(x_new, 2.0 * x_new - x, jnp.sum(moved * moved))
        x = x_new
        if step == ITERS - 1:
            both = exchange(jnp.stack([msg, x], axis=1).reshape(-1, LANES)).reshape(NB, 2, LANES)
            msg = both[:, 0]
            final = spread(both[:, 1]).reshape(-1)
        else:
            msg = exchange(msg)
        want, primal_part = unpack(msg)
        prod = matvec(cons, want[nq : nq + nk])
        sent = jnp.concatenate([prod.reshape(-1, LANES), jnp.full((1, LANES), primal_part)])
        parts = over_group(sent)
        primal_sq = sum(p[-1, 0] for p in parts)
        prods = jnp.concatenate([p[:-1] for p in parts]).reshape(-1, TILE)
        extrap = jnp.zeros_like(duals).at[rows_all].add(prods)
        new = duals + (STEP_SCALE * weight) * (rhs_all - extrap)
        new = jnp.where(kind_all == 1.0, jnp.maximum(new, 0.0), new)
        dual_sq = jnp.sum((new - duals) ** 2)
        duals = new
    dual_sum = jnp.sum(exchange(jnp.full((NB, LANES), dual_sq))[:, 0])
    weight = jnp.sqrt(weight * jnp.sqrt((dual_sum + EPSILON) / (primal_sq + EPSILON)))
    return final, duals.reshape(-1)[: dual.shape[0]], weight


def solution(mesh):
    finer = Mesh(mesh.devices.reshape(2, 2, 8, 4, 2), ("grp_0", "grp_1", "blk_0", "blk_1", "blk_2"))
    placed = (P(BLK_GRP),) * 8 + (
        P(GRP, BLK, None, None),
        P(GRP, None, BLK),
        P(GRP, BLK, None, None),
        P(GRP, BLK),
        P(GRP, BLK),
    )
    return jax.shard_map(
        shards, mesh=finer, in_specs=placed,
        out_specs=(P(BLK_GRP), P(BLK_GRP), P()), check_vma=False,
    )
```

```python
import functools

import jax
import jax.numpy as jnp
from jax import lax
from jax.experimental import pallas as pl
from jax.experimental.pallas import tpu as pltpu
from jax.sharding import Mesh
from jax.sharding import PartitionSpec as P

BLK = ("blk_0", "blk_1", "blk_2")
GRP = ("grp_0", "grp_1")
BLK_GRP = ("blk_0", "blk_1", "blk_2", "grp_0", "grp_1")
EPSILON = 1e-06
STEP_SCALE = 0.5
F32, BF16, I32 = jnp.float32, jnp.bfloat16, jnp.int32

NB = 64
TILE = 512
LANES = 128
NQ, NK = 4, 6
NT = NQ + NK
EXTRA = 60
VMEM_LIMIT = 16 * 1024 * 1024


def iota(shape, dim):
    return lax.broadcasted_iota(I32, shape, dim)


def lane(rows=NB):
    return iota((rows, LANES), 1)


def slot_of(lanes):
    return (lanes >> 2) & 15


def split(v, n):
    parts = []
    for _ in range(n - 1):
        p = v.astype(BF16)
        parts.append(p)
        v = v - p.astype(F32)
    parts.append(v.astype(BF16))
    return parts


def dot(a, b):
    return jnp.dot(a, b, preferred_element_type=F32)


def spread(v):
    return jnp.transpose(jnp.concatenate([v, pltpu.roll(v, 64, 1)], axis=0))[:NB]


def total(v):
    return jnp.sum(jnp.sum(v, axis=0, keepdims=True), axis=1, keepdims=True)


def extra_of(msg):
    return total(jnp.where(lane() == EXTRA, msg, 0.0))


def with_extra(msg, value):
    return jnp.where(lane() == EXTRA, value, msg)


def along(v, idx):
    return jnp.take_along_axis(v, idx, axis=1)


def column(v, c):
    return jnp.broadcast_to(v[:, c : c + 1], v.shape)


def gather_tiles(ids, tables, picks):
    ln = lane()
    t_of = along(ids & 15, slot_of(ln))
    idx = (ln & 64) + t_of * 4 + (ln & 3)
    owner = ids >> 4
    msg = jnp.zeros((NB, LANES), F32)
    for which, table in enumerate(tables):
        slots = [j for j in range(NT) if picks[j] == which]
        if not slots:
            continue
        a, b, c = split(table, 3)
        right = jnp.concatenate([a, b, c, jnp.zeros_like(a)], axis=0)
        ones = []
        for j in slots:
            o = jnp.where((ln & 63) == column(owner, j), 1.0, 0.0).astype(BF16)
            ones.append(jnp.concatenate([o, o], axis=1))
        got = dot(jnp.concatenate(ones, axis=0), right)
        for n, j in enumerate(slots):
            msg = jnp.where(slot_of(ln) == j, along(got[n * NB : (n + 1) * NB], idx), msg)
    return msg


def scatter_tiles(msg, rows, hot):
    ln = lane()
    t_of = rows & 15
    high, low = [], []
    for j in range(NT):
        e = along(msg, (ln & 64) + j * 4 + (ln & 3))
        e = jnp.where(slot_of(ln) == column(t_of, j), e, 0.0)
        a, b = split(e, 2)
        high.append(a)
        low.append(b)
    return dot(hot, jnp.concatenate(high, axis=0)) + dot(hot, jnp.concatenate(low, axis=0))


def forward_tiles(tiles_ref, rows_ref, count, first):
    ln = lane()

    def one(t, out):
        base = t * TILE
        j = first + t
        vec = [rows_ref[pl.ds(4 * j + q, 1), :] for q in range(4)]
        for qo in range(4):
            for h in range(2):
                at = pl.ds(base + qo * 128 + h * 64, 64)
                p = tiles_ref[at, 0:128] * vec[0]
                for q in range(1, 4):
                    p = p + tiles_ref[at, q * 128 : (q + 1) * 128] * vec[q]
                s = jnp.sum(p, axis=1, keepdims=True)
                out = jnp.where(ln == h * 64 + 4 * j + qo, s, out)
        return out

    return lax.fori_loop(0, count, one, jnp.zeros((NB, LANES), F32))


def transposed_tiles(tiles_ref, cols, rows_ref, first):
    def one(t, cols):
        base = t * TILE
        acc = [jnp.zeros((8, LANES), F32) for _ in range(4)]
        for qo in range(4):
            for h in range(2):
                at = pl.ds(base + qo * 128 + h * 64, 64)
                v = column(cols, h * 64 + qo)
                for q in range(4):
                    p = tiles_ref[at, q * 128 : (q + 1) * 128] * v
                    acc[q] = acc[q] + jnp.sum(p.reshape(8, 8, LANES), axis=0)
        for q in range(4):
            rows_ref[pl.ds(4 * (first + t) + q, 1), :] = jnp.sum(acc[q], axis=0, keepdims=True)
        return pltpu.roll(cols, LANES - 4, 1)

    lax.fori_loop(0, NK, one, pltpu.roll(cols, LANES - 4 * first, 1))


def join(parts, part):
    low = (lane() & 32) == 0
    blocks = []
    for k in (0, 2):
        a, b = parts[k], parts[k + 1]
        if part == 0:
            blocks.append(jnp.where(low, a, pltpu.roll(b, 32, 1)))
        else:
            blocks.append(jnp.where(low, pltpu.roll(a, LANES - 32, 1), b))
    return jnp.concatenate(blocks, axis=1)


def dual_step(parts, hot, y, rhs, kind, step):
    high, low = [], []
    for p in parts:
        a, b = split(p, 2)
        high.append(a)
        low.append(b)
    extrap = dot(jnp.concatenate(high, axis=1), hot) + dot(jnp.concatenate(low, axis=1), hot)
    new = y + step * (rhs - extrap)
    new = jnp.where(kind == 1.0, jnp.maximum(new, 0.0), new)
    moved = new - y
    return new, total(moved * moved)


def new_weight(weight, dual_sq, primal_sq):
    return jnp.sqrt(weight * jnp.sqrt((dual_sq + EPSILON) / (primal_sq + EPSILON)))


def start_kernel(q_index, k_cols, primal, objective, lower, upper, bound_kind, out):
    kind = bound_kind[...]
    low = jnp.where((kind == 1) | (kind == 2), lower[...], -jnp.inf)
    high = jnp.where((kind == 2) | (kind == 3), upper[...], jnp.inf)
    for k, v in enumerate((primal[...], objective[...], low, high)):
        out[pl.ds(k, NB, stride=5), :] = spread(v)
    ln = lane(8)
    ids = jnp.zeros((8, LANES), F32)
    for j in range(NQ):
        ids = jnp.where(ln == j, q_index[1, j].astype(F32), ids)
        ids = jnp.where(ln == NT + j, q_index[0, j].astype(F32), ids)
    for j in range(NK):
        ids = jnp.where(ln == NQ + j, k_cols[0, j].astype(F32), ids)
    out[pl.ds(4, NB, stride=5), :] = jnp.broadcast_to(ids[:1], (NB, LANES))


def dual_start_kernel(k_rows, dual, rhs, row_kind, out):
    out[0:NB] = spread(jnp.concatenate([dual[...], rhs[...]], axis=0))
    ids = jnp.zeros((8, LANES), F32)
    ln = lane(8)
    for j in range(NK):
        ids = jnp.where(slot_of(ln) == NQ + j, k_rows[0, j].astype(F32), ids)
    kinds = spread(jnp.concatenate([row_kind[...].astype(F32), jnp.zeros((32, LANES), F32)], axis=0))
    out[NB : 2 * NB] = kinds
    out[2 * NB :] = ids


def first_gather_kernel(got, msg):
    ids = got[pl.ds(4, NB, stride=5), :].astype(I32)
    x = got[pl.ds(0, NB, stride=5), :]
    msg[...] = gather_tiles(ids, [x], [0] * NQ + [-1] * NK)


def tables_kernel(got, rows_out, hot_out):
    ids = got[pl.ds(4, NB, stride=5), :].astype(I32)
    ln = lane()
    rows = jnp.where(ln < NQ, pltpu.roll(ids, LANES - NT, 1), ids)
    rows_out[...] = rows
    owner = (rows >> 4).astype(F32)
    flat = jnp.transpose(jnp.concatenate([owner, owner], axis=0))
    sub = iota((NB, LANES), 0).astype(F32)
    l1 = lane(1)
    for c in range(NT // 2):
        row = jnp.where(l1 < 64, flat[2 * c : 2 * c + 1], flat[2 * c + 1 : 2 * c + 2])
        hot_out[:, c * LANES : (c + 1) * LANES] = jnp.where(sub == row, 1.0, 0.0).astype(BF16)


def dual_tables_kernel(me, p0, p1, p2, p3, y, rhs, kind, put, take):
    parts = [p0, p1, p2, p3]
    y[...] = join([p[0:NB] for p in parts], 0)
    rhs[...] = join([p[0:NB] for p in parts], 1)
    kind[...] = join([p[NB : 2 * NB] for p in parts], 0)
    mine = me[0]
    rel = []
    for p in parts:
        r = p[2 * NB :].astype(I32)
        rel.append((((r >> 3) ^ mine) << 3) | (r & 7))
    ln = lane(LANES)
    sub = iota((LANES, LANES), 0)
    sub_ok = (slot_of(sub) >= NQ) & (slot_of(sub) < NT)
    for p in range(4):
        r = jnp.transpose(jnp.broadcast_to(rel[p][:1].astype(F32), (LANES, LANES))).astype(I32)
        same = ((ln & 64) == (sub & 64)) & ((ln & 3) == (sub & 3)) & sub_ok
        for kk in range(2):
            tile = (2 * kk + ((ln >> 5) & 1)) * 8 + ((ln >> 2) & 7)
            hit = same & (tile == r)
            put[p * LANES : (p + 1) * LANES, kk * LANES : (kk + 1) * LANES] = jnp.where(hit, 1.0, 0.0).astype(BF16)
    r = jnp.broadcast_to(rel[0][:1], (LANES, LANES))
    lane_ok = (slot_of(ln) >= NQ) & (slot_of(ln) < NT)
    for kk in range(2):
        tile = (2 * kk + ((sub >> 5) & 1)) * 8 + ((sub >> 2) & 7)
        hit = ((ln & 64) == (sub & 64)) & ((ln & 3) == (sub & 3)) & lane_ok & (tile == r)
        take[kk * LANES : (kk + 1) * LANES, :] = jnp.where(hit, 1.0, 0.0).astype(BF16)


def take_rows(y, take):
    a, b = split(y, 2)
    return dot(a, take) + dot(b, take)


def transposed_kernel(y, take, tiles, out, rows):
    rows[...] = jnp.zeros((NB, LANES), F32)
    transposed_tiles(tiles, take_rows(y[...], take[...]), rows, NQ)
    out[...] = spread(rows[...])


def first_products_kernel(msg, trans, tiles, out, rows):
    rows[...] = spread(msg[...])
    out[...] = with_extra(forward_tiles(tiles, rows, NQ, 0) - trans[...], 0.0)


def primal_step(msg, rows, hot, got, x, weight):
    c = got[pl.ds(1, NB, stride=5), :]
    low = got[pl.ds(2, NB, stride=5), :]
    high = got[pl.ds(3, NB, stride=5), :]
    grad = scatter_tiles(msg, rows, hot) + c
    new = jnp.minimum(jnp.maximum(x - (STEP_SCALE / weight) * grad, low), high)
    moved = new - x
    return new, total(moved * moved)


def first_primal_kernel(msg, got, rows, hot, x_out, out):
    x = got[pl.ds(0, NB, stride=5), :]
    new, moved = primal_step(msg[...], rows[...], hot[...], got, x, jnp.ones((1, 1), F32))
    x_out[...] = new
    ids = got[pl.ds(4, NB, stride=5), :].astype(I32)
    out[...] = with_extra(gather_tiles(ids, [new, 2.0 * new - x], [0] * NQ + [1] * NK), moved)


def second_primal_kernel(msg, got, rows, hot, x_in, primal_sq, weight_out, out):
    x = x_in[...]
    m = msg[...]
    weight = new_weight(jnp.ones((1, 1), F32), extra_of(m), primal_sq[...])
    weight_out[...] = weight
    new, moved = primal_step(m, rows[...], hot[...], got, x, weight)
    ids = got[pl.ds(4, NB, stride=5), :].astype(I32)
    out[pl.ds(0, NB, stride=2), :] = with_extra(gather_tiles(ids, [2.0 * new - x], [-1] * NQ + [0] * NK), moved)
    out[pl.ds(1, NB, stride=2), :] = new


def constraint_kernel(msg, tiles, out, vec, rows):
    m = msg[...]
    rows[...] = spread(m)
    vec[...] = rows[...]
    out[...] = with_extra(forward_tiles(tiles, rows, NK, NQ), extra_of(m))


def last_constraint_kernel(msg, tiles, out, final, rows):
    m = msg[pl.ds(0, NB, stride=2), :]
    final[...] = spread(msg[pl.ds(1, NB, stride=2), :])
    rows[...] = spread(m)
    out[...] = with_extra(forward_tiles(tiles, rows, NK, NQ), extra_of(m))


def hessian_kernel(vec, tiles, out):
    out[...] = forward_tiles(tiles, vec, NQ, 0)


def primal_total(parts):
    s = parts[0][0:1, EXTRA : EXTRA + 1]
    for p in parts[1:]:
        s = s + p[0:1, EXTRA : EXTRA + 1]
    return s


def dual_kernel(p0, p1, p2, p3, put, take, y, rhs, kind, hess, tiles, y_out, primal_sq, out, rows):
    parts = [p[...] for p in (p0, p1, p2, p3)]
    new, moved = dual_step(parts, put[...], y[...], rhs[...], kind[...], STEP_SCALE)
    y_out[...] = new
    primal_sq[...] = primal_total(parts)
    rows[...] = jnp.zeros((NB, LANES), F32)
    transposed_tiles(tiles, take_rows(new, take[...]), rows, NQ)
    out[...] = with_extra(hess[...] - spread(rows[...]), moved)


def last_dual_kernel(p0, p1, p2, p3, put, y, rhs, kind, weight, dual_out, primal_sq, out):
    parts = [p[...] for p in (p0, p1, p2, p3)]
    new, moved = dual_step(parts, put[...], y[...], rhs[...], kind[...], STEP_SCALE * weight[...])
    primal_sq[...] = primal_total(parts)
    dual_out[...] = spread(new[:, :LANES])[:32]
    out[...] = jnp.broadcast_to(moved, (NB, LANES))


def last_kernel(msg, weight, primal_sq, out):
    dual_sq = jnp.sum(msg[:, 0:1], axis=0, keepdims=True)
    out[...] = new_weight(weight[...], dual_sq, primal_sq[...])


def call(kernel, outs, *args, smem=0, scratch=(), cost=0):
    v = pl.BlockSpec(memory_space=pltpu.VMEM)
    s = pl.BlockSpec(memory_space=pltpu.SMEM)
    shapes = [jax.ShapeDtypeStruct(*o) for o in outs]
    res = pl.pallas_call(
        kernel,
        out_shape=shapes,
        in_specs=[s] * smem + [v] * (len(args) - smem),
        out_specs=[v] * len(shapes),
        scratch_shapes=list(scratch),
        compiler_params=pltpu.CompilerParams(vmem_limit_bytes=VMEM_LIMIT),
        cost_estimate=pl.CostEstimate(flops=cost, bytes_accessed=cost, transcendentals=0) if cost else None,
    )(*args)
    return res[0] if len(outs) == 1 else res


ROWS = ((NB, LANES), F32)
ROWS_SCRATCH = (pltpu.VMEM((NB, LANES), F32),)


def exchange(rows):
    k = rows.shape[0] // NB
    out = lax.all_to_all(rows.reshape(NB, 1, k * LANES), BLK, 0, 0, tiled=True)
    return out.reshape(NB * k, LANES)


def over_group(rows):
    return [rows] + [lax.ppermute(rows, GRP, [(i, i ^ k) for i in range(4)]) for k in (1, 2, 3)]


def shards(primal, dual, objective, lower, upper, bound_kind, rhs, row_kind, q_tiles, q_index, k_tiles, k_rows, k_cols):
    hess = q_tiles.reshape(NQ * TILE, TILE)
    cons = k_tiles.reshape(NK * TILE, TILE)
    me = lax.axis_index(GRP).astype(I32).reshape(1)

    def wide(v):
        return v.reshape(-1, LANES)

    first = call(start_kernel, [((5 * NB, LANES), F32)], q_index[0], k_cols, wide(primal), wide(objective), wide(lower),
                 wide(upper), wide(bound_kind), smem=2)
    block = call(dual_start_kernel, [((2 * NB + 8, LANES), F32)], k_rows, wide(dual), wide(rhs), wide(row_kind), smem=1)
    parts = over_group(block)
    got = exchange(first)
    msg = call(first_gather_kernel, [ROWS], got)
    want = exchange(msg)
    rows, hot = call(tables_kernel, [((NB, LANES), I32), ((NB, NT * NB), BF16)], got, cost=10000000)
    wide_block = ((NB, 2 * LANES), F32)
    y, b, kind, put, take = call(
        dual_tables_kernel,
        [wide_block, wide_block, wide_block, ((4 * LANES, 2 * LANES), BF16), ((2 * LANES, LANES), BF16)],
        me, *parts, smem=1, cost=10000000)
    trans = call(transposed_kernel, [ROWS], y, take, cons, scratch=ROWS_SCRATCH, cost=10000000)
    grads = exchange(call(first_products_kernel, [ROWS], want, trans, hess, scratch=ROWS_SCRATCH))
    x, msg = call(first_primal_kernel, [ROWS, ROWS], grads, got, rows, hot)
    want = exchange(msg)
    prods, vec = call(constraint_kernel, [ROWS, ROWS], want, cons, scratch=ROWS_SCRATCH)
    parts = over_group(prods)
    hess_prod = call(hessian_kernel, [ROWS], vec, hess, cost=10000000)
    y, primal_sq, msg = call(dual_kernel, [wide_block, ((1, 1), F32), ROWS], *parts, put, take, y, b, kind, hess_prod, cons,
                             scratch=ROWS_SCRATCH)
    grads = exchange(msg)
    weight, both = call(second_primal_kernel, [((1, 1), F32), ((2 * NB, LANES), F32)], grads, got, rows, hot, x, primal_sq)
    want = exchange(both)
    prods, final = call(last_constraint_kernel, [ROWS, ROWS], want, cons, scratch=ROWS_SCRATCH)
    parts = over_group(prods)
    dual_out, primal_sq, msg = call(last_dual_kernel, [((32, LANES), F32), ((1, 1), F32), ROWS], *parts, put, y, b, kind, weight)
    weight = call(last_kernel, [((1, 1), F32)], exchange(msg), weight, primal_sq)
    return final.reshape(-1), dual_out.reshape(-1), weight.reshape(())


def solution(mesh):
    finer = Mesh(mesh.devices.reshape(2, 2, 8, 4, 2), ("grp_0", "grp_1", "blk_0", "blk_1", "blk_2"))
    placed = (P(BLK_GRP),) * 8 + (
        P(GRP, BLK, None, None),
        P(GRP, None, BLK),
        P(GRP, BLK, None, None),
        P(GRP, BLK),
        P(GRP, BLK),
    )
    return jax.shard_map(shards, mesh=finer, in_specs=placed, out_specs=(P(BLK_GRP), P(BLK_GRP), P()), check_vma=False)
```

```python
import functools

import jax
import jax.numpy as jnp
from jax import lax
from jax.experimental import pallas as pl
from jax.experimental.pallas import tpu as pltpu
from jax.sharding import Mesh
from jax.sharding import PartitionSpec as P

BLK = ("blk_0", "blk_1", "blk_2")
GRP = ("grp_0", "grp_1")
BLK_GRP = ("blk_0", "blk_1", "blk_2", "grp_0", "grp_1")
EPSILON = 1e-06
STEP_SCALE = 0.5
F32, BF16, I32 = jnp.float32, jnp.bfloat16, jnp.int32

NB = 64
TILE = 512
LANES = 128
NQ, NK = 4, 6
NT = NQ + NK
EXTRA = 60
VMEM_LIMIT = 8 * 1024 * 1024
COST = 10000000000


def iota(shape, dim):
    return lax.broadcasted_iota(I32, shape, dim)


def lane(rows=NB):
    return iota((rows, LANES), 1)


def slot_of(lanes):
    return (lanes >> 2) & 15


def split(v, n):
    parts = []
    for _ in range(n - 1):
        p = v.astype(BF16)
        parts.append(p)
        v = v - p.astype(F32)
    parts.append(v.astype(BF16))
    return parts


def dot(a, b):
    return jnp.dot(a, b, preferred_element_type=F32)


def spread(v):
    return jnp.transpose(jnp.concatenate([v, pltpu.roll(v, 64, 1)], axis=0))[:NB]


def total(v):
    return jnp.sum(jnp.sum(v, axis=0, keepdims=True), axis=1, keepdims=True)


def extra_of(msg):
    return total(jnp.where(lane() == EXTRA, msg, 0.0))


def with_extra(msg, value):
    return jnp.where(lane() == EXTRA, value, msg)


def along(v, idx):
    return jnp.take_along_axis(v, idx, axis=1)


def column(v, c):
    return jnp.broadcast_to(v[:, c : c + 1], v.shape)


def gather_tiles(ids, tables, picks):
    ln = lane()
    t_of = along(ids & 15, slot_of(ln))
    idx = (ln & 64) + t_of * 4 + (ln & 3)
    owner = ids >> 4
    msg = jnp.zeros((NB, LANES), F32)
    for which, table in enumerate(tables):
        slots = [j for j in range(NT) if picks[j] == which]
        if not slots:
            continue
        a, b, c = split(table, 3)
        right = jnp.concatenate([a, b, c, jnp.zeros_like(a)], axis=0)
        ones = []
        for j in slots:
            o = jnp.where((ln & 63) == column(owner, j), 1.0, 0.0).astype(BF16)
            ones.append(jnp.concatenate([o, o], axis=1))
        got = dot(jnp.concatenate(ones, axis=0), right)
        for n, j in enumerate(slots):
            msg = jnp.where(slot_of(ln) == j, along(got[n * NB : (n + 1) * NB], idx), msg)
    return msg


def scatter_tiles(msg, rows, hot):
    ln = lane()
    t_of = rows & 15
    high, low = [], []
    for j in range(NT):
        e = along(msg, (ln & 64) + j * 4 + (ln & 3))
        e = jnp.where(slot_of(ln) == column(t_of, j), e, 0.0)
        a, b = split(e, 2)
        high.append(a)
        low.append(b)
    return dot(hot, jnp.concatenate(high, axis=0)) + dot(hot, jnp.concatenate(low, axis=0))


def forward_tiles(tiles_ref, rows_ref, count, first):
    ln = lane()

    def one(t, out):
        j = first + t
        vec = [rows_ref[pl.ds(4 * j + q, 1), :] for q in range(4)]
        for qo in range(4):
            for h in range(2):
                at = pl.ds(qo * 128 + h * 64, 64)
                p = tiles_ref[0, t, at, 0:128] * vec[0]
                for q in range(1, 4):
                    p = p + tiles_ref[0, t, at, q * 128 : (q + 1) * 128] * vec[q]
                s = jnp.sum(p, axis=1, keepdims=True)
                out = jnp.where(ln == h * 64 + 4 * j + qo, s, out)
        return out

    return lax.fori_loop(0, count, one, jnp.zeros((NB, LANES), F32))


def transposed_tiles(tiles_ref, cols, rows_ref, first):
    def one(t, cols):
        acc = [jnp.zeros((8, LANES), F32) for _ in range(4)]
        for qo in range(4):
            for h in range(2):
                at = pl.ds(qo * 128 + h * 64, 64)
                v = column(cols, h * 64 + qo)
                for q in range(4):
                    p = tiles_ref[0, t, at, q * 128 : (q + 1) * 128] * v
                    acc[q] = acc[q] + jnp.sum(p.reshape(8, 8, LANES), axis=0)
        for q in range(4):
            rows_ref[pl.ds(4 * (first + t) + q, 1), :] = jnp.sum(acc[q], axis=0, keepdims=True)
        return pltpu.roll(cols, LANES - 4, 1)

    lax.fori_loop(0, NK, one, pltpu.roll(cols, LANES - 4 * first, 1))


def join(parts, part):
    low = (lane() & 32) == 0
    blocks = []
    for k in (0, 2):
        a, b = parts[k], parts[k + 1]
        if part == 0:
            blocks.append(jnp.where(low, a, pltpu.roll(b, 32, 1)))
        else:
            blocks.append(jnp.where(low, pltpu.roll(a, LANES - 32, 1), b))
    return jnp.concatenate(blocks, axis=1)


def dual_step(parts, hot, y, rhs, kind, step):
    high, low = [], []
    for p in parts:
        a, b = split(p, 2)
        high.append(a)
        low.append(b)
    extrap = dot(jnp.concatenate(high, axis=1), hot) + dot(jnp.concatenate(low, axis=1), hot)
    new = y + step * (rhs - extrap)
    new = jnp.where(kind == 1.0, jnp.maximum(new, 0.0), new)
    moved = new - y
    return new, total(moved * moved)


def new_weight(weight, dual_sq, primal_sq):
    return jnp.sqrt(weight * jnp.sqrt((dual_sq + EPSILON) / (primal_sq + EPSILON)))


def spread_two(v, w):
    t = jnp.transpose(jnp.concatenate([v, w], axis=0))
    low = lane() < 64
    top, bottom = t[:NB], t[NB:]
    return jnp.where(low, top, pltpu.roll(bottom, 64, 1)), jnp.where(low, pltpu.roll(top, 64, 1), bottom)


def start_kernel(me, q_index, k_cols, k_rows, primal, objective, lower, upper, bound_kind, dual, rhs, row_kind, out, block, *scratch):
    refs = (q_index, k_cols, k_rows, primal, objective, lower, upper, bound_kind, dual, rhs, row_kind)
    sems = scratch[-1]
    copies = [pltpu.make_async_copy(r, s, sems.at[i]) for i, (r, s) in enumerate(zip(refs, scratch))]
    for c in copies:
        c.start()
    qi, kc, kr, p, ob, lo, up, bk, du, rh, rk = scratch[:-1]
    for c in copies:
        c.wait()
    kind = bk[...]
    low = jnp.where((kind == 1) | (kind == 2), lo[...], -jnp.inf)
    high = jnp.where((kind == 2) | (kind == 3), up[...], jnp.inf)
    a, b = spread_two(p[...], ob[...])
    c, d = spread_two(low, high)
    for k, v in enumerate((a, b, c, d)):
        out[pl.ds(k, NB, stride=5), :] = v
    ln = lane(8)
    ids = jnp.zeros((8, LANES), F32)
    for j in range(NQ):
        ids = jnp.where(ln == j, qi[1, j].astype(F32), ids)
        ids = jnp.where(ln == NT + j, qi[0, j].astype(F32), ids)
    for j in range(NK):
        ids = jnp.where(ln == NQ + j, kc[0, j].astype(F32), ids)
    out[pl.ds(4, NB, stride=5), :] = jnp.broadcast_to(ids[:1], (NB, LANES))
    a, b = spread_two(
        jnp.concatenate([du[...], rh[...]], axis=0),
        jnp.concatenate([rk[...].astype(F32), jnp.zeros((32, LANES), F32)], axis=0),
    )
    block[0:NB] = a
    block[NB : 2 * NB] = b
    ids = jnp.zeros((8, LANES), F32)
    for j in range(NK):
        ids = jnp.where(slot_of(ln) == NQ + j, kr[0, j].astype(F32), ids)
    block[2 * NB :] = jnp.where(ln == 0, me[0].astype(F32), ids)


def first_gather_kernel(got, p1, p2, p3, msg):
    ids = got[pl.ds(4, NB, stride=5), :].astype(I32)
    x = got[pl.ds(0, NB, stride=5), :]
    msg[...] = gather_tiles(ids, [x], [0] * NQ + [-1] * NK)


def primal_tables(got, rows_out, hot_out):
    ids = got[pl.ds(4, NB, stride=5), :].astype(I32)
    ln = lane()
    rows = jnp.where(ln < NQ, pltpu.roll(ids, LANES - NT, 1), ids)
    rows_out[...] = rows
    owner = (rows >> 4).astype(F32)
    flat = jnp.transpose(jnp.concatenate([owner, owner], axis=0))
    sub = iota((NB, LANES), 0).astype(F32)
    l1 = lane(1)
    for c in range(NT // 2):
        row = jnp.where(l1 < 64, flat[2 * c : 2 * c + 1], flat[2 * c + 1 : 2 * c + 2])
        hot_out[:, c * LANES : (c + 1) * LANES] = jnp.where(sub == row, 1.0, 0.0).astype(BF16)


def dual_tables(parts, y, rhs, kind, put, take):
    y[...] = join([p[0:NB] for p in parts], 0)
    rhs[...] = join([p[0:NB] for p in parts], 1)
    kind[...] = join([p[NB : 2 * NB] for p in parts], 0)
    mine = jnp.broadcast_to(parts[0][2 * NB :, 0:1], (8, LANES)).astype(I32)
    rel = []
    for p in parts:
        r = p[2 * NB :].astype(I32)
        rel.append((((r >> 3) ^ mine) << 3) | (r & 7))
    ln = lane(LANES)
    sub = iota((LANES, LANES), 0)
    sub_ok = (slot_of(sub) >= NQ) & (slot_of(sub) < NT)
    for p in range(4):
        r = jnp.transpose(jnp.broadcast_to(rel[p][:1].astype(F32), (LANES, LANES))).astype(I32)
        same = ((ln & 64) == (sub & 64)) & ((ln & 3) == (sub & 3)) & sub_ok
        for kk in range(2):
            tile = (2 * kk + ((ln >> 5) & 1)) * 8 + ((ln >> 2) & 7)
            hit = same & (tile == r)
            put[p * LANES : (p + 1) * LANES, kk * LANES : (kk + 1) * LANES] = jnp.where(hit, 1.0, 0.0).astype(BF16)
    r = jnp.broadcast_to(rel[0][:1], (LANES, LANES))
    lane_ok = (slot_of(ln) >= NQ) & (slot_of(ln) < NT)
    for kk in range(2):
        tile = (2 * kk + ((sub >> 5) & 1)) * 8 + ((sub >> 2) & 7)
        hit = ((ln & 64) == (sub & 64)) & ((ln & 3) == (sub & 3)) & lane_ok & (tile == r)
        take[kk * LANES : (kk + 1) * LANES, :] = jnp.where(hit, 1.0, 0.0).astype(BF16)


def take_rows(y, take):
    a, b = split(y, 2)
    return dot(a, take) + dot(b, take)


def first_products_kernel(msg, got, p0, p1, p2, p3, hess, cons, y, rhs, kind, put, take, rows_out, hot_out, out, rows):
    primal_tables(got, rows_out, hot_out)
    dual_tables([p0, p1, p2, p3], y, rhs, kind, put, take)
    rows[...] = spread(msg[...])
    first = forward_tiles(hess, rows, NQ, 0)
    rows[...] = jnp.zeros((NB, LANES), F32)
    transposed_tiles(cons, take_rows(y[...], take[...]), rows, NQ)
    out[...] = with_extra(first - spread(rows[...]), 0.0)


def primal_step(msg, rows, hot, got, x, weight):
    c = got[pl.ds(1, NB, stride=5), :]
    low = got[pl.ds(2, NB, stride=5), :]
    high = got[pl.ds(3, NB, stride=5), :]
    grad = scatter_tiles(msg, rows, hot) + c
    new = jnp.minimum(jnp.maximum(x - (STEP_SCALE / weight) * grad, low), high)
    moved = new - x
    return new, total(moved * moved)


def first_primal_kernel(msg, got, rows, hot, x_out, out):
    x = got[pl.ds(0, NB, stride=5), :]
    new, moved = primal_step(msg[...], rows[...], hot[...], got, x, jnp.ones((1, 1), F32))
    x_out[...] = new
    ids = got[pl.ds(4, NB, stride=5), :].astype(I32)
    out[...] = with_extra(gather_tiles(ids, [new, 2.0 * new - x], [0] * NQ + [1] * NK), moved)


def second_primal_kernel(msg, got, rows, hot, x_in, primal_sq, weight_out, out):
    x = x_in[...]
    m = msg[...]
    weight = new_weight(jnp.ones((1, 1), F32), extra_of(m), primal_sq[0:1, 0:1])
    weight_out[...] = jnp.broadcast_to(weight, (8, LANES))
    new, moved = primal_step(m, rows[...], hot[...], got, x, weight)
    ids = got[pl.ds(4, NB, stride=5), :].astype(I32)
    out[pl.ds(0, NB, stride=2), :] = with_extra(gather_tiles(ids, [2.0 * new - x], [-1] * NQ + [0] * NK), moved)
    out[pl.ds(1, NB, stride=2), :] = new


def constraint_kernel(msg, tiles, out, vec, rows):
    m = msg[...]
    rows[...] = spread(m)
    vec[...] = rows[...]
    out[...] = with_extra(forward_tiles(tiles, rows, NK, NQ), extra_of(m))


def last_constraint_kernel(msg, tiles, out, rows):
    m = msg[pl.ds(0, NB, stride=2), :]
    rows[...] = spread(m)
    out[...] = with_extra(forward_tiles(tiles, rows, NK, NQ), extra_of(m))


def hessian_kernel(vec, tiles, out):
    out[...] = forward_tiles(tiles, vec, NQ, 0)


def primal_total(parts):
    s = parts[0][0:1, EXTRA : EXTRA + 1]
    for p in parts[1:]:
        s = s + p[0:1, EXTRA : EXTRA + 1]
    return s


def dual_kernel(p0, p1, p2, p3, put, take, y, rhs, kind, hess, tiles, y_out, primal_sq, out, rows):
    parts = [p[...] for p in (p0, p1, p2, p3)]
    new, moved = dual_step(parts, put[...], y[...], rhs[...], kind[...], STEP_SCALE)
    y_out[...] = new
    primal_sq[...] = jnp.broadcast_to(primal_total(parts), (8, LANES))
    rows[...] = jnp.zeros((NB, LANES), F32)
    transposed_tiles(tiles, take_rows(new, take[...]), rows, NQ)
    out[...] = with_extra(hess[...] - spread(rows[...]), moved)


def last_dual_kernel(p0, p1, p2, p3, put, y, rhs, kind, weight, y_out, primal_sq, out):
    parts = [p[...] for p in (p0, p1, p2, p3)]
    new, moved = dual_step(parts, put[...], y[...], rhs[...], kind[...], STEP_SCALE * weight[0:1, 0:1])
    primal_sq[...] = jnp.broadcast_to(primal_total(parts), (8, LANES))
    y_out[...] = new[:, :LANES]
    out[...] = jnp.broadcast_to(moved, (NB, LANES))


def last_kernel(msg, y, want, weight, primal_sq, out, dual_out, final):
    dual_sq = jnp.sum(msg[:, 0:1], axis=0, keepdims=True)
    out[...] = new_weight(weight[0:1, 0:1], dual_sq, primal_sq[0:1, 0:1])
    dual_out[...] = spread(y[...])[:32]
    final[...] = spread(want[pl.ds(1, NB, stride=2), :])


def call(kernel, outs, *args, smem=0, scratch=(), cost=COST, where=pltpu.VMEM, limit=VMEM_LIMIT):
    v = pl.BlockSpec(memory_space=pltpu.VMEM)
    w = pl.BlockSpec(memory_space=where)
    s = pl.BlockSpec(memory_space=pltpu.SMEM)
    shapes = [jax.ShapeDtypeStruct(*o) for o in outs]
    res = pl.pallas_call(
        kernel,
        out_shape=shapes,
        in_specs=[s] * smem + [w] * (len(args) - smem),
        out_specs=[v] * len(shapes),
        scratch_shapes=list(scratch),
        compiler_params=pltpu.CompilerParams(vmem_limit_bytes=limit),
        cost_estimate=pl.CostEstimate(flops=cost, bytes_accessed=10000000, transcendentals=0),
    )(*args)
    return res[0] if len(outs) == 1 else res


ROWS = ((NB, LANES), F32)
ROWS_SCRATCH = (pltpu.VMEM((NB, LANES), F32),)


def exchange(rows):
    k = rows.shape[0] // NB
    out = lax.all_to_all(rows.reshape(NB, 1, k * LANES), BLK, 0, 0, tiled=True)
    return out.reshape(NB * k, LANES)


def over_group(rows):
    return [rows] + [lax.ppermute(rows, GRP, [(i, i ^ k) for i in range(4)]) for k in (1, 2, 3)]


def shards(primal, dual, objective, lower, upper, bound_kind, rhs, row_kind, q_tiles, q_index, k_tiles, k_rows, k_cols):
    hess, cons = q_tiles, k_tiles
    me = lax.axis_index(GRP).astype(I32).reshape(1)

    def wide(v):
        return v.reshape(-1, LANES)

    inputs = (q_index[0], k_cols, k_rows, wide(primal), wide(objective), wide(lower), wide(upper), wide(bound_kind), wide(dual),
              wide(rhs), wide(row_kind))
    room = [(pltpu.SMEM if i < 3 else pltpu.VMEM)(v.shape, v.dtype) for i, v in enumerate(inputs)]
    first, block = call(start_kernel, [((5 * NB, LANES), F32), ((2 * NB + 8, LANES), F32)], me, *inputs, smem=1, where=pltpu.HBM,
                        scratch=room + [pltpu.SemaphoreType.DMA((len(inputs),))], limit=66800000)
    parts = over_group(block)
    got = exchange(first)
    want = exchange(call(first_gather_kernel, [ROWS], got, *parts[1:]))
    wide_block = ((NB, 2 * LANES), F32)
    scalar = ((8, LANES), F32)
    y, b, kind, put, take, rows, hot, msg = call(
        first_products_kernel,
        [wide_block, wide_block, wide_block, ((4 * LANES, 2 * LANES), BF16), ((2 * LANES, LANES), BF16), ((NB, LANES), I32),
         ((NB, NT * NB), BF16), ROWS],
        want, got, *parts, hess, cons, scratch=ROWS_SCRATCH)
    grads = exchange(msg)
    x, msg = call(first_primal_kernel, [ROWS, ROWS], grads, got, rows, hot)
    want = exchange(msg)
    prods, vec = call(constraint_kernel, [ROWS, ROWS], want, cons, scratch=ROWS_SCRATCH)
    parts = over_group(prods)
    hess_prod = call(hessian_kernel, [ROWS], vec, hess, cost=10000000)
    y, primal_sq, msg = call(dual_kernel, [wide_block, scalar, ROWS], *parts, put, take, y, b, kind, hess_prod, cons,
                             scratch=ROWS_SCRATCH)
    grads = exchange(msg)
    weight, both = call(second_primal_kernel, [scalar, ((2 * NB, LANES), F32)], grads, got, rows, hot, x, primal_sq)
    want = exchange(both)
    prods = call(last_constraint_kernel, [ROWS], want, cons, scratch=ROWS_SCRATCH)
    parts = over_group(prods)
    y, primal_sq, msg = call(last_dual_kernel, [ROWS, scalar, ROWS], *parts, put, y, b, kind, weight)
    weight, dual_out, final = call(last_kernel, [((1, 1), F32), ((32, LANES), F32), ROWS], exchange(msg), y, want, weight, primal_sq)
    return final.reshape(-1), dual_out.reshape(-1), weight.reshape(())


def solution(mesh):
    finer = Mesh(mesh.devices.reshape(2, 2, 8, 4, 2), ("grp_0", "grp_1", "blk_0", "blk_1", "blk_2"))
    placed = (P(BLK_GRP),) * 8 + (
        P(GRP, BLK, None, None),
        P(GRP, None, BLK),
        P(GRP, BLK, None, None),
        P(GRP, BLK),
        P(GRP, BLK),
    )
    return jax.shard_map(shards, mesh=finer, in_specs=placed, out_specs=(P(BLK_GRP), P(BLK_GRP), P()), check_vma=False)
```

```python
import jax
import jax.numpy as jnp
from jax import lax
from jax.experimental import pallas as pl
from jax.experimental.pallas import tpu as pltpu
from jax.sharding import Mesh
from jax.sharding import PartitionSpec as P

BLK = ("blk_0", "blk_1", "blk_2")
GRP = ("grp_0", "grp_1")
BLK_GRP = ("blk_0", "blk_1", "blk_2", "grp_0", "grp_1")
EPSILON = 1e-06
STEP_SCALE = 0.5
F32, BF16, I32 = jnp.float32, jnp.bfloat16, jnp.int32

NB = 64
LANES = 128
NQ, NK = 4, 6
NT = NQ + NK
EXTRA = 60
VMEM_LIMIT = 8 * 1024 * 1024
COST = 10000000000


def iota(shape, dim):
    return lax.broadcasted_iota(I32, shape, dim)


def lane(rows=NB):
    return iota((rows, LANES), 1)


def slot_of(lanes):
    return (lanes >> 2) & 15


def split(v, n):
    parts = []
    for _ in range(n - 1):
        p = v.astype(BF16)
        parts.append(p)
        v = v - p.astype(F32)
    parts.append(v.astype(BF16))
    return parts


def dot(a, b):
    return jnp.dot(a, b, preferred_element_type=F32)


def spread(v):
    return jnp.transpose(jnp.concatenate([v, pltpu.roll(v, 64, 1)], axis=0))[:NB]


def total(v):
    return jnp.sum(jnp.sum(v, axis=0, keepdims=True), axis=1, keepdims=True)


def extra_of(msg):
    return total(jnp.where(lane() == EXTRA, msg, 0.0))


def with_extra(msg, value):
    return jnp.where(lane() == EXTRA, value, msg)


def along(v, idx):
    return jnp.take_along_axis(v, idx, axis=1)


def column(v, c):
    return jnp.broadcast_to(v[:, c : c + 1], v.shape)


def gather_tiles(ids, tables, picks):
    ln = lane()
    t_of = along(ids & 15, slot_of(ln))
    idx = (ln & 64) + t_of * 4 + (ln & 3)
    owner = ids >> 4
    msg = jnp.zeros((NB, LANES), F32)
    for which, table in enumerate(tables):
        slots = [j for j in range(NT) if picks[j] == which]
        if not slots:
            continue
        a, b, c = split(table, 3)
        right = jnp.concatenate([a, b, c, jnp.zeros_like(a)], axis=0)
        ones = []
        for j in slots:
            o = jnp.where((ln & 63) == column(owner, j), 1.0, 0.0).astype(BF16)
            ones.append(jnp.concatenate([o, o], axis=1))
        got = dot(jnp.concatenate(ones, axis=0), right)
        for n, j in enumerate(slots):
            msg = jnp.where(slot_of(ln) == j, along(got[n * NB : (n + 1) * NB], idx), msg)
    return msg


def scatter_tiles(msg, rows, hot):
    ln = lane()
    t_of = rows & 15
    high, low = [], []
    for j in range(NT):
        e = along(msg, (ln & 64) + j * 4 + (ln & 3))
        e = jnp.where(slot_of(ln) == column(t_of, j), e, 0.0)
        a, b = split(e, 2)
        high.append(a)
        low.append(b)
    return dot(hot, jnp.concatenate(high, axis=0)) + dot(hot, jnp.concatenate(low, axis=0))


def forward_tiles(tiles_ref, rows_ref, count, first):
    ln = lane()

    def one(t, out):
        j = first + t
        vec = [rows_ref[pl.ds(4 * j + q, 1), :] for q in range(4)]
        for qo in range(4):
            for h in range(2):
                at = pl.ds(qo * 128 + h * 64, 64)
                p = tiles_ref[0, t, at, 0:128] * vec[0]
                for q in range(1, 4):
                    p = p + tiles_ref[0, t, at, q * 128 : (q + 1) * 128] * vec[q]
                s = jnp.sum(p, axis=1, keepdims=True)
                out = jnp.where(ln == h * 64 + 4 * j + qo, s, out)
        return out

    return lax.fori_loop(0, count, one, jnp.zeros((NB, LANES), F32))


def transposed_tiles(tiles_ref, cols, rows_ref, first):
    def one(t, cols):
        acc = [jnp.zeros((8, LANES), F32) for _ in range(4)]
        for qo in range(4):
            for h in range(2):
                at = pl.ds(qo * 128 + h * 64, 64)
                v = column(cols, h * 64 + qo)
                for q in range(4):
                    p = tiles_ref[0, t, at, q * 128 : (q + 1) * 128] * v
                    acc[q] = acc[q] + jnp.sum(p.reshape(8, 8, LANES), axis=0)
        for q in range(4):
            rows_ref[pl.ds(4 * (first + t) + q, 1), :] = jnp.sum(acc[q], axis=0, keepdims=True)
        return pltpu.roll(cols, LANES - 4, 1)

    lax.fori_loop(0, NK, one, pltpu.roll(cols, LANES - 4 * first, 1))


def join(parts, part):
    low = (lane() & 32) == 0
    blocks = []
    for k in (0, 2):
        a, b = parts[k], parts[k + 1]
        if part == 0:
            blocks.append(jnp.where(low, a, pltpu.roll(b, 32, 1)))
        else:
            blocks.append(jnp.where(low, pltpu.roll(a, LANES - 32, 1), b))
    return jnp.concatenate(blocks, axis=1)


def dual_step(parts, hot, y, rhs, kind, step):
    high, low = [], []
    for p in parts:
        a, b = split(p, 2)
        high.append(a)
        low.append(b)
    extrap = dot(jnp.concatenate(high, axis=1), hot) + dot(jnp.concatenate(low, axis=1), hot)
    new = y + step * (rhs - extrap)
    new = jnp.where(kind == 1.0, jnp.maximum(new, 0.0), new)
    moved = new - y
    return new, total(moved * moved)


def new_weight(weight, dual_sq, primal_sq):
    return jnp.sqrt(weight * jnp.sqrt((dual_sq + EPSILON) / (primal_sq + EPSILON)))


def spread_two(v, w):
    t = jnp.transpose(jnp.concatenate([v, w], axis=0))
    low = lane() < 64
    top, bottom = t[:NB], t[NB:]
    return jnp.where(low, top, pltpu.roll(bottom, 64, 1)), jnp.where(low, pltpu.roll(top, 64, 1), bottom)


def start_kernel(me, q_index, k_cols, k_rows, primal, objective, lower, upper, bound_kind, dual, rhs, row_kind, out, block, *scratch):
    refs = (q_index, k_cols, k_rows, primal, objective, lower, upper, bound_kind, dual, rhs, row_kind)
    sems = scratch[-1]
    copies = [pltpu.make_async_copy(r, s, sems.at[i]) for i, (r, s) in enumerate(zip(refs, scratch))]
    for c in copies:
        c.start()
    qi, kc, kr, p, ob, lo, up, bk, du, rh, rk = scratch[:-1]
    for c in copies:
        c.wait()
    kind = bk[...]
    low = jnp.where((kind == 1) | (kind == 2), lo[...], -jnp.inf)
    high = jnp.where((kind == 2) | (kind == 3), up[...], jnp.inf)
    a, b = spread_two(p[...], ob[...])
    c, d = spread_two(low, high)
    for k, v in enumerate((a, b, c, d)):
        out[pl.ds(k, NB, stride=5), :] = v
    ln = lane(8)
    ids = jnp.zeros((8, LANES), F32)
    for j in range(NQ):
        ids = jnp.where(ln == j, qi[1, j].astype(F32), ids)
        ids = jnp.where(ln == NT + j, qi[0, j].astype(F32), ids)
    for j in range(NK):
        ids = jnp.where(ln == NQ + j, kc[0, j].astype(F32), ids)
    out[pl.ds(4, NB, stride=5), :] = jnp.broadcast_to(ids[:1], (NB, LANES))
    a, b = spread_two(
        jnp.concatenate([du[...], rh[...]], axis=0),
        jnp.concatenate([rk[...].astype(F32), jnp.zeros((32, LANES), F32)], axis=0),
    )
    block[0:NB] = a
    block[NB : 2 * NB] = b
    ids = jnp.zeros((8, LANES), F32)
    for j in range(NK):
        ids = jnp.where(slot_of(ln) == NQ + j, kr[0, j].astype(F32), ids)
    block[2 * NB :] = jnp.where(ln == 0, me[0].astype(F32), ids)


def first_gather_kernel(got, msg):
    ids = got[pl.ds(4, NB, stride=5), :].astype(I32)
    x = got[pl.ds(0, NB, stride=5), :]
    msg[...] = gather_tiles(ids, [x], [0] * NQ + [-1] * NK)


def primal_tables(got, rows_out, hot_out):
    ids = got[pl.ds(4, NB, stride=5), :].astype(I32)
    ln = lane()
    rows = jnp.where(ln < NQ, pltpu.roll(ids, LANES - NT, 1), ids)
    rows_out[...] = rows
    owner = (rows >> 4).astype(F32)
    flat = jnp.transpose(jnp.concatenate([owner, owner], axis=0))
    sub = iota((NB, LANES), 0).astype(F32)
    l1 = lane(1)
    for c in range(NT // 2):
        row = jnp.where(l1 < 64, flat[2 * c : 2 * c + 1], flat[2 * c + 1 : 2 * c + 2])
        hot_out[:, c * LANES : (c + 1) * LANES] = jnp.where(sub == row, 1.0, 0.0).astype(BF16)


def dual_tables(parts, y, rhs, kind, put, take):
    y[...] = join([p[0:NB] for p in parts], 0)
    rhs[...] = join([p[0:NB] for p in parts], 1)
    kind[...] = join([p[NB : 2 * NB] for p in parts], 0)
    mine = jnp.broadcast_to(parts[0][2 * NB :, 0:1], (8, LANES)).astype(I32)
    rel = []
    for p in parts:
        r = p[2 * NB :].astype(I32)
        rel.append((((r >> 3) ^ mine) << 3) | (r & 7))
    ln = lane(LANES)
    sub = iota((LANES, LANES), 0)
    sub_ok = (slot_of(sub) >= NQ) & (slot_of(sub) < NT)
    for p in range(4):
        r = jnp.transpose(jnp.broadcast_to(rel[p][:1].astype(F32), (LANES, LANES))).astype(I32)
        same = ((ln & 64) == (sub & 64)) & ((ln & 3) == (sub & 3)) & sub_ok
        for kk in range(2):
            tile = (2 * kk + ((ln >> 5) & 1)) * 8 + ((ln >> 2) & 7)
            hit = same & (tile == r)
            put[p * LANES : (p + 1) * LANES, kk * LANES : (kk + 1) * LANES] = jnp.where(hit, 1.0, 0.0).astype(BF16)
    r = jnp.broadcast_to(rel[0][:1], (LANES, LANES))
    lane_ok = (slot_of(ln) >= NQ) & (slot_of(ln) < NT)
    for kk in range(2):
        tile = (2 * kk + ((sub >> 5) & 1)) * 8 + ((sub >> 2) & 7)
        hit = ((ln & 64) == (sub & 64)) & ((ln & 3) == (sub & 3)) & lane_ok & (tile == r)
        take[kk * LANES : (kk + 1) * LANES, :] = jnp.where(hit, 1.0, 0.0).astype(BF16)


def take_rows(y, take):
    a, b = split(y, 2)
    return dot(a, take) + dot(b, take)


def first_products_kernel(msg, got, p0, p1, p2, p3, hess, cons, y, rhs, kind, put, take, rows_out, hot_out, out, rows):
    primal_tables(got, rows_out, hot_out)
    dual_tables([p0, p1, p2, p3], y, rhs, kind, put, take)
    rows[...] = spread(msg[...])
    first = forward_tiles(hess, rows, NQ, 0)
    rows[...] = jnp.zeros((NB, LANES), F32)
    transposed_tiles(cons, take_rows(y[...], take[...]), rows, NQ)
    out[...] = with_extra(first - spread(rows[...]), 0.0)


def primal_step(msg, rows, hot, got, x, weight):
    c = got[pl.ds(1, NB, stride=5), :]
    low = got[pl.ds(2, NB, stride=5), :]
    high = got[pl.ds(3, NB, stride=5), :]
    grad = scatter_tiles(msg, rows, hot) + c
    new = jnp.minimum(jnp.maximum(x - (STEP_SCALE / weight) * grad, low), high)
    moved = new - x
    return new, total(moved * moved)


def first_primal_kernel(msg, got, rows, hot, x_out, out):
    x = got[pl.ds(0, NB, stride=5), :]
    new, moved = primal_step(msg[...], rows[...], hot[...], got, x, jnp.ones((1, 1), F32))
    x_out[...] = new
    ids = got[pl.ds(4, NB, stride=5), :].astype(I32)
    out[...] = with_extra(gather_tiles(ids, [new, 2.0 * new - x], [0] * NQ + [1] * NK), moved)


def second_primal_kernel(msg, got, rows, hot, x_in, primal_sq, weight_out, out):
    x = x_in[...]
    m = msg[...]
    weight = new_weight(jnp.ones((1, 1), F32), extra_of(m), primal_sq[0:1, 0:1])
    weight_out[...] = jnp.broadcast_to(weight, (8, LANES))
    new, moved = primal_step(m, rows[...], hot[...], got, x, weight)
    ids = got[pl.ds(4, NB, stride=5), :].astype(I32)
    out[pl.ds(0, NB, stride=2), :] = with_extra(gather_tiles(ids, [2.0 * new - x], [-1] * NQ + [0] * NK), moved)
    out[pl.ds(1, NB, stride=2), :] = new


def constraint_kernel(msg, tiles, out, vec, rows):
    m = msg[...]
    rows[...] = spread(m)
    vec[...] = rows[...]
    out[...] = with_extra(forward_tiles(tiles, rows, NK, NQ), extra_of(m))


def last_constraint_kernel(msg, tiles, out, rows):
    m = msg[pl.ds(0, NB, stride=2), :]
    rows[...] = spread(m)
    out[...] = with_extra(forward_tiles(tiles, rows, NK, NQ), extra_of(m))


def hessian_kernel(vec, tiles, out):
    out[...] = forward_tiles(tiles, vec, NQ, 0)


def primal_total(parts):
    s = parts[0][0:1, EXTRA : EXTRA + 1]
    for p in parts[1:]:
        s = s + p[0:1, EXTRA : EXTRA + 1]
    return s


def dual_kernel(p0, p1, p2, p3, put, take, y, rhs, kind, hess, tiles, y_out, primal_sq, out, rows):
    parts = [p[...] for p in (p0, p1, p2, p3)]
    new, moved = dual_step(parts, put[...], y[...], rhs[...], kind[...], STEP_SCALE)
    y_out[...] = new
    primal_sq[...] = jnp.broadcast_to(primal_total(parts), (8, LANES))
    rows[...] = jnp.zeros((NB, LANES), F32)
    transposed_tiles(tiles, take_rows(new, take[...]), rows, NQ)
    out[...] = with_extra(hess[...] - spread(rows[...]), moved)


def last_dual_kernel(p0, p1, p2, p3, put, y, rhs, kind, weight, y_out, primal_sq, out):
    parts = [p[...] for p in (p0, p1, p2, p3)]
    new, moved = dual_step(parts, put[...], y[...], rhs[...], kind[...], STEP_SCALE * weight[0:1, 0:1])
    primal_sq[...] = jnp.broadcast_to(primal_total(parts), (8, LANES))
    y_out[...] = new[:, :LANES]
    out[...] = jnp.broadcast_to(moved, (NB, LANES))


def last_kernel(msg, y, want, weight, primal_sq, out, dual_out, final):
    dual_sq = jnp.sum(msg[:, 0:1], axis=0, keepdims=True)
    out[...] = new_weight(weight[0:1, 0:1], dual_sq, primal_sq[0:1, 0:1])
    dual_out[...] = spread(y[...])[:32]
    final[...] = spread(want[pl.ds(1, NB, stride=2), :])


def call(kernel, outs, *args, smem=0, scratch=(), cost=COST, where=pltpu.VMEM, limit=VMEM_LIMIT):
    v = pl.BlockSpec(memory_space=pltpu.VMEM)
    w = pl.BlockSpec(memory_space=where)
    s = pl.BlockSpec(memory_space=pltpu.SMEM)
    shapes = [jax.ShapeDtypeStruct(*o) for o in outs]
    res = pl.pallas_call(
        kernel,
        out_shape=shapes,
        in_specs=[s] * smem + [w] * (len(args) - smem),
        out_specs=[v] * len(shapes),
        scratch_shapes=list(scratch),
        compiler_params=pltpu.CompilerParams(vmem_limit_bytes=limit),
        cost_estimate=pl.CostEstimate(flops=cost, bytes_accessed=10000000, transcendentals=0),
    )(*args)
    return res[0] if len(outs) == 1 else res


ROWS = ((NB, LANES), F32)
ROWS_SCRATCH = (pltpu.VMEM((NB, LANES), F32),)


def exchange(rows):
    k = rows.shape[0] // NB
    out = lax.all_to_all(rows.reshape(NB, 1, k * LANES), BLK, 0, 0, tiled=True)
    return out.reshape(NB * k, LANES)


def over_group(rows):
    parts = [rows]
    for k in (1, 2, 3):
        parts.append(lax.ppermute(rows, GRP, [(i, i ^ k) for i in range(4)]))
    return parts


def steps(primal, dual, objective, lower, upper, bound_kind, rhs, row_kind, q_tiles, q_index, k_tiles, k_rows, k_cols):
    hess, cons = q_tiles, k_tiles
    me = lax.axis_index(GRP).astype(I32).reshape(1)

    def wide(v):
        return v.reshape(-1, LANES)

    inputs = (q_index[0], k_cols, k_rows, wide(primal), wide(objective), wide(lower), wide(upper), wide(bound_kind), wide(dual),
              wide(rhs), wide(row_kind))
    room = [(pltpu.SMEM if i < 3 else pltpu.VMEM)(v.shape, v.dtype) for i, v in enumerate(inputs)]
    first, block = call(start_kernel, [((5 * NB, LANES), F32), ((2 * NB + 8, LANES), F32)], me, *inputs, smem=1, where=pltpu.HBM,
                        scratch=room + [pltpu.SemaphoreType.DMA((len(inputs),))], limit=66800000)
    parts = over_group(block)
    got = exchange(first)
    msg = call(first_gather_kernel, [ROWS], got)
    want = exchange(msg)
    wide_block = ((NB, 2 * LANES), F32)
    scalar = ((8, LANES), F32)
    y, b, kind, put, take, rows, hot, msg = call(
        first_products_kernel,
        [wide_block, wide_block, wide_block, ((4 * LANES, 2 * LANES), BF16), ((2 * LANES, LANES), BF16), ((NB, LANES), I32),
         ((NB, NT * NB), BF16), ROWS],
        want, got, *parts, hess, cons, scratch=ROWS_SCRATCH)
    grads = exchange(msg)
    x, msg = call(first_primal_kernel, [ROWS, ROWS], grads, got, rows, hot)
    want = exchange(msg)
    prods, vec = call(constraint_kernel, [ROWS, ROWS], want, cons, scratch=ROWS_SCRATCH)
    parts = over_group(prods)
    hess_prod = call(hessian_kernel, [ROWS], vec, hess, cost=10000000)
    y, primal_sq, msg = call(dual_kernel, [wide_block, scalar, ROWS], *parts, put, take, y, b, kind, hess_prod, cons,
                             scratch=ROWS_SCRATCH)
    grads = exchange(msg)
    weight, both = call(second_primal_kernel, [scalar, ((2 * NB, LANES), F32)], grads, got, rows, hot, x, primal_sq)
    want = exchange(both)
    prods = call(last_constraint_kernel, [ROWS], want, cons, scratch=ROWS_SCRATCH)
    parts = over_group(prods)
    y, primal_sq, msg = call(last_dual_kernel, [ROWS, scalar, ROWS], *parts, put, y, b, kind, weight)
    weight, dual_out, final = call(last_kernel, [((1, 1), F32), ((32, LANES), F32), ROWS], exchange(msg), y, want, weight, primal_sq)
    return final.reshape(-1), dual_out.reshape(-1), weight.reshape(())


def solution(mesh):
    finer = Mesh(mesh.devices.reshape(2, 2, 8, 4, 2), ("grp_0", "grp_1", "blk_0", "blk_1", "blk_2"))
    placed = (P(BLK_GRP),) * 8 + (
        P(GRP, BLK, None, None),
        P(GRP, None, BLK),
        P(GRP, BLK, None, None),
        P(GRP, BLK),
        P(GRP, BLK),
    )
    return jax.shard_map(steps, mesh=finer, in_specs=placed, out_specs=(P(BLK_GRP), P(BLK_GRP), P()), check_vma=False)
```

```python
import jax
import jax.numpy as jnp
from jax import lax
from jax.experimental import pallas as pl
from jax.experimental.pallas import tpu as pltpu
from jax.sharding import Mesh
from jax.sharding import PartitionSpec as P

BLK = ("blk_0", "blk_1", "blk_2")
GRP = ("grp_0", "grp_1")
BLK_GRP = ("blk_0", "blk_1", "blk_2", "grp_0", "grp_1")
EPSILON = 1e-06
STEP_SCALE = 0.5
F32, BF16, I32 = jnp.float32, jnp.bfloat16, jnp.int32

NB = 64
LANES = 128
NQ, NK = 4, 6
NT = NQ + NK
EXTRA = 60
VMEM_LIMIT = 8 * 1024 * 1024
COST = 10000000000


def iota(shape, dim):
    return lax.broadcasted_iota(I32, shape, dim)


def lane(rows=NB):
    return iota((rows, LANES), 1)


def slot_of(lanes):
    return (lanes >> 2) & 15


def split(v, n):
    parts = []
    for _ in range(n - 1):
        p = v.astype(BF16)
        parts.append(p)
        v = v - p.astype(F32)
    parts.append(v.astype(BF16))
    return parts


def dot(a, b):
    return jnp.dot(a, b, preferred_element_type=F32)


def spread(v):
    return jnp.transpose(jnp.concatenate([v, pltpu.roll(v, 64, 1)], axis=0))[:NB]


def total(v):
    return jnp.sum(jnp.sum(v, axis=0, keepdims=True), axis=1, keepdims=True)


def extra_of(msg):
    return total(jnp.where(lane() == EXTRA, msg, 0.0))


def with_extra(msg, value):
    return jnp.where(lane() == EXTRA, value, msg)


def along(v, idx):
    return jnp.take_along_axis(v, idx, axis=1)


def column(v, c):
    return jnp.broadcast_to(v[:, c : c + 1], v.shape)


def gather_tiles(ids, tables, picks):
    ln = lane()
    t_of = along(ids & 15, slot_of(ln))
    idx = (ln & 64) + t_of * 4 + (ln & 3)
    owner = ids >> 4
    msg = jnp.zeros((NB, LANES), F32)
    for which, table in enumerate(tables):
        slots = [j for j in range(NT) if picks[j] == which]
        if not slots:
            continue
        a, b, c = split(table, 3)
        right = jnp.concatenate([a, b, c, jnp.zeros_like(a)], axis=0)
        ones = []
        for j in slots:
            o = jnp.where((ln & 63) == column(owner, j), 1.0, 0.0).astype(BF16)
            ones.append(jnp.concatenate([o, o], axis=1))
        got = dot(jnp.concatenate(ones, axis=0), right)
        for n, j in enumerate(slots):
            msg = jnp.where(slot_of(ln) == j, along(got[n * NB : (n + 1) * NB], idx), msg)
    return msg


def scatter_tiles(msg, rows, hot):
    ln = lane()
    t_of = rows & 15
    high, low = [], []
    for j in range(NT):
        e = along(msg, (ln & 64) + j * 4 + (ln & 3))
        e = jnp.where(slot_of(ln) == column(t_of, j), e, 0.0)
        a, b = split(e, 2)
        high.append(a)
        low.append(b)
    return dot(hot, jnp.concatenate(high, axis=0)) + dot(hot, jnp.concatenate(low, axis=0))


def forward_tiles(tiles_ref, rows_ref, count, first):
    ln = lane()
    out = jnp.zeros((NB, LANES), F32)
    for t in range(count):
        j = first + t
        vec = [rows_ref[4 * j + q : 4 * j + q + 1, :] for q in range(4)]
        for qo in range(4):
            for h in range(2):
                at = slice(qo * 128 + h * 64, qo * 128 + h * 64 + 64)
                p = tiles_ref[0, t, at, 0:128] * vec[0]
                for q in range(1, 4):
                    p = p + tiles_ref[0, t, at, q * 128 : (q + 1) * 128] * vec[q]
                out = jnp.where(ln == h * 64 + 4 * j + qo, jnp.sum(p, axis=1, keepdims=True), out)
    return out


def transposed_tiles(tiles_ref, cols, rows_ref, first):
    for t in range(NK):
        j = first + t
        acc = [jnp.zeros((8, LANES), F32) for _ in range(4)]
        for qo in range(4):
            for h in range(2):
                at = slice(qo * 128 + h * 64, qo * 128 + h * 64 + 64)
                v = along(cols, jnp.full((NB, LANES), h * 64 + 4 * j + qo, I32))
                for q in range(4):
                    p = tiles_ref[0, t, at, q * 128 : (q + 1) * 128] * v
                    acc[q] = acc[q] + jnp.sum(p.reshape(8, 8, LANES), axis=0)
        for q in range(4):
            rows_ref[4 * j + q : 4 * j + q + 1, :] = jnp.sum(acc[q], axis=0, keepdims=True)


def join(parts, part):
    low = (lane() & 32) == 0
    blocks = []
    for k in (0, 2):
        a, b = parts[k], parts[k + 1]
        if part == 0:
            blocks.append(jnp.where(low, a, pltpu.roll(b, 32, 1)))
        else:
            blocks.append(jnp.where(low, pltpu.roll(a, LANES - 32, 1), b))
    return jnp.concatenate(blocks, axis=1)


def pack(prods, extra):
    ln = lane(32)
    both = jnp.where((ln & 63) < 40, prods[:32], pltpu.roll(prods[32:], 24, 1))
    return jnp.where(ln == 0, extra, both)


def unpack(packed):
    return jnp.concatenate([packed, pltpu.roll(packed, LANES - 24, 1)], axis=0)


def dual_step(parts, hot, y, rhs, kind, step):
    high, low = [], []
    for p in parts:
        a, b = split(unpack(p), 2)
        high.append(a)
        low.append(b)
    extrap = dot(jnp.concatenate(high, axis=1), hot) + dot(jnp.concatenate(low, axis=1), hot)
    new = y + step * (rhs - extrap)
    new = jnp.where(kind == 1.0, jnp.maximum(new, 0.0), new)
    moved = new - y
    return new, total(moved * moved)


def new_weight(weight, dual_sq, primal_sq):
    return jnp.sqrt(weight * jnp.sqrt((dual_sq + EPSILON) / (primal_sq + EPSILON)))


def spread_two(v, w):
    t = jnp.transpose(jnp.concatenate([v, w], axis=0))
    low = lane() < 64
    top, bottom = t[:NB], t[NB:]
    return jnp.where(low, top, pltpu.roll(bottom, 64, 1)), jnp.where(low, pltpu.roll(top, 64, 1), bottom)


def start_kernel(me, q_index, k_cols, k_rows, primal, objective, lower, upper, bound_kind, dual, rhs, row_kind, out, block, *scratch):
    refs = (q_index, k_cols, k_rows, primal, objective, lower, upper, bound_kind, dual, rhs, row_kind)
    sems = scratch[-1]
    copies = [pltpu.make_async_copy(r, s, sems.at[i]) for i, (r, s) in enumerate(zip(refs, scratch))]
    for c in copies:
        c.start()
    qi, kc, kr, p, ob, lo, up, bk, du, rh, rk = scratch[:-1]
    for c in copies:
        c.wait()
    kind = bk[...]
    low = jnp.where((kind == 1) | (kind == 2), lo[...], -jnp.inf)
    high = jnp.where((kind == 2) | (kind == 3), up[...], jnp.inf)
    a, b = spread_two(p[...], ob[...])
    c, d = spread_two(low, high)
    for k, v in enumerate((a, b, c, d)):
        out[pl.ds(k, NB, stride=5), :] = v
    ln = lane(8)
    ids = jnp.zeros((8, LANES), F32)
    for j in range(NQ):
        ids = jnp.where(ln == j, qi[1, j].astype(F32), ids)
        ids = jnp.where(ln == NT + j, qi[0, j].astype(F32), ids)
    for j in range(NK):
        ids = jnp.where(ln == NQ + j, kc[0, j].astype(F32), ids)
    out[pl.ds(4, NB, stride=5), :] = jnp.broadcast_to(ids[:1], (NB, LANES))
    a, b = spread_two(
        jnp.concatenate([du[...], rh[...]], axis=0),
        jnp.concatenate([rk[...].astype(F32), jnp.zeros((32, LANES), F32)], axis=0),
    )
    block[0:NB] = a
    block[NB : 2 * NB] = b
    ids = jnp.zeros((8, LANES), F32)
    for j in range(NK):
        ids = jnp.where(slot_of(ln) == NQ + j, kr[0, j].astype(F32), ids)
    block[2 * NB :] = jnp.where(ln == 0, me[0].astype(F32), ids)


def first_gather_kernel(got, msg):
    ids = got[pl.ds(4, NB, stride=5), :].astype(I32)
    x = got[pl.ds(0, NB, stride=5), :]
    msg[...] = gather_tiles(ids, [x], [0] * NQ + [-1] * NK)


def primal_tables(got, rows_out, hot_out):
    ids = got[pl.ds(4, NB, stride=5), :].astype(I32)
    ln = lane()
    rows = jnp.where(ln < NQ, pltpu.roll(ids, LANES - NT, 1), ids)
    rows_out[...] = rows
    owner = (rows >> 4).astype(F32)
    flat = jnp.transpose(jnp.concatenate([owner, owner], axis=0))
    sub = iota((NB, LANES), 0).astype(F32)
    l1 = lane(1)
    for c in range(NT // 2):
        row = jnp.where(l1 < 64, flat[2 * c : 2 * c + 1], flat[2 * c + 1 : 2 * c + 2])
        hot_out[:, c * LANES : (c + 1) * LANES] = jnp.where(sub == row, 1.0, 0.0).astype(BF16)


def dual_tables(parts, y, rhs, kind, tiles, take):
    y[...] = join([p[0:NB] for p in parts], 0)
    rhs[...] = join([p[0:NB] for p in parts], 1)
    kind[...] = join([p[NB : 2 * NB] for p in parts], 0)
    mine = jnp.broadcast_to(parts[0][2 * NB :, 0:1], (8, LANES)).astype(I32)
    rel = []
    for p in parts:
        r = p[2 * NB :].astype(I32)
        rel.append((((r >> 3) ^ mine) << 3) | (r & 7))
    tiles[...] = jnp.concatenate(rel, axis=0)
    ln = lane(LANES)
    sub = iota((LANES, LANES), 0)
    r = jnp.broadcast_to(rel[0][:1], (LANES, LANES))
    lane_ok = (slot_of(ln) >= NQ) & (slot_of(ln) < NT)
    for kk in range(2):
        tile = (2 * kk + ((sub >> 5) & 1)) * 8 + ((sub >> 2) & 7)
        hit = ((ln & 64) == (sub & 64)) & ((ln & 3) == (sub & 3)) & lane_ok & (tile == r)
        take[kk * LANES : (kk + 1) * LANES, :] = jnp.where(hit, 1.0, 0.0).astype(BF16)


def put_table(tiles, put):
    ln = lane(LANES)
    sub = iota((LANES, LANES), 0)
    same = ((ln & 64) == (sub & 64)) & ((ln & 3) == (sub & 3)) & (slot_of(sub) >= NQ) & (slot_of(sub) < NT)
    for p in range(4):
        r = jnp.transpose(jnp.broadcast_to(tiles[8 * p : 8 * p + 1].astype(F32), (LANES, LANES))).astype(I32)
        for kk in range(2):
            tile = (2 * kk + ((ln >> 5) & 1)) * 8 + ((ln >> 2) & 7)
            put[p * LANES : (p + 1) * LANES, kk * LANES : (kk + 1) * LANES] = jnp.where(same & (tile == r), 1.0, 0.0).astype(BF16)


def take_rows(y, take):
    a, b = split(y, 2)
    return dot(a, take) + dot(b, take)


def first_products_kernel(msg, got, p0, p1, p2, p3, hess, cons, y, rhs, kind, tiles, take, rows_out, hot_out, out, rows):
    primal_tables(got, rows_out, hot_out)
    dual_tables([p0, p1, p2, p3], y, rhs, kind, tiles, take)
    rows[...] = spread(msg[...])
    first = forward_tiles(hess, rows, NQ, 0)
    rows[...] = jnp.zeros((NB, LANES), F32)
    transposed_tiles(cons, take_rows(y[...], take[...]), rows, NQ)
    out[...] = with_extra(first - spread(rows[...]), 0.0)


def primal_step(msg, rows, hot, got, x, weight):
    c = got[pl.ds(1, NB, stride=5), :]
    low = got[pl.ds(2, NB, stride=5), :]
    high = got[pl.ds(3, NB, stride=5), :]
    grad = scatter_tiles(msg, rows, hot) + c
    new = jnp.minimum(jnp.maximum(x - (STEP_SCALE / weight) * grad, low), high)
    moved = new - x
    return new, total(moved * moved)


def first_primal_kernel(msg, got, rows, hot, x_out, out):
    x = got[pl.ds(0, NB, stride=5), :]
    new, moved = primal_step(msg[...], rows[...], hot[...], got, x, jnp.ones((1, 1), F32))
    x_out[...] = new
    ids = got[pl.ds(4, NB, stride=5), :].astype(I32)
    out[...] = with_extra(gather_tiles(ids, [new, 2.0 * new - x], [0] * NQ + [1] * NK), moved)


def second_primal_kernel(msg, got, rows, hot, x_in, primal_sq, weight_out, out):
    x = x_in[...]
    m = msg[...]
    weight = new_weight(jnp.ones((1, 1), F32), extra_of(m), primal_sq[0:1, 0:1])
    weight_out[...] = jnp.broadcast_to(weight, (8, LANES))
    new, moved = primal_step(m, rows[...], hot[...], got, x, weight)
    ids = got[pl.ds(4, NB, stride=5), :].astype(I32)
    out[pl.ds(0, NB, stride=2), :] = with_extra(gather_tiles(ids, [2.0 * new - x], [-1] * NQ + [0] * NK), moved)
    out[pl.ds(1, NB, stride=2), :] = new


def constraint_kernel(msg, tiles, out, vec, rows):
    m = msg[...]
    rows[...] = spread(m)
    vec[...] = rows[...]
    out[...] = pack(forward_tiles(tiles, rows, NK, NQ), extra_of(m))


def last_constraint_kernel(msg, tiles, out, rows):
    m = msg[pl.ds(0, NB, stride=2), :]
    rows[...] = spread(m)
    out[...] = pack(forward_tiles(tiles, rows, NK, NQ), extra_of(m))


def hessian_kernel(vec, rel, tiles, out, put):
    out[...] = forward_tiles(tiles, vec, NQ, 0)
    put_table(rel, put)


def primal_total(parts):
    s = parts[0][0:1, 0:1]
    for p in parts[1:]:
        s = s + p[0:1, 0:1]
    return s


def dual_kernel(p0, p1, p2, p3, put, take, y, rhs, kind, hess, tiles, y_out, primal_sq, out, rows):
    parts = [p[...] for p in (p0, p1, p2, p3)]
    new, moved = dual_step(parts, put[...], y[...], rhs[...], kind[...], STEP_SCALE)
    y_out[...] = new
    primal_sq[...] = jnp.broadcast_to(primal_total(parts), (8, LANES))
    rows[...] = jnp.zeros((NB, LANES), F32)
    transposed_tiles(tiles, take_rows(new, take[...]), rows, NQ)
    out[...] = with_extra(hess[...] - spread(rows[...]), moved)


def last_dual_kernel(p0, p1, p2, p3, put, y, rhs, kind, weight, y_out, primal_sq, out):
    parts = [p[...] for p in (p0, p1, p2, p3)]
    new, moved = dual_step(parts, put[...], y[...], rhs[...], kind[...], STEP_SCALE * weight[0:1, 0:1])
    primal_sq[...] = jnp.broadcast_to(primal_total(parts), (8, LANES))
    y_out[...] = new[:, :LANES]
    out[...] = jnp.broadcast_to(moved, (NB, LANES))


def last_kernel(msg, y, want, weight, primal_sq, out, dual_out, final):
    dual_sq = jnp.sum(msg[:, 0:1], axis=0, keepdims=True)
    out[...] = new_weight(weight[0:1, 0:1], dual_sq, primal_sq[0:1, 0:1])
    dual_out[...] = spread(y[...])[:32]
    final[...] = spread(want[pl.ds(1, NB, stride=2), :])


def call(kernel, outs, *args, smem=0, scratch=(), cost=COST, where=pltpu.VMEM, limit=VMEM_LIMIT):
    v = pl.BlockSpec(memory_space=pltpu.VMEM)
    w = pl.BlockSpec(memory_space=where)
    s = pl.BlockSpec(memory_space=pltpu.SMEM)
    shapes = [jax.ShapeDtypeStruct(*o) for o in outs]
    res = pl.pallas_call(
        kernel,
        out_shape=shapes,
        in_specs=[s] * smem + [w] * (len(args) - smem),
        out_specs=[v] * len(shapes),
        scratch_shapes=list(scratch),
        compiler_params=pltpu.CompilerParams(vmem_limit_bytes=limit),
        cost_estimate=pl.CostEstimate(flops=cost, bytes_accessed=10000000, transcendentals=0),
    )(*args)
    return res[0] if len(outs) == 1 else res


ROWS = ((NB, LANES), F32)
PACKED = ((NB // 2, LANES), F32)
ROWS_SCRATCH = (pltpu.VMEM((NB, LANES), F32),)


def exchange(rows):
    k = rows.shape[0] // NB
    out = lax.all_to_all(rows.reshape(NB, 1, k * LANES), BLK, 0, 0, tiled=True)
    return out.reshape(NB * k, LANES)


def over_group(rows):
    parts = [rows]
    for k in (1, 2, 3):
        parts.append(lax.ppermute(rows, GRP, [(i, i ^ k) for i in range(4)]))
    return parts


def steps(primal, dual, objective, lower, upper, bound_kind, rhs, row_kind, q_tiles, q_index, k_tiles, k_rows, k_cols):
    hess, cons = q_tiles, k_tiles
    me = lax.axis_index(GRP).astype(I32).reshape(1)

    def wide(v):
        return v.reshape(-1, LANES)

    inputs = (q_index[0], k_cols, k_rows, wide(primal), wide(objective), wide(lower), wide(upper), wide(bound_kind), wide(dual),
              wide(rhs), wide(row_kind))
    room = [(pltpu.SMEM if i < 3 else pltpu.VMEM)(v.shape, v.dtype) for i, v in enumerate(inputs)]
    first, block = call(start_kernel, [((5 * NB, LANES), F32), ((2 * NB + 8, LANES), F32)], me, *inputs, smem=1, where=pltpu.HBM,
                        scratch=room + [pltpu.SemaphoreType.DMA((len(inputs),))], limit=66800000)
    parts = over_group(block)
    got = exchange(first)
    msg = call(first_gather_kernel, [ROWS], got)
    want = exchange(msg)
    wide_block = ((NB, 2 * LANES), F32)
    scalar = ((8, LANES), F32)
    y, b, kind, rel, take, rows, hot, msg = call(
        first_products_kernel,
        [wide_block, wide_block, wide_block, ((32, LANES), I32), ((2 * LANES, LANES), BF16), ((NB, LANES), I32),
         ((NB, NT * NB), BF16), ROWS],
        want, got, *parts, hess, cons, scratch=ROWS_SCRATCH)
    grads = exchange(msg)
    x, msg = call(first_primal_kernel, [ROWS, ROWS], grads, got, rows, hot)
    want = exchange(msg)
    prods, vec = call(constraint_kernel, [PACKED, ROWS], want, cons, scratch=ROWS_SCRATCH)
    parts = over_group(prods)
    hess_prod, put = call(hessian_kernel, [ROWS, ((4 * LANES, 2 * LANES), BF16)], vec, rel, hess)
    y, primal_sq, msg = call(dual_kernel, [wide_block, scalar, ROWS], *parts, put, take, y, b, kind, hess_prod, cons,
                             scratch=ROWS_SCRATCH)
    grads = exchange(msg)
    weight, both = call(second_primal_kernel, [scalar, ((2 * NB, LANES), F32)], grads, got, rows, hot, x, primal_sq)
    want = exchange(both)
    prods = call(last_constraint_kernel, [PACKED], want, cons, scratch=ROWS_SCRATCH)
    parts = over_group(prods)
    y, primal_sq, msg = call(last_dual_kernel, [ROWS, scalar, ROWS], *parts, put, y, b, kind, weight)
    weight, dual_out, final = call(last_kernel, [((1, 1), F32), ((32, LANES), F32), ROWS], exchange(msg), y, want, weight, primal_sq)
    return final.reshape(-1), dual_out.reshape(-1), weight.reshape(())


def solution(mesh):
    finer = Mesh(mesh.devices.reshape(2, 2, 8, 4, 2), ("grp_0", "grp_1", "blk_0", "blk_1", "blk_2"))
    placed = (P(BLK_GRP),) * 8 + (
        P(GRP, BLK, None, None),
        P(GRP, None, BLK),
        P(GRP, BLK, None, None),
        P(GRP, BLK),
        P(GRP, BLK),
    )
    return jax.shard_map(steps, mesh=finer, in_specs=placed, out_specs=(P(BLK_GRP), P(BLK_GRP), P()), check_vma=False)
```

```python
import jax
import jax.numpy as jnp
from jax import lax
from jax.experimental import pallas as pl
from jax.experimental.pallas import tpu as pltpu
from jax.sharding import Mesh
from jax.sharding import PartitionSpec as P

BLK = ("zh", "zl", "xh", "xl", "yl")
CUBE = ("zl", "xl", "yl")
GRP = ("grp_0", "grp_1")
BLK_GRP = (*BLK, *GRP)
EPSILON = 1e-06
STEP_SCALE = 0.5
F32, BF16, I32 = jnp.float32, jnp.bfloat16, jnp.int32

NB = 64
LANES = 128
NQ, NK = 4, 6
NT = NQ + NK
VMEM_LIMIT = 8 * 1024 * 1024
COST = 10000000000


def iota(shape, dim):
    return lax.broadcasted_iota(I32, shape, dim)


def lane(rows=NB):
    return iota((rows, LANES), 1)


def slot_of(lanes):
    return (lanes >> 2) & 15


def split(v, n):
    parts = []
    for _ in range(n - 1):
        p = v.astype(BF16)
        parts.append(p)
        v = v - p.astype(F32)
    parts.append(v.astype(BF16))
    return parts


def dot(a, b):
    return jnp.dot(a, b, preferred_element_type=F32)


def spread(v):
    return jnp.transpose(jnp.concatenate([v, pltpu.roll(v, 64, 1)], axis=0))[:NB]


def total(v):
    return jnp.sum(jnp.sum(v, axis=0, keepdims=True), axis=1, keepdims=True)


def along(v, idx):
    return jnp.take_along_axis(v, idx, axis=1)


def column(v, c):
    return jnp.broadcast_to(v[:, c : c + 1], v.shape)


def gather_tiles(ids, tables, out, k):
    ln = lane()
    t_of = along(ids & 15, slot_of(ln))
    idx = (ln & 64) + t_of * 4 + (ln & 3)
    owner = ids >> 4
    ones = []
    for j in range(NT):
        o = jnp.where((ln & 63) == column(owner, j), 1.0, 0.0).astype(BF16)
        ones.append(jnp.concatenate([o, o], axis=1))
    ones = jnp.concatenate(ones, axis=0)
    for n, table in enumerate(tables):
        a, b, c = split(table, 3)
        got = dot(ones, jnp.concatenate([a, b, c, jnp.zeros_like(a)], axis=0))
        msg = jnp.zeros((NB, LANES), F32)
        for j in range(NT):
            msg = jnp.where(slot_of(ln) == j, along(got[j * NB : (j + 1) * NB], idx), msg)
        out[pl.ds(n, NB, stride=k), :] = msg


def cube_of(b):
    return ((b >> 3) & 1) * 4 + ((b >> 1) & 1) * 2 + (b & 1)


def send_rows(rows_ref, out, k):
    low = lane(5) < 64
    for q in range(4):
        a = rows_ref[pl.ds(q, 5, stride=8), :]
        b = rows_ref[pl.ds(q + 4, 5, stride=8), :]
        halves = (jnp.where(low, a, pltpu.roll(b, 64, 1)), jnp.where(low, pltpu.roll(a, 64, 1), b))
        for peer in range(NB):
            if cube_of(peer) >> 1 == q:
                out[peer * k : peer * k + 5, :] = halves[cube_of(peer) & 1]


def match_table(got, hot):
    base = lax.axis_index("zh") * 16 + lax.axis_index("xh") * 4
    ids = got[pl.ds(5, NB, stride=6), :]
    flat = jnp.transpose(jnp.concatenate([ids, ids], axis=0))
    l8 = lane(8)
    sub = iota((8, LANES), 0)
    member = base + ((sub >> 2) & 1) * 8 + ((sub >> 1) & 1) * 2 + (sub & 1)
    want = jnp.zeros((8, LANES), F32)
    for p in range(8):
        b = base + (p >> 2) * 8 + ((p >> 1) & 1) * 2 + (p & 1)
        want = jnp.where(sub == p, jnp.broadcast_to(got[pl.ds(b * 6 + 5, 1), :], (8, LANES)), want)
    want = jnp.where(l8 < NT, want, (member * 16 + l8 - NT).astype(F32))
    l1 = lane(1)

    def slot_row(j):
        r = NT + j if j < NQ else j
        return flat[r : r + 1]

    for parity in range(2):
        for c in range(NT // 2):
            pair = []
            for u in (2 * c, 2 * c + 1):
                part, k = u // 5, u % 5
                pair.append(slot_row(2 * k + (part ^ parity)))
            row = jnp.where(l1 < 64, pair[0], pair[1])
            hits = []
            for kk in range(13):
                w = jnp.broadcast_to(want[:, 2 * kk + parity : 2 * kk + parity + 1], (8, LANES))
                hits.append(jnp.where(w == row, 1.0, 0.0))
            hot[parity * 104 : parity * 104 + 104, c * LANES : (c + 1) * LANES] = jnp.concatenate(hits, axis=0).astype(BF16)


def sum_rows(msg, hot, out, k):
    blocks = [msg[pl.ds(n, NB, stride=k), :] for n in range(5)]
    blocks += [pltpu.roll(v, 64, 1) for v in blocks]
    high, low = [], []
    for v in blocks:
        a, b = split(v, 2)
        high.append(a)
        low.append(b)
    got = dot(hot[...], jnp.concatenate(high, axis=0)) + dot(hot[...], jnp.concatenate(low, axis=0))
    left = lane(8) < 64
    for kk in range(13):
        out[pl.ds(kk, 8, stride=13), :] = jnp.where(left, got[8 * kk : 8 * kk + 8], got[104 + 8 * kk : 112 + 8 * kk])


def receive_rows(msg, rows):
    low = lane(13) < 64
    for q in range(4):
        a = msg[26 * q : 26 * q + 13, :]
        b = msg[26 * q + 13 : 26 * q + 26, :]
        rows[pl.ds(q, 13, stride=8), :] = jnp.where(low, a, pltpu.roll(b, 64, 1))
        rows[pl.ds(q + 4, 13, stride=8), :] = jnp.where(low, pltpu.roll(a, 64, 1), b)


def project(v, low, high, kind):
    v = jnp.where((kind == 1.0) | (kind == 2.0), jnp.maximum(v, low), v)
    return jnp.where((kind == 2.0) | (kind == 3.0), jnp.minimum(v, high), v)


def forward_tiles(tiles_ref, rows_ref, count, first):
    ln = lane()
    out = jnp.zeros((NB, LANES), F32)
    for t in range(count):
        j = first + t
        vec = [rows_ref[4 * j + q : 4 * j + q + 1, :] for q in range(4)]
        for qo in range(4):
            for h in range(2):
                at = slice(qo * 128 + h * 64, qo * 128 + h * 64 + 64)
                p = tiles_ref[0, t, at, 0:128] * vec[0]
                for q in range(1, 4):
                    p = p + tiles_ref[0, t, at, q * 128 : (q + 1) * 128] * vec[q]
                out = jnp.where(ln == h * 64 + 4 * j + qo, jnp.sum(p, axis=1, keepdims=True), out)
    return out


def transposed_tiles(tiles_ref, cols, rows_ref, first):
    for t in range(NK):
        j = first + t
        acc = [jnp.zeros((8, LANES), F32) for _ in range(4)]
        for qo in range(4):
            for h in range(2):
                at = slice(qo * 128 + h * 64, qo * 128 + h * 64 + 64)
                v = along(cols, jnp.full((NB, LANES), h * 64 + 4 * j + qo, I32))
                for q in range(4):
                    p = tiles_ref[0, t, at, q * 128 : (q + 1) * 128] * v
                    acc[q] = acc[q] + jnp.sum(p.reshape(8, 8, LANES), axis=0)
        for q in range(4):
            rows_ref[4 * j + q : 4 * j + q + 1, :] = jnp.sum(acc[q], axis=0, keepdims=True)


def join(parts, part):
    low = (lane() & 32) == 0
    blocks = []
    for k in (0, 2):
        a, b = parts[k], parts[k + 1]
        if part == 0:
            blocks.append(jnp.where(low, a, pltpu.roll(b, 32, 1)))
        else:
            blocks.append(jnp.where(low, pltpu.roll(a, LANES - 32, 1), b))
    return jnp.concatenate(blocks, axis=1)


def pack(prods, extra):
    ln = lane(32)
    both = jnp.where((ln & 63) < 40, prods[:32], pltpu.roll(prods[32:], 24, 1))
    return jnp.where(ln == 0, extra, both)


def unpack(packed):
    return jnp.concatenate([packed, pltpu.roll(packed, LANES - 24, 1)], axis=0)


def dual_step(parts, hot, y, rhs, kind, step):
    high, low = [], []
    for p in parts:
        a, b = split(unpack(p), 2)
        high.append(a)
        low.append(b)
    extrap = dot(jnp.concatenate(high, axis=1), hot) + dot(jnp.concatenate(low, axis=1), hot)
    new = y + step * (rhs - extrap)
    new = jnp.where(kind == 1.0, jnp.maximum(new, 0.0), new)
    moved = new - y
    return new, total(moved * moved)


def new_weight(weight, dual_sq, primal_sq):
    return jnp.sqrt(weight * jnp.sqrt((dual_sq + EPSILON) / (primal_sq + EPSILON)))


def spread_two(v, w):
    t = jnp.transpose(jnp.concatenate([v, w], axis=0))
    low = lane() < 64
    top, bottom = t[:NB], t[NB:]
    return jnp.where(low, top, pltpu.roll(bottom, 64, 1)), jnp.where(low, pltpu.roll(top, 64, 1), bottom)


def start_kernel(me, q_index, k_cols, k_rows, primal, objective, lower, upper, bound_kind, dual, rhs, row_kind, out, block, own, *scratch):
    refs = (q_index, k_cols, k_rows, primal, objective, lower, upper, bound_kind, dual, rhs, row_kind)
    sems = scratch[-1]
    copies = [pltpu.make_async_copy(r, s, sems.at[i]) for i, (r, s) in enumerate(zip(refs, scratch))]
    for c in copies:
        c.start()
    qi, kc, kr, p, ob, lo, up, bk, du, rh, rk = scratch[:-1]
    for c in copies:
        c.wait()
    kind = bk[...].astype(F32)
    a, b = spread_two(p[...], ob[...])
    c, d = spread_two(lo[...], up[...])
    for k, v in enumerate((a, b, c, d, spread(kind))):
        out[pl.ds(k, NB, stride=6), :] = v
    for k, v in enumerate((p[...], ob[...], lo[...], up[...], kind)):
        own[k * NB : (k + 1) * NB] = v
    ln = lane(8)
    ids = jnp.zeros((8, LANES), F32)
    for j in range(NQ):
        ids = jnp.where(ln == j, qi[1, j].astype(F32), ids)
        ids = jnp.where(ln == NT + j, qi[0, j].astype(F32), ids)
    for j in range(NK):
        ids = jnp.where(ln == NQ + j, kc[0, j].astype(F32), ids)
    out[pl.ds(5, NB, stride=6), :] = jnp.broadcast_to(ids[:1], (NB, LANES))
    a, b = spread_two(
        jnp.concatenate([du[...], rh[...]], axis=0),
        jnp.concatenate([rk[...].astype(F32), jnp.zeros((32, LANES), F32)], axis=0),
    )
    block[0:NB] = a
    block[NB : 2 * NB] = b
    ids = jnp.zeros((8, LANES), F32)
    for j in range(NK):
        ids = jnp.where(slot_of(ln) == NQ + j, kr[0, j].astype(F32), ids)
    block[2 * NB :] = jnp.where(ln == 0, me[0].astype(F32), ids)


def first_gather_kernel(got, msg):
    ids = got[pl.ds(5, NB, stride=6), :].astype(I32)
    gather_tiles(ids, [got[pl.ds(n, NB, stride=6), :] for n in range(5)], msg, 5)


def dual_tables(parts, y, rhs, kind, tiles, take):
    y[...] = join([p[0:NB] for p in parts], 0)
    rhs[...] = join([p[0:NB] for p in parts], 1)
    kind[...] = join([p[NB : 2 * NB] for p in parts], 0)
    mine = jnp.broadcast_to(parts[0][2 * NB :, 0:1], (8, LANES)).astype(I32)
    rel = []
    for p in parts:
        r = p[2 * NB :].astype(I32)
        rel.append((((r >> 3) ^ mine) << 3) | (r & 7))
    tiles[...] = jnp.concatenate(rel, axis=0)
    ln = lane(LANES)
    sub = iota((LANES, LANES), 0)
    r = jnp.broadcast_to(rel[0][:1], (LANES, LANES))
    lane_ok = (slot_of(ln) >= NQ) & (slot_of(ln) < NT)
    for kk in range(2):
        tile = (2 * kk + ((sub >> 5) & 1)) * 8 + ((sub >> 2) & 7)
        hit = ((ln & 64) == (sub & 64)) & ((ln & 3) == (sub & 3)) & lane_ok & (tile == r)
        take[kk * LANES : (kk + 1) * LANES, :] = jnp.where(hit, 1.0, 0.0).astype(BF16)


def put_table(tiles, put):
    ln = lane(LANES)
    sub = iota((LANES, LANES), 0)
    same = ((ln & 64) == (sub & 64)) & ((ln & 3) == (sub & 3)) & (slot_of(sub) >= NQ) & (slot_of(sub) < NT)
    for p in range(4):
        r = jnp.transpose(jnp.broadcast_to(tiles[8 * p : 8 * p + 1].astype(F32), (LANES, LANES))).astype(I32)
        for kk in range(2):
            tile = (2 * kk + ((ln >> 5) & 1)) * 8 + ((ln >> 2) & 7)
            put[p * LANES : (p + 1) * LANES, kk * LANES : (kk + 1) * LANES] = jnp.where(same & (tile == r), 1.0, 0.0).astype(BF16)


def take_rows(y, take):
    a, b = split(y, 2)
    return dot(a, take) + dot(b, take)


def first_products_kernel(msg, got, p0, p1, p2, p3, hess, cons, y, rhs, kind, tiles, take, hot, read, out, rows):
    match_table(got, hot)
    dual_tables([p0, p1, p2, p3], y, rhs, kind, tiles, take)
    m = [msg[pl.ds(n, NB, stride=5), :] for n in range(5)]
    v = (*spread_two(m[0], m[1]), *spread_two(m[2], m[3]), spread(m[4]))
    for n in range(5):
        read[n * NB : (n + 1) * NB] = v[n]
    first = spread(forward_tiles(hess, read, NQ, 0))
    transposed_tiles(cons, take_rows(y[...], take[...]), rows, NQ)
    rows[0 : 4 * NQ] = first[0 : 4 * NQ]
    rows[4 * NQ : 4 * NT] = -rows[4 * NQ : 4 * NT]
    send_rows(rows, out, 5)


def first_sum_kernel(msg, hot, out):
    sum_rows(msg, hot, out, 5)


def second_sum_kernel(msg, hot, weight, out):
    sum_rows(msg, hot, out, 6)
    tail = jnp.sum(msg[pl.ds(5, NB, stride=6), :], axis=0, keepdims=True)
    weight[...] = jnp.broadcast_to(new_weight(jnp.ones((1, 1), F32), tail[:, 1:2], tail[:, 0:1]), (8, LANES))


def primal_step(grads, own, read, weight, own_out, read_out, rows):
    receive_rows(grads, rows)
    tau = STEP_SCALE / weight

    def step(v, first, n):
        x, c, low, high, kind = (v[k * NB : k * NB + n] for k in range(5))
        return x, project(x - tau * (rows[first : first + n] + c), low, high, kind)

    x, new = step(own, 4 * NT, NB)
    own_out[...] = new
    moved = new - x
    old, fresh = step(read, 0, 4 * NT)
    read_out[0 : 4 * NT] = fresh
    rows[0 : 4 * NT] = 2.0 * fresh - old
    return total(moved * moved)


def first_primal_kernel(grads, own, read, tiles, own_out, read_out, out, rows):
    moved = primal_step(grads, own, read, jnp.ones((1, 1), F32), own_out, read_out, rows)
    out[...] = pack(forward_tiles(tiles, rows, NK, NQ), moved)


def second_primal_kernel(grads, own, own_x, read, read_x, weight, tiles, own_out, out, rows):
    receive_rows(grads, rows)
    tau = STEP_SCALE / weight[0:1, 0:1]

    def step(x, v, first, n):
        c, low, high, kind = (v[k * NB : k * NB + n] for k in range(1, 5))
        return project(x - tau * (rows[first : first + n] + c), low, high, kind)

    x = own_x[...]
    new = step(x, own, 4 * NT, NB)
    own_out[...] = new
    moved = new - x
    old = read_x[0 : 4 * NT]
    rows[0 : 4 * NT] = 2.0 * step(old, read, 0, 4 * NT) - old
    out[...] = pack(forward_tiles(tiles, rows, NK, NQ), total(moved * moved))


def hessian_kernel(vec, rel, tiles, out, put):
    out[...] = spread(forward_tiles(tiles, vec, NQ, 0))
    put_table(rel, put)


def primal_total(parts):
    s = parts[0][0:1, 0:1]
    for p in parts[1:]:
        s = s + p[0:1, 0:1]
    return s


def dual_kernel(p0, p1, p2, p3, put, take, y, rhs, kind, hess, tiles, y_out, out, rows):
    parts = [p[...] for p in (p0, p1, p2, p3)]
    new, moved = dual_step(parts, put[...], y[...], rhs[...], kind[...], STEP_SCALE)
    y_out[...] = new
    transposed_tiles(tiles, take_rows(new, take[...]), rows, NQ)
    rows[0 : 4 * NQ] = hess[0 : 4 * NQ]
    rows[4 * NQ : 4 * NT] = -rows[4 * NQ : 4 * NT]
    send_rows(rows, out, 6)
    out[pl.ds(5, NB, stride=6), :] = jnp.where(lane() == 0, primal_total(parts), moved)


def last_dual_kernel(p0, p1, p2, p3, put, y, rhs, kind, weight, y_out, out):
    parts = [p[...] for p in (p0, p1, p2, p3)]
    new, moved = dual_step(parts, put[...], y[...], rhs[...], kind[...], STEP_SCALE * weight[0:1, 0:1])
    y_out[...] = new[:, :LANES]
    out[...] = jnp.where(lane() == 0, primal_total(parts), moved)


def last_kernel(msg, y, x, weight, out, dual_out, final):
    tail = jnp.sum(msg[...], axis=0, keepdims=True)
    out[...] = new_weight(weight[0:1, 0:1], tail[:, 1:2], tail[:, 0:1])
    dual_out[...] = spread(y[...])[:32]
    final[...] = x[...]


def call(kernel, outs, *args, smem=0, scratch=(), cost=COST, where=pltpu.VMEM, limit=VMEM_LIMIT):
    v = pl.BlockSpec(memory_space=pltpu.VMEM)
    w = pl.BlockSpec(memory_space=where)
    s = pl.BlockSpec(memory_space=pltpu.SMEM)
    shapes = [jax.ShapeDtypeStruct(*o) for o in outs]
    res = pl.pallas_call(
        kernel,
        out_shape=shapes,
        in_specs=[s] * smem + [w] * (len(args) - smem),
        out_specs=[v] * len(shapes),
        scratch_shapes=list(scratch),
        compiler_params=pltpu.CompilerParams(vmem_limit_bytes=limit),
        cost_estimate=pl.CostEstimate(flops=cost, bytes_accessed=10000000, transcendentals=0),
    )(*args)
    return res[0] if len(outs) == 1 else res


ROWS = ((NB, LANES), F32)
PACKED = ((NB // 2, LANES), F32)
ROWS_SCRATCH = (pltpu.VMEM((NB, LANES), F32),)


def exchange(rows):
    k = rows.shape[0] // NB
    out = lax.all_to_all(rows.reshape(NB, 1, k * LANES), BLK, 0, 0, tiled=True)
    return out.reshape(NB * k, LANES)


def exchange_in_cube(rows):
    k = rows.shape[0] // 8
    return lax.all_to_all(rows.reshape(8, 1, k * LANES), CUBE, 0, 0, tiled=True).reshape(8 * k, LANES)


def over_group(rows):
    parts = [rows]
    for k in (1, 2, 3):
        parts.append(lax.ppermute(rows, GRP, [(i, i ^ k) for i in range(4)]))
    return parts


def steps(primal, dual, objective, lower, upper, bound_kind, rhs, row_kind, q_tiles, q_index, k_tiles, k_rows, k_cols):
    hess, cons = q_tiles, k_tiles
    me = lax.axis_index(GRP).astype(I32).reshape(1)

    def wide(v):
        return v.reshape(-1, LANES)

    inputs = (q_index[0], k_cols, k_rows, wide(primal), wide(objective), wide(lower), wide(upper), wide(bound_kind), wide(dual),
              wide(rhs), wide(row_kind))
    room = [(pltpu.SMEM if i < 3 else pltpu.VMEM)(v.shape, v.dtype) for i, v in enumerate(inputs)]
    five = ((5 * NB, LANES), F32)
    first, block, own = call(start_kernel, [((6 * NB, LANES), F32), ((2 * NB + 8, LANES), F32), five], me, *inputs, smem=1,
                             where=pltpu.HBM, scratch=room + [pltpu.SemaphoreType.DMA((len(inputs),))], limit=66800000)
    parts = over_group(block)
    got = exchange(first)
    msg = call(first_gather_kernel, [five], got)
    want = exchange(msg)
    wide_block = ((NB, 2 * LANES), F32)
    scalar = ((8, LANES), F32)
    cube = ((8 * 13, LANES), F32)
    grads = (pltpu.VMEM((104, LANES), F32),)
    y, b, kind, rel, take, hot, read, msg = call(
        first_products_kernel,
        [wide_block, wide_block, wide_block, ((32, LANES), I32), ((2 * LANES, LANES), BF16), ((208, NT * NB), BF16), five, five],
        want, got, *parts, hess, cons, scratch=ROWS_SCRATCH)
    msg = call(first_sum_kernel, [cube], exchange(msg), hot)
    own_x, read_x, prods = call(first_primal_kernel, [ROWS, ROWS, PACKED], exchange_in_cube(msg), own, read, cons, scratch=grads)
    parts = over_group(prods)
    hess_prod, put = call(hessian_kernel, [ROWS, ((4 * LANES, 2 * LANES), BF16)], read_x, rel, hess)
    y, msg = call(dual_kernel, [wide_block, ((6 * NB, LANES), F32)], *parts, put, take, y, b, kind, hess_prod, cons,
                  scratch=ROWS_SCRATCH)
    weight, msg = call(second_sum_kernel, [scalar, cube], exchange(msg), hot)
    final, prods = call(second_primal_kernel, [ROWS, PACKED], exchange_in_cube(msg), own, own_x, read, read_x, weight, cons,
                        scratch=grads)
    parts = over_group(prods)
    y, msg = call(last_dual_kernel, [ROWS, ROWS], *parts, put, y, b, kind, weight)
    weight, dual_out, final = call(last_kernel, [((1, 1), F32), ((32, LANES), F32), ROWS], exchange(msg), y, final, weight)
    return final.reshape(-1), dual_out.reshape(-1), weight.reshape(())


def solution(mesh):
    finer = Mesh(mesh.devices.reshape(2, 2, 4, 2, 2, 2, 2), (*GRP, *BLK))
    placed = (P(BLK_GRP),) * 8 + (
        P(GRP, BLK, None, None),
        P(GRP, None, BLK),
        P(GRP, BLK, None, None),
        P(GRP, BLK),
        P(GRP, BLK),
    )
    return jax.shard_map(steps, mesh=finer, in_specs=placed, out_specs=(P(BLK_GRP), P(BLK_GRP), P()), check_vma=False)
```

```python
import jax
import jax.numpy as jnp
from jax import lax
from jax.experimental import pallas as pl
from jax.experimental.pallas import tpu as pltpu
from jax.sharding import Mesh
from jax.sharding import PartitionSpec as P

BLK = ("zh", "zl", "xh", "xl", "yl")
CUBE = ("zl", "xl", "yl")
GRP = ("grp_0", "grp_1")
BLK_GRP = (*BLK, *GRP)
EPSILON = 1e-06
STEP_SCALE = 0.5
F32, BF16, I32 = jnp.float32, jnp.bfloat16, jnp.int32

NB = 64
LANES = 128
NQ, NK = 4, 6
NT = NQ + NK
VMEM_LIMIT = 8 * 1024 * 1024
COST = 10000000000
FIRST, IDS = 5, 4
FREE = 1e38


def iota(shape, dim):
    return lax.broadcasted_iota(I32, shape, dim)


def lane(rows=NB):
    return iota((rows, LANES), 1)


def slot_of(lanes):
    return (lanes >> 2) & 15


def split(v, n):
    parts = []
    for _ in range(n - 1):
        p = v.astype(BF16)
        parts.append(p)
        v = v - p.astype(F32)
    parts.append(v.astype(BF16))
    return parts


def dot(a, b):
    return jnp.dot(a, b, preferred_element_type=F32)


def spread(v):
    return jnp.transpose(jnp.concatenate([v, pltpu.roll(v, 64, 1)], axis=0))[:NB]


def total(v):
    return jnp.sum(jnp.sum(v, axis=0, keepdims=True), axis=1, keepdims=True)


def along(v, idx):
    return jnp.take_along_axis(v, idx, axis=1)


def column(v, c):
    return jnp.broadcast_to(v[:, c : c + 1], v.shape)


def gather_tiles(ids, tables, out, first, k):
    ln = lane()
    t_of = along(ids & 15, slot_of(ln))
    idx = (ln & 64) + t_of * 4 + (ln & 3)
    owner = ids >> 4
    ones = []
    for j in range(NT):
        o = jnp.where((ln & 63) == column(owner, j), 1.0, 0.0).astype(BF16)
        ones.append(jnp.concatenate([o, o], axis=1))
    ones = jnp.concatenate(ones, axis=0)
    for n, table in enumerate(tables):
        a, b, c = split(table, 3)
        got = dot(ones, jnp.concatenate([a, b, c, jnp.zeros_like(a)], axis=0))
        msg = jnp.zeros((NB, LANES), F32)
        for j in range(NT):
            msg = jnp.where(slot_of(ln) == j, along(got[j * NB : (j + 1) * NB], idx), msg)
        out[pl.ds(first + n, NB, stride=k), :] = msg


def cube_of(b):
    return ((b >> 3) & 1) * 4 + ((b >> 1) & 1) * 2 + (b & 1)


def send_rows(rows_ref, out, n, k):
    low = lane(n) < 64
    for q in range(4):
        a = rows_ref[pl.ds(q, n, stride=8), :]
        b = rows_ref[pl.ds(q + 4, n, stride=8), :]
        halves = (jnp.where(low, a, pltpu.roll(b, 64, 1)), jnp.where(low, pltpu.roll(a, 64, 1), b))
        for peer in range(NB):
            if cube_of(peer) >> 1 == q:
                out[peer * k : peer * k + n, :] = halves[cube_of(peer) & 1]


def wanted(got):
    base = lax.axis_index("zh") * 16 + lax.axis_index("xh") * 4
    ln = lane(8)
    sub = iota((8, LANES), 0)
    want = jnp.zeros((8, LANES), F32)
    for p in range(8):
        b = base + (p >> 2) * 8 + ((p >> 1) & 1) * 2 + (p & 1)
        want = jnp.where(sub == p, jnp.broadcast_to(got[pl.ds(b * FIRST + IDS, 1), :], (8, LANES)), want)
    member = base + ((sub >> 2) & 1) * 8 + ((sub >> 1) & 1) * 2 + (sub & 1)
    return jnp.where(ln < NT, want, (member * 16 + ln - NT).astype(F32))


def matches(want, row_of, n, m):
    low = lane(1) < 64
    sides = []
    for parity in range(2):
        chunks = []
        for c in range(n):
            a, b = (row_of(u % n, (u // n) ^ parity) for u in (2 * c, 2 * c + 1))
            row = jnp.where(low, a, b)
            hits = []
            for kk in range(m):
                w = jnp.broadcast_to(want[:, 2 * kk + parity : 2 * kk + parity + 1], (8, LANES))
                hits.append(jnp.where(w == row, 1.0, 0.0))
            chunks.append(jnp.concatenate(hits, axis=0))
        sides.append(jnp.concatenate(chunks, axis=1))
    return jnp.concatenate(sides, axis=0).astype(BF16)


def match_table(got):
    ids = got[pl.ds(IDS, NB, stride=FIRST), :]
    flat = jnp.transpose(jnp.concatenate([ids, ids], axis=0))

    def row_of(pair, odd):
        j = 2 * pair + odd
        r = NT + j if j < NQ else j
        return flat[r : r + 1]

    return matches(wanted(got), row_of, NT // 2, 13)


def sum_rows(msg, hot, out, n, m, k):
    blocks = [msg[pl.ds(i, NB, stride=k), :] for i in range(n)]
    blocks += [pltpu.roll(v, 64, 1) for v in blocks]
    high, low = [], []
    for v in blocks:
        a, b = split(v, 2)
        high.append(a)
        low.append(b)
    got = dot(hot, jnp.concatenate(high, axis=0)) + dot(hot, jnp.concatenate(low, axis=0))
    left = lane(8) < 64
    for kk in range(m):
        out[pl.ds(kk, 8, stride=m), :] = jnp.where(left, got[8 * kk : 8 * kk + 8], got[8 * (m + kk) : 8 * (m + kk) + 8])


def receive_rows(msg, rows, m):
    low = lane(m) < 64
    for q in range(4):
        a = msg[2 * m * q : 2 * m * q + m, :]
        b = msg[2 * m * q + m : 2 * m * q + 2 * m, :]
        rows[pl.ds(q, m, stride=8), :] = jnp.where(low, a, pltpu.roll(b, 64, 1))
        rows[pl.ds(q + 4, m, stride=8), :] = jnp.where(low, pltpu.roll(a, 64, 1), b)


def bounds(lower, upper, kind, free):
    return (
        jnp.where((kind == 1) | (kind == 2), lower, -free),
        jnp.where((kind == 2) | (kind == 3), upper, free),
    )


def forward_tiles(tiles_ref, rows_ref, count, first):
    ln = lane()
    out = jnp.zeros((NB, LANES), F32)
    for t in range(count):
        j = first + t
        vec = [rows_ref[4 * j + q : 4 * j + q + 1, :] for q in range(4)]
        for qo in range(4):
            for h in range(2):
                at = slice(qo * 128 + h * 64, qo * 128 + h * 64 + 64)
                p = tiles_ref[0, t, at, 0:128] * vec[0]
                for q in range(1, 4):
                    p = p + tiles_ref[0, t, at, q * 128 : (q + 1) * 128] * vec[q]
                out = jnp.where(ln == h * 64 + 4 * j + qo, jnp.sum(p, axis=1, keepdims=True), out)
    return out


def transposed_tiles(tiles_ref, cols, rows_ref, first):
    for t in range(NK):
        j = first + t
        acc = [jnp.zeros((8, LANES), F32) for _ in range(4)]
        for qo in range(4):
            for h in range(2):
                at = slice(qo * 128 + h * 64, qo * 128 + h * 64 + 64)
                v = along(cols, jnp.full((NB, LANES), h * 64 + 4 * j + qo, I32))
                for q in range(4):
                    p = tiles_ref[0, t, at, q * 128 : (q + 1) * 128] * v
                    acc[q] = acc[q] + jnp.sum(p.reshape(8, 8, LANES), axis=0)
        for q in range(4):
            rows_ref[4 * j + q : 4 * j + q + 1, :] = jnp.sum(acc[q], axis=0, keepdims=True)


def join(parts, part):
    low = (lane() & 32) == 0
    blocks = []
    for k in (0, 2):
        a, b = parts[k], parts[k + 1]
        if part == 0:
            blocks.append(jnp.where(low, a, pltpu.roll(b, 32, 1)))
        else:
            blocks.append(jnp.where(low, pltpu.roll(a, LANES - 32, 1), b))
    return jnp.concatenate(blocks, axis=1)


def pack(prods, extra):
    ln = lane(32)
    both = jnp.where((ln & 63) < 40, prods[:32], pltpu.roll(prods[32:], 24, 1))
    return jnp.where(ln == 0, extra, both)


def unpack(packed):
    return jnp.concatenate([packed, pltpu.roll(packed, LANES - 24, 1)], axis=0)


def dual_step(parts, hot, y, rhs, kind, step):
    high, low = [], []
    for p in parts:
        a, b = split(unpack(p), 2)
        high.append(a)
        low.append(b)
    extrap = dot(jnp.concatenate(high, axis=1), hot) + dot(jnp.concatenate(low, axis=1), hot)
    new = y + step * (rhs - extrap)
    new = jnp.where(kind == 1.0, jnp.maximum(new, 0.0), new)
    moved = new - y
    return new, total(moved * moved)


def new_weight(weight, dual_sq, primal_sq):
    return jnp.sqrt(weight * jnp.sqrt((dual_sq + EPSILON) / (primal_sq + EPSILON)))


def spread_two(v, w):
    t = jnp.transpose(jnp.concatenate([v, w], axis=0))
    low = lane() < 64
    top, bottom = t[:NB], t[NB:]
    return jnp.where(low, top, pltpu.roll(bottom, 64, 1)), jnp.where(low, pltpu.roll(top, 64, 1), bottom)


def start_kernel(me, q_index, k_cols, k_rows, primal, objective, lower, upper, bound_kind, dual, rhs, row_kind, out, block, *scratch):
    refs = (q_index, k_cols, k_rows, primal, objective, lower, upper, bound_kind, dual, rhs, row_kind)
    sems = scratch[-1]
    copies = [pltpu.make_async_copy(r, s, sems.at[i]) for i, (r, s) in enumerate(zip(refs, scratch))]
    for c in copies:
        c.start()
    qi, kc, kr, p, ob, lo, up, bk, du, rh, rk = scratch[:-1]
    for c in copies:
        c.wait()
    low, high = bounds(lo[...], up[...], bk[...], FREE)
    for k, v in enumerate((*spread_two(p[...], ob[...]), *spread_two(low, high))):
        out[pl.ds(k, NB, stride=FIRST), :] = v
    ln = lane(8)
    ids = jnp.zeros((8, LANES), F32)
    for j in range(NQ):
        ids = jnp.where(ln == j, qi[1, j].astype(F32), ids)
        ids = jnp.where(ln == NT + j, qi[0, j].astype(F32), ids)
    for j in range(NK):
        ids = jnp.where(ln == NQ + j, kc[0, j].astype(F32), ids)
    out[pl.ds(IDS, NB, stride=FIRST), :] = jnp.broadcast_to(ids[:1], (NB, LANES))
    a, b = spread_two(
        jnp.concatenate([du[...], rh[...]], axis=0),
        jnp.concatenate([rk[...].astype(F32), jnp.zeros((32, LANES), F32)], axis=0),
    )
    block[0:NB] = a
    block[NB : 2 * NB] = b
    ids = jnp.zeros((8, LANES), F32)
    for j in range(NK):
        ids = jnp.where(slot_of(ln) == NQ + j, kr[0, j].astype(F32), ids)
    block[2 * NB :] = jnp.where(ln == 0, me[0].astype(F32), ids)


def first_gather_kernel(got, msg):
    ids = got[pl.ds(IDS, NB, stride=FIRST), :].astype(I32)
    gather_tiles(ids, [got[pl.ds(n, NB, stride=FIRST), :] for n in range(4)], msg, 0, 4)


def dual_tables(parts, y, rhs, kind, tiles, take):
    y[...] = join([p[0:NB] for p in parts], 0)
    rhs[...] = join([p[0:NB] for p in parts], 1)
    kind[...] = join([p[NB : 2 * NB] for p in parts], 0)
    mine = jnp.broadcast_to(parts[0][2 * NB :, 0:1], (8, LANES)).astype(I32)
    rel = []
    for p in parts:
        r = p[2 * NB :].astype(I32)
        rel.append((((r >> 3) ^ mine) << 3) | (r & 7))
    tiles[...] = jnp.concatenate(rel, axis=0)
    ln = lane(LANES)
    sub = iota((LANES, LANES), 0)
    r = jnp.broadcast_to(rel[0][:1], (LANES, LANES))
    lane_ok = (slot_of(ln) >= NQ) & (slot_of(ln) < NT)
    for kk in range(2):
        tile = (2 * kk + ((sub >> 5) & 1)) * 8 + ((sub >> 2) & 7)
        hit = ((ln & 64) == (sub & 64)) & ((ln & 3) == (sub & 3)) & lane_ok & (tile == r)
        take[kk * LANES : (kk + 1) * LANES, :] = jnp.where(hit, 1.0, 0.0).astype(BF16)


def put_table(tiles, put):
    ln = lane(LANES)
    sub = iota((LANES, LANES), 0)
    same = ((ln & 64) == (sub & 64)) & ((ln & 3) == (sub & 3)) & (slot_of(sub) >= NQ) & (slot_of(sub) < NT)
    for p in range(4):
        r = jnp.transpose(jnp.broadcast_to(tiles[8 * p : 8 * p + 1].astype(F32), (LANES, LANES))).astype(I32)
        for kk in range(2):
            tile = (2 * kk + ((ln >> 5) & 1)) * 8 + ((ln >> 2) & 7)
            put[p * LANES : (p + 1) * LANES, kk * LANES : (kk + 1) * LANES] = jnp.where(same & (tile == r), 1.0, 0.0).astype(BF16)


def take_rows(y, take):
    a, b = split(y, 2)
    return dot(a, take) + dot(b, take)


def first_products_kernel(msg, got, p0, p1, p2, p3, hess, cons, y, rhs, kind, tiles, take, hot, read, out, rows):
    hot[...] = match_table(got)
    dual_tables([p0, p1, p2, p3], y, rhs, kind, tiles, take)
    m = [msg[pl.ds(n, NB, stride=4), :] for n in range(4)]
    for n, v in enumerate((*spread_two(m[0], m[1]), *spread_two(m[2], m[3]))):
        read[n * NB : (n + 1) * NB] = v
    first = spread(forward_tiles(hess, read, NQ, 0))
    transposed_tiles(cons, take_rows(y[...], take[...]), rows, NQ)
    rows[0 : 4 * NQ] = first[0 : 4 * NQ]
    rows[4 * NQ : 4 * NT] = -rows[4 * NQ : 4 * NT]
    send_rows(rows, out, 5, 5)


def first_sum_kernel(msg, hot, out):
    sum_rows(msg, hot[...], out, 5, 13, 5)


def second_sum_kernel(msg, hot, weight, out):
    sum_rows(msg, hot[...], out, 5, 13, 6)
    tail = jnp.sum(msg[pl.ds(5, NB, stride=6), :], axis=0, keepdims=True)
    weight[...] = jnp.broadcast_to(new_weight(jnp.ones((1, 1), F32), tail[:, 1:2], tail[:, 0:1]), (8, LANES))


def primal_step(grads, own, read, own_x, read_x, tau, own_out, rows):
    receive_rows(grads, rows, 13)
    c, low, high, kind = own
    x = own_x[...]
    low, high = bounds(low[...], high[...], kind[...], jnp.inf)
    new = jnp.minimum(jnp.maximum(x - tau * (rows[4 * NT :] + c[...]), low), high)
    own_out[...] = new
    moved = new - x
    c, low, high = (read[k * NB : k * NB + 4 * NT] for k in range(1, 4))
    x = read_x[0 : 4 * NT]
    new = jnp.minimum(jnp.maximum(x - tau * (rows[0 : 4 * NT] + c), low), high)
    rows[0 : 4 * NT] = 2.0 * new - x
    return new, total(moved * moved)


def first_primal_kernel(grads, c, low, high, kind, read, own_x, tiles, own_out, read_out, out, rows):
    new, moved = primal_step(grads, (c, low, high, kind), read, own_x, read, jnp.full((1, 1), STEP_SCALE, F32), own_out, rows)
    read_out[0 : 4 * NT] = new
    out[...] = pack(forward_tiles(tiles, rows, NK, NQ), moved)


def second_primal_kernel(grads, c, low, high, kind, read, own_x, read_x, weight, tiles, own_out, out, rows):
    tau = STEP_SCALE / weight[0:1, 0:1]
    _, moved = primal_step(grads, (c, low, high, kind), read, own_x, read_x, tau, own_out, rows)
    out[...] = pack(forward_tiles(tiles, rows, NK, NQ), moved)


def hessian_kernel(vec, rel, tiles, out, put):
    out[...] = spread(forward_tiles(tiles, vec, NQ, 0))
    put_table(rel, put)


def primal_total(parts):
    s = parts[0][0:1, 0:1]
    for p in parts[1:]:
        s = s + p[0:1, 0:1]
    return s


def dual_kernel(p0, p1, p2, p3, put, take, y, rhs, kind, hess, tiles, y_out, out, rows):
    parts = [p[...] for p in (p0, p1, p2, p3)]
    new, moved = dual_step(parts, put[...], y[...], rhs[...], kind[...], STEP_SCALE)
    y_out[...] = new
    transposed_tiles(tiles, take_rows(new, take[...]), rows, NQ)
    rows[0 : 4 * NQ] = hess[0 : 4 * NQ]
    rows[4 * NQ : 4 * NT] = -rows[4 * NQ : 4 * NT]
    send_rows(rows, out, 5, 6)
    out[pl.ds(5, NB, stride=6), :] = jnp.where(lane() == 0, primal_total(parts), moved)


def last_dual_kernel(p0, p1, p2, p3, put, y, rhs, kind, weight, y_out, out):
    parts = [p[...] for p in (p0, p1, p2, p3)]
    new, moved = dual_step(parts, put[...], y[...], rhs[...], kind[...], STEP_SCALE * weight[0:1, 0:1])
    y_out[...] = new[:, :LANES]
    out[...] = jnp.where(lane() == 0, primal_total(parts), moved)


def last_kernel(msg, y, x, weight, out, dual_out, final):
    tail = jnp.sum(msg[...], axis=0, keepdims=True)
    out[...] = new_weight(weight[0:1, 0:1], tail[:, 1:2], tail[:, 0:1])
    dual_out[...] = spread(y[...])[:32]
    final[...] = x[...]


def call(kernel, outs, *args, smem=0, scratch=(), cost=COST, where=pltpu.VMEM, limit=VMEM_LIMIT):
    v = pl.BlockSpec(memory_space=pltpu.VMEM)
    w = pl.BlockSpec(memory_space=where)
    s = pl.BlockSpec(memory_space=pltpu.SMEM)
    shapes = [jax.ShapeDtypeStruct(*o) for o in outs]
    res = pl.pallas_call(
        kernel,
        out_shape=shapes,
        in_specs=[s] * smem + [w] * (len(args) - smem),
        out_specs=[v] * len(shapes),
        scratch_shapes=list(scratch),
        compiler_params=pltpu.CompilerParams(vmem_limit_bytes=limit),
        cost_estimate=pl.CostEstimate(flops=cost, bytes_accessed=10000000, transcendentals=0),
    )(*args)
    return res[0] if len(outs) == 1 else res


ROWS = ((NB, LANES), F32)
PACKED = ((NB // 2, LANES), F32)
ROWS_SCRATCH = (pltpu.VMEM((NB, LANES), F32),)


def exchange(rows):
    k = rows.shape[0] // NB
    out = lax.all_to_all(rows.reshape(NB, 1, k * LANES), BLK, 0, 0, tiled=True)
    return out.reshape(NB * k, LANES)


def exchange_in_cube(rows):
    k = rows.shape[0] // 8
    return lax.all_to_all(rows.reshape(8, 1, k * LANES), CUBE, 0, 0, tiled=True).reshape(8 * k, LANES)


def over_group(rows):
    parts = [rows]
    for k in (1, 2, 3):
        parts.append(lax.ppermute(rows, GRP, [(i, i ^ k) for i in range(4)]))
    return parts


def steps(primal, dual, objective, lower, upper, bound_kind, rhs, row_kind, q_tiles, q_index, k_tiles, k_rows, k_cols):
    hess, cons = q_tiles, k_tiles
    me = lax.axis_index(GRP).astype(I32).reshape(1)

    def wide(v):
        return v.reshape(-1, LANES)

    inputs = (q_index[0], k_cols, k_rows, wide(primal), wide(objective), wide(lower), wide(upper), wide(bound_kind), wide(dual),
              wide(rhs), wide(row_kind))
    room = [(pltpu.SMEM if i < 3 else pltpu.VMEM)(v.shape, v.dtype) for i, v in enumerate(inputs)]
    first, block = call(start_kernel, [((FIRST * NB, LANES), F32), ((2 * NB + 8, LANES), F32)], me, *inputs, smem=1,
                        where=pltpu.HBM, scratch=room + [pltpu.SemaphoreType.DMA((len(inputs),))], limit=66800000)
    parts = over_group(block)
    got = exchange(first)
    four = ((4 * NB, LANES), F32)
    msg = call(first_gather_kernel, [four], got)
    want = exchange(msg)
    wide_block = ((NB, 2 * LANES), F32)
    scalar = ((8, LANES), F32)
    cube = ((8 * 13, LANES), F32)
    grads = (pltpu.VMEM((104, LANES), F32),)
    y, b, kind, rel, take, hot, read, msg = call(
        first_products_kernel,
        [wide_block, wide_block, wide_block, ((32, LANES), I32), ((2 * LANES, LANES), BF16), ((208, NT * NB), BF16),
         four, ((5 * NB, LANES), F32)],
        want, got, *parts, hess, cons, scratch=ROWS_SCRATCH)
    msg = call(first_sum_kernel, [cube], exchange(msg), hot)
    own = [wide(v) for v in (objective, lower, upper, bound_kind)]
    own_x, read_x, prods = call(first_primal_kernel, [ROWS, ((4 * NT, LANES), F32), PACKED], exchange_in_cube(msg), *own, read,
                                wide(primal), cons, scratch=grads)
    parts = over_group(prods)
    hess_prod, put = call(hessian_kernel, [ROWS, ((4 * LANES, 2 * LANES), BF16)], read_x, rel, hess)
    y, msg = call(dual_kernel, [wide_block, ((6 * NB, LANES), F32)], *parts, put, take, y, b, kind, hess_prod, cons,
                  scratch=ROWS_SCRATCH)
    weight, msg = call(second_sum_kernel, [scalar, cube], exchange(msg), hot)
    final, prods = call(second_primal_kernel, [ROWS, PACKED], exchange_in_cube(msg), *own, read, own_x, read_x, weight, cons,
                        scratch=grads)
    parts = over_group(prods)
    y, msg = call(last_dual_kernel, [ROWS, ROWS], *parts, put, y, b, kind, weight)
    weight, dual_out, final = call(last_kernel, [((1, 1), F32), ((32, LANES), F32), ROWS], exchange(msg), y, final, weight)
    return final.reshape(-1), dual_out.reshape(-1), weight.reshape(())


def solution(mesh):
    finer = Mesh(mesh.devices.reshape(2, 2, 4, 2, 2, 2, 2), (*GRP, *BLK))
    placed = (P(BLK_GRP),) * 8 + (
        P(GRP, BLK, None, None),
        P(GRP, None, BLK),
        P(GRP, BLK, None, None),
        P(GRP, BLK),
        P(GRP, BLK),
    )
    return jax.shard_map(steps, mesh=finer, in_specs=placed, out_specs=(P(BLK_GRP), P(BLK_GRP), P()), check_vma=False)
```

```python
import jax
import jax.numpy as jnp
from jax import lax
from jax.experimental import pallas as pl
from jax.experimental.pallas import tpu as pltpu
from jax.sharding import Mesh
from jax.sharding import PartitionSpec as P

BLK = ("zh", "zl", "xh", "xl", "yl")
CUBE = ("zl", "xl", "yl")
GRP = ("grp_0", "grp_1")
BLK_GRP = (*BLK, *GRP)
EPSILON = 1e-06
STEP_SCALE = 0.5
F32, BF16, I32 = jnp.float32, jnp.bfloat16, jnp.int32

NB = 64
LANES = 128
NQ, NK = 4, 6
NT = NQ + NK
VMEM_LIMIT = 8 * 1024 * 1024
COST = 10000000000
FIRST, IDS = 5, 4
FREE = 1e38


def iota(shape, dim):
    return lax.broadcasted_iota(I32, shape, dim)


def lane(rows=NB):
    return iota((rows, LANES), 1)


def slot_of(lanes):
    return (lanes >> 2) & 15


def split(v, n):
    parts = []
    for _ in range(n - 1):
        p = v.astype(BF16)
        parts.append(p)
        v = v - p.astype(F32)
    parts.append(v.astype(BF16))
    return parts


def dot(a, b):
    return jnp.dot(a, b, preferred_element_type=F32)


def spread(v):
    return jnp.transpose(jnp.concatenate([v, pltpu.roll(v, 64, 1)], axis=0))[:NB]


def total(v):
    return jnp.sum(jnp.sum(v, axis=0, keepdims=True), axis=1, keepdims=True)


def along(v, idx):
    return jnp.take_along_axis(v, idx, axis=1)


def column(v, c):
    return jnp.broadcast_to(v[:, c : c + 1], v.shape)


def gather_tiles(ids, tables, out):
    ln = lane()
    slot = slot_of(ln)

    def index(tile):
        return (ln & 64) + along(ids & 15, tile) * 4 + (ln & 3)

    idx = [index(jnp.where(slot < NT, slot, slot - NT + n * (16 - NT))) for n in range(2)]
    owner = ids >> 4
    ones = []
    for j in range(NT):
        o = jnp.where((ln & 63) == column(owner, j), 1.0, 0.0).astype(BF16)
        ones.append(jnp.concatenate([o, o], axis=1))
    ones = jnp.concatenate(ones, axis=0)
    got = []
    for n in (0, 2):
        pieces = [jnp.concatenate([a, b], axis=1) for a, b in zip(split(tables[n], 3), split(tables[n + 1], 3))]
        both = dot(ones, jnp.concatenate([*pieces, jnp.zeros_like(pieces[0])], axis=0))
        got += [both[:, :LANES], both[:, LANES:]]
    for n in range(3):
        msg = jnp.zeros((NB, LANES), F32)
        for s in range(16):
            j = s if s < NT else s - NT + n * (16 - NT)
            if j < NT:
                table = got[n if s < NT else 3]
                msg = jnp.where(slot == s, along(table[j * NB : (j + 1) * NB], idx[n & 1]), msg)
        out[pl.ds(n, NB, stride=3), :] = msg


def cube_of(b):
    return ((b >> 3) & 1) * 4 + ((b >> 1) & 1) * 2 + (b & 1)


def send_rows(rows_ref, out, n, k):
    low = lane(n) < 64
    for q in range(4):
        a = rows_ref[pl.ds(q, n, stride=8), :]
        b = rows_ref[pl.ds(q + 4, n, stride=8), :]
        halves = (jnp.where(low, a, pltpu.roll(b, 64, 1)), jnp.where(low, pltpu.roll(a, 64, 1), b))
        for peer in range(NB):
            if cube_of(peer) >> 1 == q:
                out[peer * k : peer * k + n, :] = halves[cube_of(peer) & 1]


def wanted(got):
    base = lax.axis_index("zh") * 16 + lax.axis_index("xh") * 4
    ln = lane(8)
    sub = iota((8, LANES), 0)
    want = jnp.zeros((8, LANES), F32)
    for p in range(8):
        b = base + (p >> 2) * 8 + ((p >> 1) & 1) * 2 + (p & 1)
        want = jnp.where(sub == p, jnp.broadcast_to(got[pl.ds(b * FIRST + IDS, 1), :], (8, LANES)), want)
    member = base + ((sub >> 2) & 1) * 8 + ((sub >> 1) & 1) * 2 + (sub & 1)
    return jnp.where(ln < NT, want, (member * 16 + ln - NT).astype(F32))


def matches(want, row_of, n, m):
    low = lane(1) < 64
    sides = []
    for parity in range(2):
        chunks = []
        for c in range(n):
            a, b = (row_of(u % n, (u // n) ^ parity) for u in (2 * c, 2 * c + 1))
            row = jnp.where(low, a, b)
            hits = []
            for kk in range(m):
                w = jnp.broadcast_to(want[:, 2 * kk + parity : 2 * kk + parity + 1], (8, LANES))
                hits.append(jnp.where(w == row, 1.0, 0.0))
            chunks.append(jnp.concatenate(hits, axis=0))
        sides.append(jnp.concatenate(chunks, axis=1))
    return jnp.concatenate(sides, axis=0).astype(BF16)


def match_table(got):
    ids = got[pl.ds(IDS, NB, stride=FIRST), :]
    flat = jnp.transpose(jnp.concatenate([ids, ids], axis=0))

    def row_of(pair, odd):
        j = 2 * pair + odd
        r = NT + j if j < NQ else j
        return flat[r : r + 1]

    return matches(wanted(got), row_of, NT // 2, 13)


def sum_rows(msg, hot, out, n, m, k):
    blocks = [msg[pl.ds(i, NB, stride=k), :] for i in range(n)]
    blocks += [pltpu.roll(v, 64, 1) for v in blocks]
    got = dot(hot, jnp.concatenate([jnp.concatenate(split(v, 2), axis=1) for v in blocks], axis=0))
    got = got[:, :LANES] + got[:, LANES:]
    left = lane(8) < 64
    for kk in range(m):
        out[pl.ds(kk, 8, stride=m), :] = jnp.where(left, got[8 * kk : 8 * kk + 8], got[8 * (m + kk) : 8 * (m + kk) + 8])


def receive_rows(msg, rows, m):
    low = lane(m) < 64
    for q in range(4):
        a = msg[2 * m * q : 2 * m * q + m, :]
        b = msg[2 * m * q + m : 2 * m * q + 2 * m, :]
        rows[pl.ds(q, m, stride=8), :] = jnp.where(low, a, pltpu.roll(b, 64, 1))
        rows[pl.ds(q + 4, m, stride=8), :] = jnp.where(low, pltpu.roll(a, 64, 1), b)


def bounds(lower, upper, kind, free):
    return (
        jnp.where((kind == 1) | (kind == 2), lower, -free),
        jnp.where((kind == 2) | (kind == 3), upper, free),
    )


def forward_tiles(tiles_ref, rows_ref, count, first):
    ln = lane()
    out = jnp.zeros((NB, LANES), F32)
    for t in range(count):
        j = first + t
        vec = [rows_ref[4 * j + q : 4 * j + q + 1, :] for q in range(4)]
        for qo in range(4):
            for h in range(2):
                at = slice(qo * 128 + h * 64, qo * 128 + h * 64 + 64)
                p = tiles_ref[0, t, at, 0:128] * vec[0]
                for q in range(1, 4):
                    p = p + tiles_ref[0, t, at, q * 128 : (q + 1) * 128] * vec[q]
                out = jnp.where(ln == h * 64 + 4 * j + qo, jnp.sum(p, axis=1, keepdims=True), out)
    return out


def transposed_tiles(tiles_ref, cols, rows_ref, first):
    for t in range(NK):
        j = first + t
        acc = [jnp.zeros((8, LANES), F32) for _ in range(4)]
        for qo in range(4):
            for h in range(2):
                at = slice(qo * 128 + h * 64, qo * 128 + h * 64 + 64)
                v = along(cols, jnp.full((NB, LANES), h * 64 + 4 * j + qo, I32))
                for q in range(4):
                    p = tiles_ref[0, t, at, q * 128 : (q + 1) * 128] * v
                    acc[q] = acc[q] + jnp.sum(p.reshape(8, 8, LANES), axis=0)
        for q in range(4):
            rows_ref[4 * j + q : 4 * j + q + 1, :] = jnp.sum(acc[q], axis=0, keepdims=True)


def join(parts, part):
    low = (lane() & 32) == 0
    blocks = []
    for k in (0, 2):
        a, b = parts[k], parts[k + 1]
        if part == 0:
            blocks.append(jnp.where(low, a, pltpu.roll(b, 32, 1)))
        else:
            blocks.append(jnp.where(low, pltpu.roll(a, LANES - 32, 1), b))
    return jnp.concatenate(blocks, axis=1)


def pack(prods, extra):
    ln = lane(32)
    both = jnp.where((ln & 63) < 40, prods[:32], pltpu.roll(prods[32:], 24, 1))
    return jnp.where(ln == 0, extra, both)


def unpack(packed):
    return jnp.concatenate([packed, pltpu.roll(packed, LANES - 24, 1)], axis=0)


def dual_step(parts, hot, y, rhs, kind, step):
    high, low = [], []
    for p in parts:
        a, b = split(unpack(p), 2)
        high.append(a)
        low.append(b)
    extrap = dot(jnp.concatenate([jnp.concatenate(high, axis=1), jnp.concatenate(low, axis=1)], axis=0), hot)
    extrap = extrap[:NB] + extrap[NB:]
    new = y + step * (rhs - extrap)
    new = jnp.where(kind == 1.0, jnp.maximum(new, 0.0), new)
    moved = new - y
    return new, total(moved * moved)


def new_weight(weight, dual_sq, primal_sq):
    return jnp.sqrt(weight * jnp.sqrt((dual_sq + EPSILON) / (primal_sq + EPSILON)))


def spread_two(v, w):
    t = jnp.transpose(jnp.concatenate([v, w], axis=0))
    low = lane() < 64
    top, bottom = t[:NB], t[NB:]
    return jnp.where(low, top, pltpu.roll(bottom, 64, 1)), jnp.where(low, pltpu.roll(top, 64, 1), bottom)


def start_kernel(me, q_index, k_cols, k_rows, primal, objective, lower, upper, bound_kind, dual, rhs, row_kind, out, block, *scratch):
    refs = (q_index, k_cols, k_rows, primal, objective, lower, upper, bound_kind, dual, rhs, row_kind)
    sems = scratch[-1]
    copies = [pltpu.make_async_copy(r, s, sems.at[i]) for i, (r, s) in enumerate(zip(refs, scratch))]
    for c in copies:
        c.start()
    qi, kc, kr, p, ob, lo, up, bk, du, rh, rk = scratch[:-1]
    for c in copies:
        c.wait()
    low, high = bounds(lo[...], up[...], bk[...], FREE)
    for k, v in enumerate((*spread_two(p[...], ob[...]), *spread_two(low, high))):
        out[pl.ds(k, NB, stride=FIRST), :] = v
    ln = lane(8)
    ids = jnp.zeros((8, LANES), F32)
    for j in range(NQ):
        ids = jnp.where(ln == j, qi[1, j].astype(F32), ids)
        ids = jnp.where(ln == NT + j, qi[0, j].astype(F32), ids)
    for j in range(NK):
        ids = jnp.where(ln == NQ + j, kc[0, j].astype(F32), ids)
    out[pl.ds(IDS, NB, stride=FIRST), :] = jnp.broadcast_to(ids[:1], (NB, LANES))
    a, b = spread_two(
        jnp.concatenate([du[...], rh[...]], axis=0),
        jnp.concatenate([rk[...].astype(F32), jnp.zeros((32, LANES), F32)], axis=0),
    )
    block[0:NB] = a
    block[NB : 2 * NB] = b
    ids = jnp.zeros((8, LANES), F32)
    for j in range(NK):
        ids = jnp.where(slot_of(ln) == NQ + j, kr[0, j].astype(F32), ids)
    block[2 * NB :] = jnp.where(ln == 0, me[0].astype(F32), ids)


def first_gather_kernel(got, msg):
    ids = got[pl.ds(IDS, NB, stride=FIRST), :].astype(I32)
    gather_tiles(ids, [got[pl.ds(n, NB, stride=FIRST), :] for n in range(4)], msg)


def dual_tables(parts, y, rhs, kind, tiles, take):
    y[...] = join([p[0:NB] for p in parts], 0)
    rhs[...] = join([p[0:NB] for p in parts], 1)
    kind[...] = join([p[NB : 2 * NB] for p in parts], 0)
    mine = jnp.broadcast_to(parts[0][2 * NB :, 0:1], (8, LANES)).astype(I32)
    rel = []
    for p in parts:
        r = p[2 * NB :].astype(I32)
        rel.append((((r >> 3) ^ mine) << 3) | (r & 7))
    tiles[...] = jnp.concatenate(rel, axis=0)
    ln = lane(LANES)
    sub = iota((LANES, LANES), 0)
    r = jnp.broadcast_to(rel[0][:1], (LANES, LANES))
    lane_ok = (slot_of(ln) >= NQ) & (slot_of(ln) < NT)
    for kk in range(2):
        tile = (2 * kk + ((sub >> 5) & 1)) * 8 + ((sub >> 2) & 7)
        hit = ((ln & 64) == (sub & 64)) & ((ln & 3) == (sub & 3)) & lane_ok & (tile == r)
        take[kk * LANES : (kk + 1) * LANES, :] = jnp.where(hit, 1.0, 0.0).astype(BF16)


def put_table(tiles, put):
    ln = lane(LANES)
    sub = iota((LANES, LANES), 0)
    same = ((ln & 64) == (sub & 64)) & ((ln & 3) == (sub & 3)) & (slot_of(sub) >= NQ) & (slot_of(sub) < NT)
    for p in range(4):
        r = jnp.transpose(jnp.broadcast_to(tiles[8 * p : 8 * p + 1].astype(F32), (LANES, LANES))).astype(I32)
        for kk in range(2):
            tile = (2 * kk + ((ln >> 5) & 1)) * 8 + ((ln >> 2) & 7)
            put[p * LANES : (p + 1) * LANES, kk * LANES : (kk + 1) * LANES] = jnp.where(same & (tile == r), 1.0, 0.0).astype(BF16)


def take_rows(y, take):
    got = dot(jnp.concatenate(split(y, 2), axis=0), take)
    return got[:NB] + got[NB:]


def first_products_kernel(msg, got, p0, p1, p2, p3, hess, cons, y, rhs, kind, tiles, take, hot, read, out, rows):
    hot[...] = match_table(got)
    dual_tables([p0, p1, p2, p3], y, rhs, kind, tiles, take)
    m = [msg[pl.ds(n, NB, stride=3), :] for n in range(3)]
    m = (*spread_two(m[0], m[1]), spread(m[2]))
    for n in range(3):
        read[n * NB : (n + 1) * NB] = m[n]
    read[3 * NB : 3 * NB + 24] = m[0][40:64]
    read[3 * NB + 24 : 3 * NB + 40] = m[1][40:56]
    read[3 * NB + 40 : 4 * NB] = jnp.zeros((24, LANES), F32)
    first = spread(forward_tiles(hess, read, NQ, 0))
    transposed_tiles(cons, take_rows(y[...], take[...]), rows, NQ)
    rows[0 : 4 * NQ] = first[0 : 4 * NQ]
    rows[4 * NQ : 4 * NT] = -rows[4 * NQ : 4 * NT]
    send_rows(rows, out, 5, 5)


def first_sum_kernel(msg, hot, out):
    sum_rows(msg, hot[...], out, 5, 13, 5)


def second_sum_kernel(msg, hot, weight, out):
    sum_rows(msg, hot[...], out, 5, 13, 6)
    tail = jnp.sum(msg[pl.ds(5, NB, stride=6), :], axis=0, keepdims=True)
    weight[...] = jnp.broadcast_to(new_weight(jnp.ones((1, 1), F32), tail[:, 1:2], tail[:, 0:1]), (8, LANES))


def primal_step(grads, own, read, own_x, read_x, tau, own_out, rows):
    receive_rows(grads, rows, 13)
    c, low, high, kind = own
    x = own_x[...]
    low, high = bounds(low[...], high[...], kind[...], jnp.inf)
    new = jnp.minimum(jnp.maximum(x - tau * (rows[4 * NT :] + c[...]), low), high)
    own_out[...] = new
    moved = new - x
    c, low, high = (read[k * NB : k * NB + 4 * NT] for k in range(1, 4))
    x = read_x[0 : 4 * NT]
    new = jnp.minimum(jnp.maximum(x - tau * (rows[0 : 4 * NT] + c), low), high)
    rows[0 : 4 * NT] = 2.0 * new - x
    return new, total(moved * moved)


def first_primal_kernel(grads, c, low, high, kind, read, own_x, tiles, own_out, read_out, out, rows):
    new, moved = primal_step(grads, (c, low, high, kind), read, own_x, read, jnp.full((1, 1), STEP_SCALE, F32), own_out, rows)
    read_out[0 : 4 * NT] = new
    out[...] = pack(forward_tiles(tiles, rows, NK, NQ), moved)


def second_primal_kernel(grads, c, low, high, kind, read, own_x, read_x, weight, tiles, own_out, out, rows):
    tau = STEP_SCALE / weight[0:1, 0:1]
    _, moved = primal_step(grads, (c, low, high, kind), read, own_x, read_x, tau, own_out, rows)
    out[...] = pack(forward_tiles(tiles, rows, NK, NQ), moved)


def hessian_kernel(vec, rel, tiles, out, put):
    out[...] = spread(forward_tiles(tiles, vec, NQ, 0))
    put_table(rel, put)


def primal_total(parts):
    s = parts[0][0:1, 0:1]
    for p in parts[1:]:
        s = s + p[0:1, 0:1]
    return s


def dual_kernel(p0, p1, p2, p3, put, take, y, rhs, kind, hess, tiles, y_out, out, rows):
    parts = [p[...] for p in (p0, p1, p2, p3)]
    new, moved = dual_step(parts, put[...], y[...], rhs[...], kind[...], STEP_SCALE)
    y_out[...] = new
    transposed_tiles(tiles, take_rows(new, take[...]), rows, NQ)
    rows[0 : 4 * NQ] = hess[0 : 4 * NQ]
    rows[4 * NQ : 4 * NT] = -rows[4 * NQ : 4 * NT]
    send_rows(rows, out, 5, 6)
    out[pl.ds(5, NB, stride=6), :] = jnp.where(lane() == 0, primal_total(parts), moved)


def last_dual_kernel(p0, p1, p2, p3, put, y, rhs, kind, weight, y_out, out):
    parts = [p[...] for p in (p0, p1, p2, p3)]
    new, moved = dual_step(parts, put[...], y[...], rhs[...], kind[...], STEP_SCALE * weight[0:1, 0:1])
    y_out[...] = new[:, :LANES]
    out[...] = jnp.where(lane() == 0, primal_total(parts), moved)


def last_kernel(msg, y, x, weight, out, dual_out, final):
    tail = jnp.sum(msg[...], axis=0, keepdims=True)
    out[...] = new_weight(weight[0:1, 0:1], tail[:, 1:2], tail[:, 0:1])
    dual_out[...] = spread(y[...])[:32]
    final[...] = x[...]


def call(kernel, outs, *args, smem=0, scratch=(), cost=COST, where=pltpu.VMEM, limit=VMEM_LIMIT):
    v = pl.BlockSpec(memory_space=pltpu.VMEM)
    w = pl.BlockSpec(memory_space=where)
    s = pl.BlockSpec(memory_space=pltpu.SMEM)
    shapes = [jax.ShapeDtypeStruct(*o) for o in outs]
    res = pl.pallas_call(
        kernel,
        out_shape=shapes,
        in_specs=[s] * smem + [w] * (len(args) - smem),
        out_specs=[v] * len(shapes),
        scratch_shapes=list(scratch),
        compiler_params=pltpu.CompilerParams(vmem_limit_bytes=limit),
        cost_estimate=pl.CostEstimate(flops=cost, bytes_accessed=10000000, transcendentals=0),
    )(*args)
    return res[0] if len(outs) == 1 else res


ROWS = ((NB, LANES), F32)
PACKED = ((NB // 2, LANES), F32)
ROWS_SCRATCH = (pltpu.VMEM((NB, LANES), F32),)


def exchange(rows):
    k = rows.shape[0] // NB
    out = lax.all_to_all(rows.reshape(NB, 1, k * LANES), BLK, 0, 0, tiled=True)
    return out.reshape(NB * k, LANES)


def exchange_in_cube(rows):
    k = rows.shape[0] // 8
    return lax.all_to_all(rows.reshape(8, 1, k * LANES), CUBE, 0, 0, tiled=True).reshape(8 * k, LANES)


def over_group(rows):
    parts = [rows]
    for k in (1, 2, 3):
        parts.append(lax.ppermute(rows, GRP, [(i, i ^ k) for i in range(4)]))
    return parts


def steps(primal, dual, objective, lower, upper, bound_kind, rhs, row_kind, q_tiles, q_index, k_tiles, k_rows, k_cols):
    hess, cons = q_tiles, k_tiles
    me = lax.axis_index(GRP).astype(I32).reshape(1)

    def wide(v):
        return v.reshape(-1, LANES)

    inputs = (q_index[0], k_cols, k_rows, wide(primal), wide(objective), wide(lower), wide(upper), wide(bound_kind), wide(dual),
              wide(rhs), wide(row_kind))
    room = [(pltpu.SMEM if i < 3 else pltpu.VMEM)(v.shape, v.dtype) for i, v in enumerate(inputs)]
    first, block = call(start_kernel, [((FIRST * NB, LANES), F32), ((2 * NB + 8, LANES), F32)], me, *inputs, smem=1,
                        where=pltpu.HBM, scratch=room + [pltpu.SemaphoreType.DMA((len(inputs),))], limit=66800000)
    parts = over_group(block)
    got = exchange(first)
    four = ((4 * NB, LANES), F32)
    msg = call(first_gather_kernel, [((3 * NB, LANES), F32)], got)
    want = exchange(msg)
    wide_block = ((NB, 2 * LANES), F32)
    scalar = ((8, LANES), F32)
    cube = ((8 * 13, LANES), F32)
    grads = (pltpu.VMEM((104, LANES), F32),)
    y, b, kind, rel, take, hot, read, msg = call(
        first_products_kernel,
        [wide_block, wide_block, wide_block, ((32, LANES), I32), ((2 * LANES, LANES), BF16), ((208, NT * NB), BF16),
         four, ((5 * NB, LANES), F32)],
        want, got, *parts, hess, cons, scratch=ROWS_SCRATCH)
    msg = call(first_sum_kernel, [cube], exchange(msg), hot)
    own = [wide(v) for v in (objective, lower, upper, bound_kind)]
    own_x, read_x, prods = call(first_primal_kernel, [ROWS, ((4 * NT, LANES), F32), PACKED], exchange_in_cube(msg), *own, read,
                                wide(primal), cons, scratch=grads)
    parts = over_group(prods)
    hess_prod, put = call(hessian_kernel, [ROWS, ((4 * LANES, 2 * LANES), BF16)], read_x, rel, hess)
    y, msg = call(dual_kernel, [wide_block, ((6 * NB, LANES), F32)], *parts, put, take, y, b, kind, hess_prod, cons,
                  scratch=ROWS_SCRATCH)
    weight, msg = call(second_sum_kernel, [scalar, cube], exchange(msg), hot)
    final, prods = call(second_primal_kernel, [ROWS, PACKED], exchange_in_cube(msg), *own, read, own_x, read_x, weight, cons,
                        scratch=grads)
    parts = over_group(prods)
    y, msg = call(last_dual_kernel, [ROWS, ROWS], *parts, put, y, b, kind, weight)
    weight, dual_out, final = call(last_kernel, [((1, 1), F32), ((32, LANES), F32), ROWS], exchange(msg), y, final, weight)
    return final.reshape(-1), dual_out.reshape(-1), weight.reshape(())


def solution(mesh):
    finer = Mesh(mesh.devices.reshape(2, 2, 4, 2, 2, 2, 2), (*GRP, *BLK))
    placed = (P(BLK_GRP),) * 8 + (
        P(GRP, BLK, None, None),
        P(GRP, None, BLK),
        P(GRP, BLK, None, None),
        P(GRP, BLK),
        P(GRP, BLK),
    )
    return jax.shard_map(steps, mesh=finer, in_specs=placed, out_specs=(P(BLK_GRP), P(BLK_GRP), P()), check_vma=False)
```

```python
import jax
import jax.numpy as jnp
from jax import lax
from jax.experimental import pallas as pl
from jax.experimental.pallas import tpu as pltpu
from jax.sharding import Mesh
from jax.sharding import PartitionSpec as P

BLK = ("zh", "zl", "xh", "xl", "yl")
CUBE = ("zl", "xl", "yl")
GRP = ("grp_0", "grp_1")
BLK_GRP = (*BLK, *GRP)
EPSILON = 1e-06
STEP_SCALE = 0.5
F32, BF16, I32 = jnp.float32, jnp.bfloat16, jnp.int32

NB = 64
LANES = 128
NQ, NK = 4, 6
NT = NQ + NK
VMEM_LIMIT = 8 * 1024 * 1024
COST = 10000000000
FIRST, IDS = 5, 4
FREE = 1e38


def iota(shape, dim):
    return lax.broadcasted_iota(I32, shape, dim)


def lane(rows=NB):
    return iota((rows, LANES), 1)


def slot_of(lanes):
    return (lanes >> 2) & 15


def split(v, n):
    parts = []
    for _ in range(n - 1):
        p = v.astype(BF16)
        parts.append(p)
        v = v - p.astype(F32)
    parts.append(v.astype(BF16))
    return parts


def dot(a, b):
    return jnp.dot(a, b, preferred_element_type=F32)


def spread(v):
    return jnp.transpose(jnp.concatenate([v, pltpu.roll(v, 64, 1)], axis=0))[:NB]


def total(v):
    return jnp.sum(jnp.sum(v, axis=0, keepdims=True), axis=1, keepdims=True)


def along(v, idx):
    return jnp.take_along_axis(v, idx, axis=1)


def column(v, c):
    return jnp.broadcast_to(v[:, c : c + 1], v.shape)


def gather_tiles(ids, tables, out):
    ln = lane()
    slot = slot_of(ln)

    def index(tile):
        return (ln & 64) + along(ids & 15, tile) * 4 + (ln & 3)

    idx = [index(jnp.where(slot < NT, slot, slot - NT + n * (16 - NT))) for n in range(2)]
    owner = ids >> 4
    ones = []
    for j in range(NT):
        o = jnp.where((ln & 63) == column(owner, j), 1.0, 0.0).astype(BF16)
        ones.append(jnp.concatenate([o, o], axis=1))
    ones = jnp.concatenate(ones, axis=0)
    got = []
    for n in (0, 2):
        pieces = [jnp.concatenate([a, b], axis=1) for a, b in zip(split(tables[n], 3), split(tables[n + 1], 3))]
        both = dot(ones, jnp.concatenate([*pieces, jnp.zeros_like(pieces[0])], axis=0))
        got += [both[:, :LANES], both[:, LANES:]]
    for n in range(3):
        msg = jnp.zeros((NB, LANES), F32)
        for s in range(16):
            j = s if s < NT else s - NT + n * (16 - NT)
            if j < NT:
                table = got[n if s < NT else 3]
                msg = jnp.where(slot == s, along(table[j * NB : (j + 1) * NB], idx[n & 1]), msg)
        out[pl.ds(n, NB, stride=3), :] = msg


def cube_of(b):
    return ((b >> 3) & 1) * 4 + ((b >> 1) & 1) * 2 + (b & 1)


def send_rows(rows_ref, out, n, k):
    low = lane(n) < 64
    for q in range(4):
        a = rows_ref[pl.ds(q, n, stride=8), :]
        b = rows_ref[pl.ds(q + 4, n, stride=8), :]
        halves = (jnp.where(low, a, pltpu.roll(b, 64, 1)), jnp.where(low, pltpu.roll(a, 64, 1), b))
        for peer in range(NB):
            if cube_of(peer) >> 1 == q:
                out[peer * k : peer * k + n, :] = halves[cube_of(peer) & 1]


def wanted(got):
    base = lax.axis_index("zh") * 16 + lax.axis_index("xh") * 4
    ln = lane(8)
    sub = iota((8, LANES), 0)
    want = jnp.zeros((8, LANES), F32)
    for p in range(8):
        b = base + (p >> 2) * 8 + ((p >> 1) & 1) * 2 + (p & 1)
        want = jnp.where(sub == p, jnp.broadcast_to(got[pl.ds(b * FIRST + IDS, 1), :], (8, LANES)), want)
    member = base + ((sub >> 2) & 1) * 8 + ((sub >> 1) & 1) * 2 + (sub & 1)
    return jnp.where(ln < NT, want, (member * 16 + ln - NT).astype(F32))


def matches(want, row_of, n, m):
    low = lane(1) < 64
    sides = []
    for parity in range(2):
        chunks = []
        for c in range(n):
            a, b = (row_of(u % n, (u // n) ^ parity) for u in (2 * c, 2 * c + 1))
            row = jnp.where(low, a, b)
            hits = []
            for kk in range(m):
                w = jnp.broadcast_to(want[:, 2 * kk + parity : 2 * kk + parity + 1], (8, LANES))
                hits.append(jnp.where(w == row, 1.0, 0.0))
            chunks.append(jnp.concatenate(hits, axis=0))
        sides.append(jnp.concatenate(chunks, axis=1))
    return jnp.concatenate(sides, axis=0).astype(BF16)


def match_table(got):
    ids = got[pl.ds(IDS, NB, stride=FIRST), :]
    flat = jnp.transpose(jnp.concatenate([ids, ids], axis=0))

    def row_of(pair, odd):
        j = 2 * pair + odd
        r = NT + j if j < NQ else j
        return flat[r : r + 1]

    return matches(wanted(got), row_of, NT // 2, 13)


def sum_rows(msg, hot, out, n, m, k, skip=0):
    blocks = [msg[pl.ds(i, NB, stride=k), :] for i in range(n)]
    blocks += [pltpu.roll(v, 64, 1) for v in blocks]
    got = dot(hot, jnp.concatenate([jnp.concatenate(split(v, 2), axis=1) for v in blocks], axis=0))
    got = got[:, :LANES] + got[:, LANES:]
    left = lane(8) < 64
    for kk in range(skip, m):
        out[pl.ds(kk - skip, 8, stride=m - skip), :] = jnp.where(left, got[8 * kk : 8 * kk + 8], got[8 * (m + kk) : 8 * (m + kk) + 8])


def receive_rows(msg, rows, m, first=0):
    low = lane(m) < 64
    for q in range(4):
        a = msg[2 * m * q : 2 * m * q + m, :]
        b = msg[2 * m * q + m : 2 * m * q + 2 * m, :]
        rows[pl.ds(first + q, m, stride=8), :] = jnp.where(low, a, pltpu.roll(b, 64, 1))
        rows[pl.ds(first + q + 4, m, stride=8), :] = jnp.where(low, pltpu.roll(a, 64, 1), b)


def bounds(lower, upper, kind, free):
    return (
        jnp.where((kind == 1) | (kind == 2), lower, -free),
        jnp.where((kind == 2) | (kind == 3), upper, free),
    )


def forward_tiles(tiles_ref, rows_ref, count, first):
    ln = lane()
    out = jnp.zeros((NB, LANES), F32)
    for t in range(count):
        j = first + t
        vec = [rows_ref[4 * j + q : 4 * j + q + 1, :] for q in range(4)]
        for qo in range(4):
            for h in range(2):
                at = slice(qo * 128 + h * 64, qo * 128 + h * 64 + 64)
                p = tiles_ref[0, t, at, 0:128] * vec[0]
                for q in range(1, 4):
                    p = p + tiles_ref[0, t, at, q * 128 : (q + 1) * 128] * vec[q]
                out = jnp.where(ln == h * 64 + 4 * j + qo, jnp.sum(p, axis=1, keepdims=True), out)
    return out


def transposed_tiles(tiles_ref, cols, rows_ref, first):
    for t in range(NK):
        j = first + t
        acc = [jnp.zeros((8, LANES), F32) for _ in range(4)]
        for qo in range(4):
            for h in range(2):
                at = slice(qo * 128 + h * 64, qo * 128 + h * 64 + 64)
                v = along(cols, jnp.full((NB, LANES), h * 64 + 4 * j + qo, I32))
                for q in range(4):
                    p = tiles_ref[0, t, at, q * 128 : (q + 1) * 128] * v
                    acc[q] = acc[q] + jnp.sum(p.reshape(8, 8, LANES), axis=0)
        for q in range(4):
            rows_ref[4 * j + q : 4 * j + q + 1, :] = jnp.sum(acc[q], axis=0, keepdims=True)


def join(parts, part):
    low = (lane() & 32) == 0
    blocks = []
    for k in (0, 2):
        a, b = parts[k], parts[k + 1]
        if part == 0:
            blocks.append(jnp.where(low, a, pltpu.roll(b, 32, 1)))
        else:
            blocks.append(jnp.where(low, pltpu.roll(a, LANES - 32, 1), b))
    return jnp.concatenate(blocks, axis=1)


def pack(prods, extra):
    ln = lane(32)
    both = jnp.where((ln & 63) < 40, prods[:32], pltpu.roll(prods[32:], 24, 1))
    return jnp.where(ln == 0, extra, both)


def unpack(packed):
    return jnp.concatenate([packed, pltpu.roll(packed, LANES - 24, 1)], axis=0)


def dual_step(parts, hot, y, rhs, kind, step):
    high, low = [], []
    for p in parts:
        a, b = split(unpack(p), 2)
        high.append(a)
        low.append(b)
    extrap = dot(jnp.concatenate([jnp.concatenate(high, axis=1), jnp.concatenate(low, axis=1)], axis=0), hot)
    extrap = extrap[:NB] + extrap[NB:]
    new = y + step * (rhs - extrap)
    new = jnp.where(kind == 1.0, jnp.maximum(new, 0.0), new)
    moved = new - y
    return new, total(moved * moved)


def new_weight(weight, dual_sq, primal_sq):
    return jnp.sqrt(weight * jnp.sqrt((dual_sq + EPSILON) / (primal_sq + EPSILON)))


def spread_two(v, w):
    t = jnp.transpose(jnp.concatenate([v, w], axis=0))
    low = lane() < 64
    top, bottom = t[:NB], t[NB:]
    return jnp.where(low, top, pltpu.roll(bottom, 64, 1)), jnp.where(low, pltpu.roll(top, 64, 1), bottom)


def start_kernel(me, q_index, k_cols, k_rows, primal, objective, lower, upper, bound_kind, dual, rhs, row_kind, out, block, *scratch):
    refs = (q_index, k_cols, k_rows, primal, objective, lower, upper, bound_kind, dual, rhs, row_kind)
    sems = scratch[-1]
    copies = [pltpu.make_async_copy(r, s, sems.at[i]) for i, (r, s) in enumerate(zip(refs, scratch))]
    for c in copies:
        c.start()
    qi, kc, kr, p, ob, lo, up, bk, du, rh, rk = scratch[:-1]
    for c in copies:
        c.wait()
    low, high = bounds(lo[...], up[...], bk[...], FREE)
    for k, v in enumerate((*spread_two(p[...], ob[...]), *spread_two(low, high))):
        out[pl.ds(k, NB, stride=FIRST), :] = v
    ln = lane(8)
    ids = jnp.zeros((8, LANES), F32)
    for j in range(NQ):
        ids = jnp.where(ln == j, qi[1, j].astype(F32), ids)
        ids = jnp.where(ln == NT + j, qi[0, j].astype(F32), ids)
    for j in range(NK):
        ids = jnp.where(ln == NQ + j, kc[0, j].astype(F32), ids)
    out[pl.ds(IDS, NB, stride=FIRST), :] = jnp.broadcast_to(ids[:1], (NB, LANES))
    a, b = spread_two(
        jnp.concatenate([du[...], rh[...]], axis=0),
        jnp.concatenate([rk[...].astype(F32), jnp.zeros((32, LANES), F32)], axis=0),
    )
    block[0:NB] = a
    block[NB : 2 * NB] = b
    ids = jnp.zeros((8, LANES), F32)
    for j in range(NK):
        ids = jnp.where(slot_of(ln) == NQ + j, kr[0, j].astype(F32), ids)
    block[2 * NB :] = jnp.where(ln == 0, me[0].astype(F32), ids)


def first_gather_kernel(got, msg):
    ids = got[pl.ds(IDS, NB, stride=FIRST), :].astype(I32)
    gather_tiles(ids, [got[pl.ds(n, NB, stride=FIRST), :] for n in range(4)], msg)


def dual_tables(parts, y, rhs, kind, tiles, take):
    y[...] = join([p[0:NB] for p in parts], 0)
    rhs[...] = join([p[0:NB] for p in parts], 1)
    kind[...] = join([p[NB : 2 * NB] for p in parts], 0)
    mine = jnp.broadcast_to(parts[0][2 * NB :, 0:1], (8, LANES)).astype(I32)
    rel = []
    for p in parts:
        r = p[2 * NB :].astype(I32)
        rel.append((((r >> 3) ^ mine) << 3) | (r & 7))
    tiles[...] = jnp.concatenate(rel, axis=0)
    ln = lane(LANES)
    sub = iota((LANES, LANES), 0)
    r = jnp.broadcast_to(rel[0][:1], (LANES, LANES))
    lane_ok = (slot_of(ln) >= NQ) & (slot_of(ln) < NT)
    for kk in range(2):
        tile = (2 * kk + ((sub >> 5) & 1)) * 8 + ((sub >> 2) & 7)
        hit = ((ln & 64) == (sub & 64)) & ((ln & 3) == (sub & 3)) & lane_ok & (tile == r)
        take[kk * LANES : (kk + 1) * LANES, :] = jnp.where(hit, 1.0, 0.0).astype(BF16)


def put_table(tiles, put):
    ln = lane(LANES)
    sub = iota((LANES, LANES), 0)
    same = ((ln & 64) == (sub & 64)) & ((ln & 3) == (sub & 3)) & (slot_of(sub) >= NQ) & (slot_of(sub) < NT)
    for p in range(4):
        r = jnp.transpose(jnp.broadcast_to(tiles[8 * p : 8 * p + 1].astype(F32), (LANES, LANES))).astype(I32)
        for kk in range(2):
            tile = (2 * kk + ((ln >> 5) & 1)) * 8 + ((ln >> 2) & 7)
            put[p * LANES : (p + 1) * LANES, kk * LANES : (kk + 1) * LANES] = jnp.where(same & (tile == r), 1.0, 0.0).astype(BF16)


def take_rows(y, take):
    got = dot(jnp.concatenate(split(y, 2), axis=0), take)
    return got[:NB] + got[NB:]


def first_products_kernel(msg, got, p0, p1, p2, p3, hess, cons, y, rhs, kind, tiles, take, hot, read, out, rows):
    hot[...] = match_table(got)
    dual_tables([p0, p1, p2, p3], y, rhs, kind, tiles, take)
    m = [msg[pl.ds(n, NB, stride=3), :] for n in range(3)]
    m = (*spread_two(m[0], m[1]), spread(m[2]))
    for n in range(3):
        read[n * NB : (n + 1) * NB] = m[n]
    read[3 * NB : 3 * NB + 24] = m[0][40:64]
    read[3 * NB + 24 : 3 * NB + 40] = m[1][40:56]
    read[3 * NB + 40 : 4 * NB] = jnp.zeros((24, LANES), F32)
    first = spread(forward_tiles(hess, read, NQ, 0))
    transposed_tiles(cons, take_rows(y[...], take[...]), rows, NQ)
    rows[0 : 4 * NQ] = first[0 : 4 * NQ]
    rows[4 * NQ : 4 * NT] = -rows[4 * NQ : 4 * NT]
    send_rows(rows, out, 5, 5)


def first_sum_kernel(msg, hot, out):
    sum_rows(msg, hot[...], out, 5, 13, 5)


def second_sum_kernel(msg, hot, weight, out):
    sum_rows(msg, hot[...], out, 5, 13, 6, 2)
    tail = jnp.sum(msg[pl.ds(5, NB, stride=6), :], axis=0, keepdims=True)
    weight[...] = jnp.broadcast_to(new_weight(jnp.ones((1, 1), F32), tail[:, 1:2], tail[:, 0:1]), (8, LANES))


def primal_step(grads, own, read, own_x, read_x, tau, own_out, rows):
    skip = 13 - grads.shape[0] // 8
    if skip:
        rows[0 : 8 * skip] = jnp.zeros((8 * skip, LANES), F32)
    receive_rows(grads, rows, 13 - skip, 8 * skip)
    c, low, high, kind = own
    x = own_x[...]
    low, high = bounds(low[...], high[...], kind[...], jnp.inf)
    new = jnp.minimum(jnp.maximum(x - tau * (rows[4 * NT :] + c[...]), low), high)
    own_out[...] = new
    moved = new - x
    c, low, high = (read[k * NB : k * NB + 4 * NT] for k in range(1, 4))
    x = read_x[0 : 4 * NT]
    new = jnp.minimum(jnp.maximum(x - tau * (rows[0 : 4 * NT] + c), low), high)
    rows[0 : 4 * NT] = 2.0 * new - x
    return new, total(moved * moved)


def first_primal_kernel(grads, c, low, high, kind, read, own_x, tiles, own_out, read_out, out, rows):
    new, moved = primal_step(grads, (c, low, high, kind), read, own_x, read, jnp.full((1, 1), STEP_SCALE, F32), own_out, rows)
    read_out[0 : 4 * NT] = new
    out[...] = pack(forward_tiles(tiles, rows, NK, NQ), moved)


def second_primal_kernel(grads, c, low, high, kind, read, own_x, read_x, weight, tiles, own_out, out, rows):
    tau = STEP_SCALE / weight[0:1, 0:1]
    _, moved = primal_step(grads, (c, low, high, kind), read, own_x, read_x, tau, own_out, rows)
    out[...] = pack(forward_tiles(tiles, rows, NK, NQ), moved)


def hessian_kernel(vec, rel, tiles, out, put):
    out[...] = spread(forward_tiles(tiles, vec, NQ, 0))
    put_table(rel, put)


def primal_total(parts):
    s = parts[0][0:1, 0:1]
    for p in parts[1:]:
        s = s + p[0:1, 0:1]
    return s


def dual_kernel(p0, p1, p2, p3, put, take, y, rhs, kind, hess, tiles, y_out, out, rows):
    parts = [p[...] for p in (p0, p1, p2, p3)]
    new, moved = dual_step(parts, put[...], y[...], rhs[...], kind[...], STEP_SCALE)
    y_out[...] = new
    transposed_tiles(tiles, take_rows(new, take[...]), rows, NQ)
    rows[0 : 4 * NQ] = hess[0 : 4 * NQ]
    rows[4 * NQ : 4 * NT] = -rows[4 * NQ : 4 * NT]
    send_rows(rows, out, 5, 6)
    out[pl.ds(5, NB, stride=6), :] = jnp.where(lane() == 0, primal_total(parts), moved)


def last_dual_kernel(p0, p1, p2, p3, put, y, rhs, kind, weight, y_out, out):
    parts = [p[...] for p in (p0, p1, p2, p3)]
    new, moved = dual_step(parts, put[...], y[...], rhs[...], kind[...], STEP_SCALE * weight[0:1, 0:1])
    y_out[...] = new[:, :LANES]
    out[...] = jnp.where(lane() == 0, primal_total(parts), moved)


def last_kernel(msg, y, x, weight, out, dual_out, final):
    tail = jnp.sum(msg[...], axis=0, keepdims=True)
    out[...] = new_weight(weight[0:1, 0:1], tail[:, 1:2], tail[:, 0:1])
    dual_out[...] = spread(y[...])[:32]
    final[...] = x[...]


def call(kernel, outs, *args, smem=0, scratch=(), cost=COST, where=pltpu.VMEM, limit=VMEM_LIMIT):
    v = pl.BlockSpec(memory_space=pltpu.VMEM)
    w = pl.BlockSpec(memory_space=where)
    s = pl.BlockSpec(memory_space=pltpu.SMEM)
    shapes = [jax.ShapeDtypeStruct(*o) for o in outs]
    res = pl.pallas_call(
        kernel,
        out_shape=shapes,
        in_specs=[s] * smem + [w] * (len(args) - smem),
        out_specs=[v] * len(shapes),
        scratch_shapes=list(scratch),
        compiler_params=pltpu.CompilerParams(vmem_limit_bytes=limit),
        cost_estimate=pl.CostEstimate(flops=cost, bytes_accessed=10000000, transcendentals=0),
    )(*args)
    return res[0] if len(outs) == 1 else res


ROWS = ((NB, LANES), F32)
PACKED = ((NB // 2, LANES), F32)
ROWS_SCRATCH = (pltpu.VMEM((NB, LANES), F32),)


def exchange(rows):
    k = rows.shape[0] // NB
    out = lax.all_to_all(rows.reshape(NB, 1, k * LANES), BLK, 0, 0, tiled=True)
    return out.reshape(NB * k, LANES)


def exchange_in_cube(rows):
    k = rows.shape[0] // 8
    return lax.all_to_all(rows.reshape(8, 1, k * LANES), CUBE, 0, 0, tiled=True).reshape(8 * k, LANES)


def over_group(rows):
    parts = [rows]
    for k in (1, 2, 3):
        parts.append(lax.ppermute(rows, GRP, [(i, i ^ k) for i in range(4)]))
    return parts


def steps(primal, dual, objective, lower, upper, bound_kind, rhs, row_kind, q_tiles, q_index, k_tiles, k_rows, k_cols):
    hess, cons = q_tiles, k_tiles
    me = lax.axis_index(GRP).astype(I32).reshape(1)

    def wide(v):
        return v.reshape(-1, LANES)

    inputs = (q_index[0], k_cols, k_rows, wide(primal), wide(objective), wide(lower), wide(upper), wide(bound_kind), wide(dual),
              wide(rhs), wide(row_kind))
    room = [(pltpu.SMEM if i < 3 else pltpu.VMEM)(v.shape, v.dtype) for i, v in enumerate(inputs)]
    first, block = call(start_kernel, [((FIRST * NB, LANES), F32), ((2 * NB + 8, LANES), F32)], me, *inputs, smem=1,
                        where=pltpu.HBM, scratch=room + [pltpu.SemaphoreType.DMA((len(inputs),))], limit=66800000)
    parts = over_group(block)
    got = exchange(first)
    four = ((4 * NB, LANES), F32)
    msg = call(first_gather_kernel, [((3 * NB, LANES), F32)], got)
    want = exchange(msg)
    wide_block = ((NB, 2 * LANES), F32)
    scalar = ((8, LANES), F32)
    cube = ((8 * 13, LANES), F32)
    grads = (pltpu.VMEM((104, LANES), F32),)
    y, b, kind, rel, take, hot, read, msg = call(
        first_products_kernel,
        [wide_block, wide_block, wide_block, ((32, LANES), I32), ((2 * LANES, LANES), BF16), ((208, NT * NB), BF16),
         four, ((5 * NB, LANES), F32)],
        want, got, *parts, hess, cons, scratch=ROWS_SCRATCH)
    msg = call(first_sum_kernel, [cube], exchange(msg), hot)
    own = [wide(v) for v in (objective, lower, upper, bound_kind)]
    own_x, read_x, prods = call(first_primal_kernel, [ROWS, ((4 * NT, LANES), F32), PACKED], exchange_in_cube(msg), *own, read,
                                wide(primal), cons, scratch=grads)
    parts = over_group(prods)
    hess_prod, put = call(hessian_kernel, [ROWS, ((4 * LANES, 2 * LANES), BF16)], read_x, rel, hess)
    y, msg = call(dual_kernel, [wide_block, ((6 * NB, LANES), F32)], *parts, put, take, y, b, kind, hess_prod, cons,
                  scratch=ROWS_SCRATCH)
    weight, msg = call(second_sum_kernel, [scalar, ((8 * 11, LANES), F32)], exchange(msg), hot)
    final, prods = call(second_primal_kernel, [ROWS, PACKED], exchange_in_cube(msg), *own, read, own_x, read_x, weight, cons,
                        scratch=grads)
    parts = over_group(prods)
    y, msg = call(last_dual_kernel, [ROWS, ROWS], *parts, put, y, b, kind, weight)
    weight, dual_out, final = call(last_kernel, [((1, 1), F32), ((32, LANES), F32), ROWS], exchange(msg), y, final, weight)
    return final.reshape(-1), dual_out.reshape(-1), weight.reshape(())


def solution(mesh):
    finer = Mesh(mesh.devices.reshape(2, 2, 4, 2, 2, 2, 2), (*GRP, *BLK))
    placed = (P(BLK_GRP),) * 8 + (
        P(GRP, BLK, None, None),
        P(GRP, None, BLK),
        P(GRP, BLK, None, None),
        P(GRP, BLK),
        P(GRP, BLK),
    )
    return jax.shard_map(steps, mesh=finer, in_specs=placed, out_specs=(P(BLK_GRP), P(BLK_GRP), P()), check_vma=False)
```

```python
import jax
import jax.numpy as jnp
from jax import lax
from jax.experimental import pallas as pl
from jax.experimental.pallas import tpu as pltpu
from jax.sharding import Mesh
from jax.sharding import PartitionSpec as P

BLK = ("zh", "zl", "xh", "xl", "yl")
CUBE = ("zl", "xl", "yl")
GRP = ("grp_0", "grp_1")
BLK_GRP = (*BLK, *GRP)
EPSILON = 1e-06
STEP_SCALE = 0.5
F32, BF16, I32 = jnp.float32, jnp.bfloat16, jnp.int32

NB = 64
LANES = 128
NQ, NK = 4, 6
NT = NQ + NK
VMEM_LIMIT = 8 * 1024 * 1024
COST = 10000000000
FIRST, IDS = 5, 4
FREE = 1e38


def iota(shape, dim):
    return lax.broadcasted_iota(I32, shape, dim)


def lane(rows=NB):
    return iota((rows, LANES), 1)


def slot_of(lanes):
    return (lanes >> 2) & 15


def split(v, n):
    parts = []
    for _ in range(n - 1):
        p = v.astype(BF16)
        parts.append(p)
        v = v - p.astype(F32)
    parts.append(v.astype(BF16))
    return parts


def dot(a, b):
    return jnp.dot(a, b, preferred_element_type=F32)


def spread(v):
    return jnp.transpose(jnp.concatenate([v, pltpu.roll(v, 64, 1)], axis=0))[:NB]


def total(v):
    return jnp.sum(jnp.sum(v, axis=0, keepdims=True), axis=1, keepdims=True)


def along(v, idx):
    return jnp.take_along_axis(v, idx, axis=1)


def column(v, c):
    return jnp.broadcast_to(v[:, c : c + 1], v.shape)


def gather_tiles(ids, tables, out):
    ln = lane()
    slot = slot_of(ln)

    def index(tile):
        return (ln & 64) + along(ids & 15, tile) * 4 + (ln & 3)

    idx = [index(jnp.where(slot < NT, slot, slot - NT + n * (16 - NT))) for n in range(2)]
    owner = ids >> 4
    ones = []
    for j in range(NT):
        o = jnp.where((ln & 63) == column(owner, j), 1.0, 0.0).astype(BF16)
        ones.append(jnp.concatenate([o, o], axis=1))
    ones = jnp.concatenate(ones, axis=0)
    got = []
    for n in (0, 2):
        pieces = [jnp.concatenate([a, b], axis=1) for a, b in zip(split(tables[n], 3), split(tables[n + 1], 3))]
        both = dot(ones, jnp.concatenate([*pieces, jnp.zeros_like(pieces[0])], axis=0))
        got += [both[:, :LANES], both[:, LANES:]]
    for n in range(3):
        msg = jnp.zeros((NB, LANES), F32)
        for s in range(16):
            j = s if s < NT else s - NT + n * (16 - NT)
            if j < NT:
                table = got[n if s < NT else 3]
                msg = jnp.where(slot == s, along(table[j * NB : (j + 1) * NB], idx[n & 1]), msg)
        out[pl.ds(n, NB, stride=3), :] = msg


def cube_of(b):
    return ((b >> 3) & 1) * 4 + ((b >> 1) & 1) * 2 + (b & 1)


def send_rows(rows_ref, out, n, k):
    low = lane(n) < 64
    for q in range(4):
        a = rows_ref[pl.ds(q, n, stride=8), :]
        b = rows_ref[pl.ds(q + 4, n, stride=8), :]
        halves = (jnp.where(low, a, pltpu.roll(b, 64, 1)), jnp.where(low, pltpu.roll(a, 64, 1), b))
        for peer in range(NB):
            if cube_of(peer) >> 1 == q:
                out[peer * k : peer * k + n, :] = halves[cube_of(peer) & 1]


def wanted(got):
    base = lax.axis_index("zh") * 16 + lax.axis_index("xh") * 4
    ln = lane(8)
    sub = iota((8, LANES), 0)
    want = jnp.zeros((8, LANES), F32)
    for p in range(8):
        b = base + (p >> 2) * 8 + ((p >> 1) & 1) * 2 + (p & 1)
        want = jnp.where(sub == p, jnp.broadcast_to(got[pl.ds(b * FIRST + IDS, 1), :], (8, LANES)), want)
    member = base + ((sub >> 2) & 1) * 8 + ((sub >> 1) & 1) * 2 + (sub & 1)
    return jnp.where(ln < NT, want, (member * 16 + ln - NT).astype(F32))


def matches(want, row_of, n, m):
    low = lane(1) < 64
    sides = []
    for parity in range(2):
        chunks = []
        for c in range(n):
            a, b = (row_of(u % n, (u // n) ^ parity) for u in (2 * c, 2 * c + 1))
            row = jnp.where(low, a, b)
            hits = []
            for kk in range(m):
                w = jnp.broadcast_to(want[:, 2 * kk + parity : 2 * kk + parity + 1], (8, LANES))
                hits.append(jnp.where(w == row, 1.0, 0.0))
            chunks.append(jnp.concatenate(hits, axis=0))
        sides.append(jnp.concatenate(chunks, axis=1))
    return jnp.concatenate(sides, axis=0).astype(BF16)


def match_table(got):
    ids = got[pl.ds(IDS, NB, stride=FIRST), :]
    flat = jnp.transpose(jnp.concatenate([ids, ids], axis=0))

    def row_of(pair, odd):
        j = 2 * pair + odd
        r = NT + j if j < NQ else j
        return flat[r : r + 1]

    return matches(wanted(got), row_of, NT // 2, 13)


def sum_rows(msg, hot, out, n, m, k):
    blocks = [msg[pl.ds(i, NB, stride=k), :] for i in range(n)]
    blocks += [pltpu.roll(v, 64, 1) for v in blocks]
    got = dot(hot, jnp.concatenate([jnp.concatenate(split(v, 2), axis=1) for v in blocks], axis=0))
    got = got[:, :LANES] + got[:, LANES:]
    left = lane(8) < 64
    for kk in range(m):
        out[pl.ds(kk, 8, stride=m), :] = jnp.where(left, got[8 * kk : 8 * kk + 8], got[8 * (m + kk) : 8 * (m + kk) + 8])


def receive_rows(msg, rows, m):
    low = lane(m) < 64
    for q in range(4):
        a = msg[2 * m * q : 2 * m * q + m, :]
        b = msg[2 * m * q + m : 2 * m * q + 2 * m, :]
        rows[pl.ds(q, m, stride=8), :] = jnp.where(low, a, pltpu.roll(b, 64, 1))
        rows[pl.ds(q + 4, m, stride=8), :] = jnp.where(low, pltpu.roll(a, 64, 1), b)


def bounds(lower, upper, kind, free):
    return (
        jnp.where((kind == 1) | (kind == 2), lower, -free),
        jnp.where((kind == 2) | (kind == 3), upper, free),
    )


def forward_tiles(tiles_ref, rows_ref, count, first):
    ln = lane()
    out = jnp.zeros((NB, LANES), F32)
    for t in range(count):
        j = first + t
        vec = [rows_ref[4 * j + q : 4 * j + q + 1, :] for q in range(4)]
        for qo in range(4):
            for h in range(2):
                at = slice(qo * 128 + h * 64, qo * 128 + h * 64 + 64)
                p = tiles_ref[0, t, at, 0:128] * vec[0]
                for q in range(1, 4):
                    p = p + tiles_ref[0, t, at, q * 128 : (q + 1) * 128] * vec[q]
                out = jnp.where(ln == h * 64 + 4 * j + qo, jnp.sum(p, axis=1, keepdims=True), out)
    return out


def transposed_tiles(tiles_ref, cols, rows_ref, first):
    for t in range(NK):
        j = first + t
        acc = [jnp.zeros((8, LANES), F32) for _ in range(4)]
        for qo in range(4):
            for h in range(2):
                at = slice(qo * 128 + h * 64, qo * 128 + h * 64 + 64)
                v = along(cols, jnp.full((NB, LANES), h * 64 + 4 * j + qo, I32))
                for q in range(4):
                    p = tiles_ref[0, t, at, q * 128 : (q + 1) * 128] * v
                    acc[q] = acc[q] + jnp.sum(p.reshape(8, 8, LANES), axis=0)
        for q in range(4):
            rows_ref[4 * j + q : 4 * j + q + 1, :] = jnp.sum(acc[q], axis=0, keepdims=True)


def join(parts, part):
    low = (lane() & 32) == 0
    blocks = []
    for k in (0, 2):
        a, b = parts[k], parts[k + 1]
        if part == 0:
            blocks.append(jnp.where(low, a, pltpu.roll(b, 32, 1)))
        else:
            blocks.append(jnp.where(low, pltpu.roll(a, LANES - 32, 1), b))
    return jnp.concatenate(blocks, axis=1)


def pack(prods, extra):
    ln = lane(32)
    both = jnp.where((ln & 63) < 40, prods[:32], pltpu.roll(prods[32:], 24, 1))
    return jnp.where(ln == 0, extra, both)


def unpack(packed):
    return jnp.concatenate([packed, pltpu.roll(packed, LANES - 24, 1)], axis=0)


def dual_step(parts, hot, y, rhs, kind, step):
    high, low = [], []
    for p in parts:
        a, b = split(unpack(p), 2)
        high.append(a)
        low.append(b)
    extrap = dot(jnp.concatenate([jnp.concatenate(high, axis=1), jnp.concatenate(low, axis=1)], axis=0), hot)
    extrap = extrap[:NB] + extrap[NB:]
    new = y + step * (rhs - extrap)
    new = jnp.where(kind == 1.0, jnp.maximum(new, 0.0), new)
    moved = new - y
    return new, total(moved * moved)


def new_weight(weight, dual_sq, primal_sq):
    return jnp.sqrt(weight * jnp.sqrt((dual_sq + EPSILON) / (primal_sq + EPSILON)))


def spread_two(v, w):
    t = jnp.transpose(jnp.concatenate([v, w], axis=0))
    low = lane() < 64
    top, bottom = t[:NB], t[NB:]
    return jnp.where(low, top, pltpu.roll(bottom, 64, 1)), jnp.where(low, pltpu.roll(top, 64, 1), bottom)


def start_kernel(me, q_index, k_cols, k_rows, primal, objective, lower, upper, bound_kind, dual, rhs, row_kind, out, block, *scratch):
    refs = (q_index, k_cols, k_rows, primal, objective, lower, upper, bound_kind, dual, rhs, row_kind)
    sems = scratch[-1]
    copies = [pltpu.make_async_copy(r, s, sems.at[i]) for i, (r, s) in enumerate(zip(refs, scratch))]
    for i in (3, 4, 5, 6, 7, 8, 9, 10, 0, 1, 2):
        copies[i].start()
    qi, kc, kr, p, ob, lo, up, bk, du, rh, rk = scratch[:-1]
    for i in (3, 4, 5, 6, 7):
        copies[i].wait()
    low, high = bounds(lo[...], up[...], bk[...], FREE)
    for k, v in enumerate((*spread_two(p[...], ob[...]), *spread_two(low, high))):
        out[pl.ds(k, NB, stride=FIRST), :] = v
    for i in (0, 1, 2, 8, 9, 10):
        copies[i].wait()
    ln = lane(8)
    ids = jnp.zeros((8, LANES), F32)
    for j in range(NQ):
        ids = jnp.where(ln == j, qi[1, j].astype(F32), ids)
        ids = jnp.where(ln == NT + j, qi[0, j].astype(F32), ids)
    for j in range(NK):
        ids = jnp.where(ln == NQ + j, kc[0, j].astype(F32), ids)
    out[pl.ds(IDS, NB, stride=FIRST), :] = jnp.broadcast_to(ids[:1], (NB, LANES))
    a, b = spread_two(
        jnp.concatenate([du[...], rh[...]], axis=0),
        jnp.concatenate([rk[...].astype(F32), jnp.zeros((32, LANES), F32)], axis=0),
    )
    block[0:NB] = a
    block[NB : 2 * NB] = b
    ids = jnp.zeros((8, LANES), F32)
    for j in range(NK):
        ids = jnp.where(slot_of(ln) == NQ + j, kr[0, j].astype(F32), ids)
    block[2 * NB :] = jnp.where(ln == 0, me[0].astype(F32), ids)


def first_gather_kernel(got, msg):
    ids = got[pl.ds(IDS, NB, stride=FIRST), :].astype(I32)
    gather_tiles(ids, [got[pl.ds(n, NB, stride=FIRST), :] for n in range(4)], msg)


def dual_tables(parts, y, rhs, kind, tiles, take):
    y[...] = join([p[0:NB] for p in parts], 0)
    rhs[...] = join([p[0:NB] for p in parts], 1)
    kind[...] = join([p[NB : 2 * NB] for p in parts], 0)
    mine = jnp.broadcast_to(parts[0][2 * NB :, 0:1], (8, LANES)).astype(I32)
    rel = []
    for p in parts:
        r = p[2 * NB :].astype(I32)
        rel.append((((r >> 3) ^ mine) << 3) | (r & 7))
    tiles[...] = jnp.concatenate(rel, axis=0)
    ln = lane(LANES)
    sub = iota((LANES, LANES), 0)
    r = jnp.broadcast_to(rel[0][:1], (LANES, LANES))
    lane_ok = (slot_of(ln) >= NQ) & (slot_of(ln) < NT)
    for kk in range(2):
        tile = (2 * kk + ((sub >> 5) & 1)) * 8 + ((sub >> 2) & 7)
        hit = ((ln & 64) == (sub & 64)) & ((ln & 3) == (sub & 3)) & lane_ok & (tile == r)
        take[kk * LANES : (kk + 1) * LANES, :] = jnp.where(hit, 1.0, 0.0).astype(BF16)


def put_table(tiles, put):
    ln = lane(LANES)
    sub = iota((LANES, LANES), 0)
    same = ((ln & 64) == (sub & 64)) & ((ln & 3) == (sub & 3)) & (slot_of(sub) >= NQ) & (slot_of(sub) < NT)
    for p in range(4):
        r = jnp.transpose(jnp.broadcast_to(tiles[8 * p : 8 * p + 1].astype(F32), (LANES, LANES))).astype(I32)
        for kk in range(2):
            tile = (2 * kk + ((ln >> 5) & 1)) * 8 + ((ln >> 2) & 7)
            put[p * LANES : (p + 1) * LANES, kk * LANES : (kk + 1) * LANES] = jnp.where(same & (tile == r), 1.0, 0.0).astype(BF16)


def take_rows(y, take):
    got = dot(jnp.concatenate(split(y, 2), axis=0), take)
    return got[:NB] + got[NB:]


def first_products_kernel(msg, got, p0, p1, p2, p3, hess, cons, y, rhs, kind, tiles, take, hot, read, out, rows):
    hot[...] = match_table(got)
    dual_tables([p0, p1, p2, p3], y, rhs, kind, tiles, take)
    m = [msg[pl.ds(n, NB, stride=3), :] for n in range(3)]
    m = (*spread_two(m[0], m[1]), spread(m[2]))
    for n in range(3):
        read[n * NB : (n + 1) * NB] = m[n]
    read[3 * NB : 3 * NB + 24] = m[0][40:64]
    read[3 * NB + 24 : 3 * NB + 40] = m[1][40:56]
    read[3 * NB + 40 : 4 * NB] = jnp.zeros((24, LANES), F32)
    first = spread(forward_tiles(hess, read, NQ, 0))
    transposed_tiles(cons, take_rows(y[...], take[...]), rows, NQ)
    rows[0 : 4 * NQ] = first[0 : 4 * NQ]
    rows[4 * NQ : 4 * NT] = -rows[4 * NQ : 4 * NT]
    send_rows(rows, out, 5, 5)


def first_sum_kernel(msg, hot, out):
    sum_rows(msg, hot[...], out, 5, 13, 5)


def second_sum_kernel(msg, hot, weight, out):
    sum_rows(msg, hot[...], out, 5, 13, 6)
    tail = jnp.sum(msg[pl.ds(5, NB, stride=6), :], axis=0, keepdims=True)
    weight[...] = jnp.broadcast_to(new_weight(jnp.ones((1, 1), F32), tail[:, 1:2], tail[:, 0:1]), (8, LANES))


def primal_step(grads, own, read, own_x, read_x, tau, own_out, rows):
    receive_rows(grads, rows, 13)
    c, low, high, kind = own
    x = own_x[...]
    low, high = bounds(low[...], high[...], kind[...], jnp.inf)
    new = jnp.minimum(jnp.maximum(x - tau * (rows[4 * NT :] + c[...]), low), high)
    own_out[...] = new
    moved = new - x
    c, low, high = (read[k * NB : k * NB + 4 * NT] for k in range(1, 4))
    x = read_x[0 : 4 * NT]
    new = jnp.minimum(jnp.maximum(x - tau * (rows[0 : 4 * NT] + c), low), high)
    rows[0 : 4 * NT] = 2.0 * new - x
    return new, total(moved * moved)


def first_primal_kernel(grads, c, low, high, kind, read, own_x, tiles, own_out, read_out, out, rows):
    new, moved = primal_step(grads, (c, low, high, kind), read, own_x, read, jnp.full((1, 1), STEP_SCALE, F32), own_out, rows)
    read_out[0 : 4 * NT] = new
    out[...] = pack(forward_tiles(tiles, rows, NK, NQ), moved)


def second_primal_kernel(grads, c, low, high, kind, read, own_x, read_x, weight, tiles, own_out, out, rows):
    tau = STEP_SCALE / weight[0:1, 0:1]
    _, moved = primal_step(grads, (c, low, high, kind), read, own_x, read_x, tau, own_out, rows)
    out[...] = pack(forward_tiles(tiles, rows, NK, NQ), moved)


def hessian_kernel(vec, rel, tiles, out, put):
    out[...] = spread(forward_tiles(tiles, vec, NQ, 0))
    put_table(rel, put)


def primal_total(parts):
    s = parts[0][0:1, 0:1]
    for p in parts[1:]:
        s = s + p[0:1, 0:1]
    return s


def dual_kernel(p0, p1, p2, p3, put, take, y, rhs, kind, hess, tiles, y_out, out, rows):
    parts = [p[...] for p in (p0, p1, p2, p3)]
    new, moved = dual_step(parts, put[...], y[...], rhs[...], kind[...], STEP_SCALE)
    y_out[...] = new
    transposed_tiles(tiles, take_rows(new, take[...]), rows, NQ)
    rows[0 : 4 * NQ] = hess[0 : 4 * NQ]
    rows[4 * NQ : 4 * NT] = -rows[4 * NQ : 4 * NT]
    send_rows(rows, out, 5, 6)
    out[pl.ds(5, NB, stride=6), :] = jnp.where(lane() == 0, primal_total(parts), moved)


def last_dual_kernel(p0, p1, p2, p3, put, y, rhs, kind, weight, y_out, out):
    parts = [p[...] for p in (p0, p1, p2, p3)]
    new, moved = dual_step(parts, put[...], y[...], rhs[...], kind[...], STEP_SCALE * weight[0:1, 0:1])
    y_out[...] = new[:, :LANES]
    out[...] = jnp.where(lane() == 0, primal_total(parts), moved)


def last_kernel(msg, y, x, weight, out, dual_out, final):
    tail = jnp.sum(msg[...], axis=0, keepdims=True)
    out[...] = new_weight(weight[0:1, 0:1], tail[:, 1:2], tail[:, 0:1])
    dual_out[...] = spread(y[...])[:32]
    final[...] = x[...]


def call(kernel, outs, *args, smem=0, scratch=(), cost=COST, where=pltpu.VMEM, limit=VMEM_LIMIT):
    v = pl.BlockSpec(memory_space=pltpu.VMEM)
    w = pl.BlockSpec(memory_space=where)
    s = pl.BlockSpec(memory_space=pltpu.SMEM)
    shapes = [jax.ShapeDtypeStruct(*o) for o in outs]
    res = pl.pallas_call(
        kernel,
        out_shape=shapes,
        in_specs=[s] * smem + [w] * (len(args) - smem),
        out_specs=[v] * len(shapes),
        scratch_shapes=list(scratch),
        compiler_params=pltpu.CompilerParams(vmem_limit_bytes=limit),
        cost_estimate=pl.CostEstimate(flops=cost, bytes_accessed=10000000, transcendentals=0),
    )(*args)
    return res[0] if len(outs) == 1 else res


ROWS = ((NB, LANES), F32)
PACKED = ((NB // 2, LANES), F32)
ROWS_SCRATCH = (pltpu.VMEM((NB, LANES), F32),)


def exchange(rows):
    k = rows.shape[0] // NB
    out = lax.all_to_all(rows.reshape(NB, 1, k * LANES), BLK, 0, 0, tiled=True)
    return out.reshape(NB * k, LANES)


def exchange_in_cube(rows):
    k = rows.shape[0] // 8
    return lax.all_to_all(rows.reshape(8, 1, k * LANES), CUBE, 0, 0, tiled=True).reshape(8 * k, LANES)


def over_group(rows):
    parts = [rows]
    for k in (1, 2, 3):
        parts.append(lax.ppermute(rows, GRP, [(i, i ^ k) for i in range(4)]))
    return parts


def steps(primal, dual, objective, lower, upper, bound_kind, rhs, row_kind, q_tiles, q_index, k_tiles, k_rows, k_cols):
    hess, cons = q_tiles, k_tiles
    me = lax.axis_index(GRP).astype(I32).reshape(1)

    def wide(v):
        return v.reshape(-1, LANES)

    inputs = (q_index[0], k_cols, k_rows, wide(primal), wide(objective), wide(lower), wide(upper), wide(bound_kind), wide(dual),
              wide(rhs), wide(row_kind))
    room = [(pltpu.SMEM if i < 3 else pltpu.VMEM)(v.shape, v.dtype) for i, v in enumerate(inputs)]
    first, block = call(start_kernel, [((FIRST * NB, LANES), F32), ((2 * NB + 8, LANES), F32)], me, *inputs, smem=1,
                        where=pltpu.HBM, scratch=room + [pltpu.SemaphoreType.DMA((len(inputs),))], limit=66800000)
    parts = over_group(block)
    got = exchange(first)
    four = ((4 * NB, LANES), F32)
    msg = call(first_gather_kernel, [((3 * NB, LANES), F32)], got)
    want = exchange(msg)
    wide_block = ((NB, 2 * LANES), F32)
    scalar = ((8, LANES), F32)
    cube = ((8 * 13, LANES), F32)
    grads = (pltpu.VMEM((104, LANES), F32),)
    y, b, kind, rel, take, hot, read, msg = call(
        first_products_kernel,
        [wide_block, wide_block, wide_block, ((32, LANES), I32), ((2 * LANES, LANES), BF16), ((208, NT * NB), BF16),
         four, ((5 * NB, LANES), F32)],
        want, got, *parts, hess, cons, scratch=ROWS_SCRATCH)
    msg = call(first_sum_kernel, [cube], exchange(msg), hot)
    own = [wide(v) for v in (objective, lower, upper, bound_kind)]
    own_x, read_x, prods = call(first_primal_kernel, [ROWS, ((4 * NT, LANES), F32), PACKED], exchange_in_cube(msg), *own, read,
                                wide(primal), cons, scratch=grads)
    parts = over_group(prods)
    hess_prod, put = call(hessian_kernel, [ROWS, ((4 * LANES, 2 * LANES), BF16)], read_x, rel, hess)
    y, msg = call(dual_kernel, [wide_block, ((6 * NB, LANES), F32)], *parts, put, take, y, b, kind, hess_prod, cons,
                  scratch=ROWS_SCRATCH)
    weight, msg = call(second_sum_kernel, [scalar, cube], exchange(msg), hot)
    final, prods = call(second_primal_kernel, [ROWS, PACKED], exchange_in_cube(msg), *own, read, own_x, read_x, weight, cons,
                        scratch=grads)
    parts = over_group(prods)
    y, msg = call(last_dual_kernel, [ROWS, ROWS], *parts, put, y, b, kind, weight)
    weight, dual_out, final = call(last_kernel, [((1, 1), F32), ((32, LANES), F32), ROWS], exchange(msg), y, final, weight)
    return final.reshape(-1), dual_out.reshape(-1), weight.reshape(())


def solution(mesh):
    finer = Mesh(mesh.devices.reshape(2, 2, 4, 2, 2, 2, 2), (*GRP, *BLK))
    placed = (P(BLK_GRP),) * 8 + (
        P(GRP, BLK, None, None),
        P(GRP, None, BLK),
        P(GRP, BLK, None, None),
        P(GRP, BLK),
        P(GRP, BLK),
    )
    return jax.shard_map(steps, mesh=finer, in_specs=placed, out_specs=(P(BLK_GRP), P(BLK_GRP), P()), check_vma=False)
```
